32 devices in a mesh: dp: 4 (over y, z), a: 8 (over x, core).
Axes of the slice: x: 4, y: 2, z: 2, core: 2. Of those that a mesh axis runs over, the one named last changes fastest.
The devices are a block of a 4x4x8 slice.
Arguments:
- hidden_in: bfloat16 [4, 3584], P('dp'), parts along dimension 0
- loc_k: bfloat16 [4, 8, 8192, 256], P('dp', None, 'a'), parts along dimension 0
- loc_v: bfloat16 [4, 8, 8192, 256], P('dp', None, 'a'), parts along dimension 0
- glo_k: bfloat16 [4, 8, 8192, 256], P('dp', None, 'a'), parts along dimension 0
- glo_v: bfloat16 [4, 8, 8192, 256], P('dp', None, 'a'), parts along dimension 0
- loc_wq: bfloat16 [3584, 4096], P(None, 'a')
- loc_wk: bfloat16 [3584, 2048], P(None, 'a')
- loc_wv: bfloat16 [3584, 2048], P(None, 'a')
- loc_wo: bfloat16 [4096, 3584], P('a')
- loc_pre: bfloat16 [3584], replicated
- loc_post: bfloat16 [3584], replicated
- glo_wq: bfloat16 [3584, 4096], P(None, 'a')
- glo_wk: bfloat16 [3584, 2048], P(None, 'a')
- glo_wv: bfloat16 [3584, 2048], P(None, 'a')
- glo_wo: bfloat16 [4096, 3584], P('a')
- glo_pre: bfloat16 [3584], replicated
- glo_post: bfloat16 [3584], replicated
Outputs:
- output 1: bfloat16 [4, 3584], P('dp'), parts along dimension 0
- output 2: bfloat16 [4, 8, 4096, 256], P('dp', 'a'), parts along dimension 0
- output 3: bfloat16 [4, 8, 4096, 256], P('dp', 'a'), parts along dimension 0
- output 4: bfloat16 [4, 8, 8704, 256], P('dp', 'a'), parts along dimension 0
- output 5: bfloat16 [4, 8, 8704, 256], P('dp', 'a'), parts along dimension 0
There are 4 independent parts. The reference program is written for one: setup_inputs(seed, part) draws one part's arguments, and reference() takes and returns one part's arrays. A program takes and returns all parts, laid end to end along the dimension named above; an argument that names none is the same for every part.
All inputs are finite; a program needn't handle non-finite values.
Results may differ from the reference program's by a relative error of at most 0.02.
Values are sent between devices in bfloat16 or wider.
A program may use at most 768 MiB of HBM per device.

```python
import jax
import jax.numpy as jnp
from jax import lax

BATCH_SIZE = 1
SEQ_LEN = 8192
WINDOW = 4096
D_MODEL = 3584
NUM_HEADS = 16
KV_HEADS = 8
HEAD_DIM = 256
CACHE_ROOM = 512

Q_GROUPS = NUM_HEADS // KV_HEADS
Q_COLS = NUM_HEADS * HEAD_DIM
KV_COLS = KV_HEADS * HEAD_DIM
SOFTCAP = 50.0
NORM_EPS = 1e-6
ROPE_BASE = 10000.0
KEY_GAIN = 4.0


def draw_normal(rng_key, shape, std_dev):
    return (std_dev * jax.random.normal(rng_key, shape, jnp.float32)).astype(jnp.bfloat16)


def setup_inputs(seed: int = 0, part: int = 0) -> dict:
    part_keys = jax.random.split(jax.random.fold_in(jax.random.key(seed), part), 5)
    shared_keys = jax.random.split(jax.random.key(seed + 1), 12)
    cache_shape = (BATCH_SIZE, KV_HEADS, SEQ_LEN, HEAD_DIM)
    in_std = D_MODEL ** -0.5
    key_std = KEY_GAIN * in_std
    out_std = Q_COLS ** -0.5
    return {
        'hidden_in': draw_normal(part_keys[0], (BATCH_SIZE, D_MODEL), 1.0),
        'loc_k': draw_normal(part_keys[1], cache_shape, 1.0),
        'loc_v': draw_normal(part_keys[2], cache_shape, 1.0),
        'glo_k': draw_normal(part_keys[3], cache_shape, 1.0),
        'glo_v': draw_normal(part_keys[4], cache_shape, 1.0),
        'loc_wq': draw_normal(shared_keys[0], (D_MODEL, Q_COLS), in_std),
        'loc_wk': draw_normal(shared_keys[1], (D_MODEL, KV_COLS), key_std),
        'loc_wv': draw_normal(shared_keys[2], (D_MODEL, KV_COLS), in_std),
        'loc_wo': draw_normal(shared_keys[3], (Q_COLS, D_MODEL), out_std),
        'loc_pre': draw_normal(shared_keys[4], (D_MODEL,), 0.5),
        'loc_post': draw_normal(shared_keys[5], (D_MODEL,), 0.5),
        'glo_wq': draw_normal(shared_keys[6], (D_MODEL, Q_COLS), in_std),
        'glo_wk': draw_normal(shared_keys[7], (D_MODEL, KV_COLS), key_std),
        'glo_wv': draw_normal(shared_keys[8], (D_MODEL, KV_COLS), in_std),
        'glo_wo': draw_normal(shared_keys[9], (Q_COLS, D_MODEL), out_std),
        'glo_pre': draw_normal(shared_keys[10], (D_MODEL,), 0.5),
        'glo_post': draw_normal(shared_keys[11], (D_MODEL,), 0.5),
    }


def rms_norm(hidden, gain):
    mean_sq = jnp.mean(hidden * hidden, axis=-1, keepdims=True)
    return hidden * lax.rsqrt(mean_sq + NORM_EPS) * (1.0 + gain.astype(jnp.float32))


def rope_at(heads, position):
    half_dim = HEAD_DIM // 2
    inv_freq = ROPE_BASE ** (-2.0 * jnp.arange(half_dim, dtype=jnp.float32) / HEAD_DIM)
    angles = position * inv_freq
    cosine = jnp.cos(angles)
    sine_val = jnp.sin(angles)
    first_half = heads[..., :half_dim]
    second_half = heads[..., half_dim:]
    return jnp.concatenate([first_half * cosine - second_half * sine_val, second_half * cosine + first_half * sine_val], axis=-1)


def attend(q_heads, keys_all, values_all):
    scores = jnp.einsum('bkgd,bkld->bkgl', q_heads.astype(jnp.float32), keys_all.astype(jnp.float32)) * HEAD_DIM ** -0.5
    scores = SOFTCAP * jnp.tanh(scores / SOFTCAP)
    top_score = jnp.max(scores, axis=-1, keepdims=True)
    weights = jnp.exp(scores - top_score)
    denom_sum = jnp.sum(weights, axis=-1, keepdims=True)
    weighted = jnp.einsum('bkgl,bkld->bkgd', weights.astype(jnp.bfloat16).astype(jnp.float32), values_all.astype(jnp.float32))
    return (weighted / denom_sum).astype(jnp.bfloat16).reshape(BATCH_SIZE, Q_COLS)


def layer_step(hidden, cache_k, cache_v, w_q, w_k, w_v, w_o, pre_gain, post_gain, is_local):
    normed = rms_norm(hidden.astype(jnp.float32), pre_gain).astype(jnp.bfloat16)
    q_proj = jnp.dot(normed, w_q, preferred_element_type=jnp.float32).reshape(BATCH_SIZE, KV_HEADS, Q_GROUPS, HEAD_DIM)
    q_heads = rope_at(q_proj, SEQ_LEN).astype(jnp.bfloat16)
    k_proj = jnp.dot(normed, w_k, preferred_element_type=jnp.float32).reshape(BATCH_SIZE, KV_HEADS, 1, HEAD_DIM)
    new_k = rope_at(k_proj, SEQ_LEN).astype(jnp.bfloat16)
    new_v = jnp.dot(normed, w_v, preferred_element_type=jnp.float32).astype(jnp.bfloat16).reshape(BATCH_SIZE, KV_HEADS, 1, HEAD_DIM)
    if is_local:
        ordered_k = jnp.concatenate([cache_k[:, :, SEQ_LEN - WINDOW + 1:], new_k], axis=2)
        ordered_v = jnp.concatenate([cache_v[:, :, SEQ_LEN - WINDOW + 1:], new_v], axis=2)
        attn_out = attend(q_heads, ordered_k, ordered_v)
        out_k = jnp.roll(ordered_k, (SEQ_LEN + 1) % WINDOW, axis=2)
        out_v = jnp.roll(ordered_v, (SEQ_LEN + 1) % WINDOW, axis=2)
    else:
        zero_pad = jnp.zeros((BATCH_SIZE, KV_HEADS, CACHE_ROOM - 1, HEAD_DIM), jnp.bfloat16)
        out_k = jnp.concatenate([cache_k, new_k, zero_pad], axis=2)
        out_v = jnp.concatenate([cache_v, new_v, zero_pad], axis=2)
        attn_out = attend(q_heads, out_k[:, :, :SEQ_LEN + 1], out_v[:, :, :SEQ_LEN + 1])
    proj_out = jnp.dot(attn_out, w_o, preferred_element_type=jnp.float32)
    hidden = (hidden.astype(jnp.float32) + rms_norm(proj_out, post_gain)).astype(jnp.bfloat16)
    return hidden, out_k, out_v


def reference(hidden_in, loc_k, loc_v, glo_k, glo_v, loc_wq, loc_wk, loc_wv, loc_wo, loc_pre, loc_post, glo_wq, glo_wk, glo_wv, glo_wo, glo_pre, glo_post):
    hidden, loc_k_out, loc_v_out = layer_step(hidden_in, loc_k, loc_v, loc_wq, loc_wk, loc_wv, loc_wo, loc_pre, loc_post, True)
    hidden_out, glo_k_out, glo_v_out = layer_step(hidden, glo_k, glo_v, glo_wq, glo_wk, glo_wv, glo_wo, glo_pre, glo_post, False)
    return (hidden_out, loc_k_out, loc_v_out, glo_k_out, glo_v_out)
```

```python
import functools

import jax
import jax.numpy as jnp
import numpy as np
from jax import lax
from jax.experimental import pallas as pl
from jax.experimental.pallas import tpu as pltpu
from jax.sharding import PartitionSpec as P

SOFTCAP = 50.0
NORM_EPS = 1e-6
ROPE_BASE = 10000.0
WINDOW = 4096
CACHE_ROOM = 512
MESH = pl.DeviceIdType.MESH
CORES = 2
ROW = 512
NEG = -1e30


def rope_tables(head_dim, position):
    half = head_dim // 2
    inv = np.float32(ROPE_BASE) ** (np.float32(-2.0) * np.arange(half, dtype=np.float32) / np.float32(head_dim))
    ang = np.float32(position) * inv.astype(np.float32)
    return np.cos(ang).astype(np.float32), np.sin(ang).astype(np.float32)


def softcap(scores, scale):
    return SOFTCAP * jnp.tanh(scores * scale / SOFTCAP)


def rows_like(width):
    return lax.broadcasted_iota(jnp.int32, (8, width), 0)


class Kernel:
    def __init__(self, n, d_model, heads, blk, hd, slots):
        self.n, self.d_model, self.heads, self.blk, self.hd, self.slots = n, d_model, heads, blk, hd, slots
        self.seq = n * blk
        self.first_pos = self.seq - WINDOW + 1
        self.first_src = self.first_pos // blk
        self.chunks = d_model // ROW
        self.q_groups = 2

    def __call__(self, small, loc_k, loc_v, glo_k, glo_v, lwq, lwk, lwv, lwo, gwq, gwk, gwv, gwo,
                 hid_out, lk_out, lv_out, gk_out, gv_out,
                 wq_b, wk_b, wv_b, wo_b, kv_b, q_msg, q_all, p_msg, p_all, y_all,
                 f_sem, g_sem, d_sem, own_sem, glo_rsem, loc_rsem, w_sem, kv_sem,
                 qs_sem, qr_sem, ps_sem, pr_sem, ys_sem, yr_sem):
        n, blk, hd = self.n, self.blk, self.hd
        half = hd // 2
        me = lax.axis_index("a")
        chips = n // CORES
        chip, core = me // CORES, lax.rem(me, CORES)
        has_loc = me >= self.first_src
        right, left, opp = [lax.rem(chip + i, chips) for i in (1, chips - 1, chips // 2)]
        even = lax.rem(chip, 2) == 0
        near_f = jnp.where(even, right, left)
        near_g = jnp.where(even, left, right)

        barrier = pltpu.get_barrier_semaphore()
        for i in range(1, n):
            pl.semaphore_signal(barrier, inc=1, device_id={"a": lax.rem(me + i, n)}, device_id_type=MESH)

        weights = [((lwq, gwq), wq_b), ((lwk, gwk), wk_b), ((lwv, gwv), wv_b), ((lwo, gwo), wo_b)]
        w_cp = [[pltpu.make_async_copy(srcs[la], dst.at[la], w_sem.at[la, j]) for j, (srcs, dst) in enumerate(weights)] for la in range(2)]
        kv_cp = [[pltpu.make_async_copy(src.at[0], kv_b.at[la, j], kv_sem.at[la, j]) for j, src in enumerate(pair)]
                 for la, pair in enumerate(((loc_k, loc_v), (glo_k, glo_v)))]
        glo_pairs = ((glo_k, gk_out), (glo_v, gv_out))
        loc_pairs = ((loc_k, lk_out), (loc_v, lv_out))

        def glo_dst(out, src_dev):
            return out.at[0, 0, pl.ds(pl.multiple_of(src_dev * blk, blk), blk)]

        def loc_dst(out, src_dev):
            return out.at[0, 0, pl.ds(pl.multiple_of(lax.rem(src_dev * blk, WINDOW), blk), blk)]

        for j in range(3):
            w_cp[0][j].start()

        @pl.when(has_loc)
        def _():
            for cp in kv_cp[0]:
                cp.start()

        w_cp[0][3].start()

        pl.semaphore_wait(barrier, n - 1)

        def glo_send(kv, dst, sem):
            src, out = glo_pairs[kv]
            return pltpu.make_async_remote_copy(src_ref=src.at[0, dst], dst_ref=glo_dst(out, me), send_sem=sem,
                                                recv_sem=glo_rsem.at[kv, me], device_id={"a": dst}, device_id_type=MESH)

        def loc_send(kv, dst, sem):
            src, out = loc_pairs[kv]
            return pltpu.make_async_remote_copy(src_ref=src.at[0, dst], dst_ref=loc_dst(out, me), send_sem=sem,
                                                recv_sem=loc_rsem.at[kv, me], device_id={"a": dst}, device_id_type=MESH)

        def step_items(step):
            dst_chip = near_f if step < 4 else opp
            part = step % 4
            items = [(part % 2, dst_chip * CORES + lax.rem(core + part // 2, CORES), f_sem, step)]
            if step < 4:
                items.append((part % 2, near_g * CORES + lax.rem(core + part // 2, CORES), g_sem, step))
            return items

        def bulk_start(step):
            items = step_items(step)
            for kv, dst, sem, s in items:
                glo_send(kv, dst, sem.at[s, 0]).start()

            @pl.when(has_loc)
            def _():
                for kv, dst, sem, s in items:
                    loc_send(kv, dst, sem.at[s, 1]).start()

        def bulk_wait(step):
            items = step_items(step)
            for kv, dst, sem, s in items:
                glo_send(kv, dst, sem.at[s, 0]).wait_send()

            @pl.when(has_loc)
            def _():
                for kv, dst, sem, s in items:
                    loc_send(kv, dst, sem.at[s, 1]).wait_send()

        bulk_start(0)
        mate = chip * CORES + (CORES - 1 - core)
        own_glo = [pltpu.make_async_copy(src.at[0, me], glo_dst(out, me), own_sem.at[0, kv]) for kv, (src, out) in enumerate(glo_pairs)]
        own_loc = [pltpu.make_async_copy(src.at[0, me], loc_dst(out, me), own_sem.at[1, kv]) for kv, (src, out) in enumerate(loc_pairs)]
        for kv in range(2):
            glo_send(kv, mate, d_sem.at[0, kv]).start()
            own_glo[kv].start()

        @pl.when(has_loc)
        def _():
            for kv in range(2):
                loc_send(kv, mate, d_sem.at[1, kv]).start()
                own_loc[kv].start()

        for cp in w_cp[1] + kv_cp[1]:
            cp.start()

        def q_send(la, dst, i):
            return pltpu.make_async_remote_copy(src_ref=q_msg.at[la], dst_ref=q_all.at[la, me], send_sem=qs_sem.at[la, i - 1],
                                                recv_sem=qr_sem.at[la, me], device_id={"a": dst}, device_id_type=MESH)

        def p_send(la, dst, i):
            return pltpu.make_async_remote_copy(src_ref=p_msg.at[la, dst], dst_ref=p_all.at[la, me], send_sem=ps_sem.at[la, i - 1],
                                                recv_sem=pr_sem.at[la, me], device_id={"a": dst}, device_id_type=MESH)

        def y_send(la, dst, i):
            return pltpu.make_async_remote_copy(src_ref=y_all.at[la, me], dst_ref=y_all.at[la, me], send_sem=ys_sem.at[la, i - 1],
                                                recv_sem=yr_sem.at[la, me], device_id={"a": dst}, device_id_type=MESH)

        def q_arrival(la, src):
            return pltpu.make_async_remote_copy(src_ref=q_msg.at[la], dst_ref=q_all.at[la, src], send_sem=qs_sem.at[la, 0],
                                                recv_sem=qr_sem.at[la, src], device_id={"a": src}, device_id_type=MESH)

        def p_arrival(la, src):
            return pltpu.make_async_remote_copy(src_ref=p_msg.at[la, 0], dst_ref=p_all.at[la, src], send_sem=ps_sem.at[la, 0],
                                                recv_sem=pr_sem.at[la, src], device_id={"a": src}, device_id_type=MESH)

        def y_arrival(la, src):
            return pltpu.make_async_remote_copy(src_ref=y_all.at[la, src], dst_ref=y_all.at[la, src], send_sem=ys_sem.at[la, 0],
                                                recv_sem=yr_sem.at[la, src], device_id={"a": src}, device_id_type=MESH)

        def peers():
            return [(lax.rem(me + i, n), i) for i in range(1, n)]

        def norm(x):
            total = jnp.sum(jnp.sum(x * x, axis=1, keepdims=True), axis=0, keepdims=True)
            return x * lax.rsqrt(total / self.d_model + NORM_EPS)

        cosine = small[5, 0:1, 0:half]
        sine = small[5, 1:2, 0:half]

        def rope(x):
            first, second = x[:, :half], x[:, half:]
            return jnp.concatenate([first * cosine - second * sine, second * cosine + first * sine], axis=1)

        def round_bf16(x):
            return x.astype(jnp.bfloat16).astype(jnp.float32)

        def project(la, hidden, gain):
            a = norm(hidden) * (1.0 + gain)
            for j in range(3):
                w_cp[la][j].wait()
            q = k = v = None
            for i in range(self.chunks):
                lhs = jnp.broadcast_to(a[i:i + 1, :], (16, ROW)).astype(jnp.bfloat16)
                part = [jnp.dot(lhs, w[la, i * ROW:(i + 1) * ROW, :], preferred_element_type=jnp.float32) for w in (wq_b, wk_b, wv_b)]
                q, k, v = part if q is None else (q + part[0], k + part[1], v + part[2])
            q, k, v = q[:8], k[:8], v[:8]
            q0, q1 = rope(q[:, :hd]), rope(q[:, hd:])
            q = round_bf16(jnp.where(rows_like(hd) == 0, q0, q1))
            return q, round_bf16(rope(k)), round_bf16(v)

        def attend_block(la, h, masked):
            q = q_all[la, h].astype(jnp.bfloat16)
            s = lax.dot_general(q, kv_b[la, 0, h], (((1,), (1,)), ((), ())), preferred_element_type=jnp.float32)
            s = softcap(s, hd ** -0.5)
            if masked:
                pos = me * blk + lax.broadcasted_iota(jnp.int32, s.shape, 1)
                s = jnp.where(pos >= self.first_pos, s, NEG)
            top = jnp.max(s, axis=1, keepdims=True)
            e = jnp.exp(s - top)
            if masked:
                e = jnp.where(pos >= self.first_pos, e, 0.0)
            total = jnp.sum(e, axis=1, keepdims=True)
            o = jnp.dot(e.astype(jnp.bfloat16), kv_b[la, 1, h], preferred_element_type=jnp.float32)
            lane = lax.broadcasted_iota(jnp.int32, (8, 128), 1)
            p_msg[la, h, :, 0:hd] = o
            p_msg[la, h, :, hd:hd + 128] = jnp.where(lane < 64, top, total)

        def attend_all(la, masked):
            for cp in kv_cp[la]:
                cp.wait()

            def body(h, carry):
                attend_block(la, h, masked)
                return carry

            lax.fori_loop(0, n, body, 0)
            for dst, i in peers():
                p_send(la, dst, i).start()
            p_all[la, me] = p_msg[la, me]

        def combine(la, q, k_new, v_new, first_src):
            s_new = softcap(jnp.sum(q * k_new, axis=1, keepdims=True), hd ** -0.5)
            tops = [p_all[la, s, :, hd:hd + 1] for s in range(first_src, n)]
            sums = [p_all[la, s, :, hd + 64:hd + 65] for s in range(first_src, n)]
            top = s_new
            for t in tops:
                top = jnp.maximum(top, t)
            e_new = jnp.exp(s_new - top)
            denom = e_new
            o = round_bf16(e_new) * v_new
            for idx, s in enumerate(range(first_src, n)):
                w = jnp.exp(tops[idx] - top)
                denom = denom + w * sums[idx]
                o = o + w * p_all[la, s, :, 0:hd]
            return o / denom

        def out_project(la, o):
            w_cp[la][3].wait()
            lhs = [jnp.broadcast_to(o[g:g + 1, :], (16, hd)).astype(jnp.bfloat16) for g in range(self.q_groups)]
            row = rows_like(ROW)
            msg = jnp.zeros((8, ROW), jnp.float32)
            for i in range(self.chunks):
                y = None
                for g in range(self.q_groups):
                    part = jnp.dot(lhs[g], wo_b[la, g * hd:(g + 1) * hd, i * ROW:(i + 1) * ROW], preferred_element_type=jnp.float32)
                    y = part if y is None else y + part
                msg = jnp.where(row == i, y[:8], msg)
            y_all[la, me] = msg
            for dst, i in peers():
                y_send(la, dst, i).start()

        hidden = small[0]
        fresh = []
        for la in range(2):
            pre, post = small[1 + 2 * la], small[2 + 2 * la]
            q, k_new, v_new = project(la, hidden, pre)
            fresh.append((k_new, v_new))
            q_msg[la] = q
            q_all[la, me] = q
            for dst, i in peers():
                q_send(la, dst, i).start()
            step = 3 * la + 1
            bulk_start(step)
            bulk_wait(step - 1)
            for src, i in peers():
                q_arrival(la, src).wait_recv()
            if la == 0:
                @pl.when(has_loc)
                def _():
                    attend_all(0, True)
            else:
                attend_all(1, False)
            bulk_start(step + 1)
            bulk_wait(step)
            first_src = self.first_src if la == 0 else 0
            for src, i in peers():
                if la == 0:
                    @pl.when(src >= first_src)
                    def _():
                        p_arrival(0, src).wait_recv()
                else:
                    p_arrival(la, src).wait_recv()
            out_project(la, combine(la, q, k_new, v_new, first_src))
            bulk_start(step + 2)
            bulk_wait(step + 1)
            for src, i in peers():
                y_arrival(la, src).wait_recv()
            y = y_all[la, 0]
            for s in range(1, n):
                y = y + y_all[la, s]
            hidden = round_bf16(hidden + norm(y) * (1.0 + post))
        for i in range(self.chunks):
            hid_out[:, i * ROW:(i + 1) * ROW] = hidden[i:i + 1, :].astype(jnp.bfloat16)

        bulk_start(7)
        row16 = lax.broadcasted_iota(jnp.int32, (16, hd), 0)
        for kv, out in enumerate((gk_out, gv_out)):
            new = jnp.concatenate([fresh[1][kv], fresh[1][kv]], axis=0)
            out[0, 0, self.seq:self.seq + 16, :] = jnp.where(row16 == 0, new, 0.0).astype(jnp.bfloat16)
            out[0, 0, self.seq + 16:self.slots, :] = jnp.zeros((self.slots - self.seq - 16, hd), jnp.bfloat16)

        for la in range(2):
            for dst, i in peers():
                q_send(la, dst, i).wait_send()
                y_send(la, dst, i).wait_send()
        for dst, i in peers():
            p_send(1, dst, i).wait_send()

        @pl.when(has_loc)
        def _():
            for dst, i in peers():
                p_send(0, dst, i).wait_send()
            for kv in range(2):
                loc_send(kv, mate, d_sem.at[1, kv]).wait_send()
                own_loc[kv].wait()

        for kv in range(2):
            glo_send(kv, mate, d_sem.at[0, kv]).wait_send()
            own_glo[kv].wait()

        def glo_arrival(kv, src_dev):
            src, out = glo_pairs[kv]
            return pltpu.make_async_remote_copy(src_ref=src.at[0, 0], dst_ref=glo_dst(out, src_dev), send_sem=d_sem.at[0, kv],
                                                recv_sem=glo_rsem.at[kv, src_dev], device_id={"a": src_dev}, device_id_type=MESH)

        def loc_arrival(kv, src_dev):
            src, out = loc_pairs[kv]
            return pltpu.make_async_remote_copy(src_ref=src.at[0, 0], dst_ref=loc_dst(out, src_dev), send_sem=d_sem.at[1, kv],
                                                recv_sem=loc_rsem.at[kv, src_dev], device_id={"a": src_dev}, device_id_type=MESH)

        for src_dev, i in peers():
            @pl.when(src_dev >= self.first_src)
            def _():
                for kv in range(2):
                    loc_arrival(kv, src_dev).wait_recv()
        slot = (self.seq % WINDOW) // 16 * 16
        for kv, out in enumerate((lk_out, lv_out)):
            new = jnp.concatenate([fresh[0][kv], fresh[0][kv]], axis=0)
            old = out[0, 0, slot:slot + 16, :].astype(jnp.float32)
            out[0, 0, slot:slot + 16, :] = jnp.where(row16 == self.seq % WINDOW - slot, new, old).astype(jnp.bfloat16)

        bulk_wait(6)
        bulk_wait(7)
        for src_dev, i in peers():
            for kv in range(2):
                glo_arrival(kv, src_dev).wait_recv()


def solution(mesh):
    n = mesh.shape["a"]
    cache_in = P("dp", None, "a", None)
    cache_out = P("dp", "a", None, None)
    rows_spec = P("dp", None)
    layer_specs = (P(None, "a"), P(None, "a"), P(None, "a"), P("a", None), P(None), P(None))
    in_specs = (rows_spec, cache_in, cache_in, cache_in, cache_in) + layer_specs + layer_specs
    out_specs = (rows_spec, cache_out, cache_out, cache_out, cache_out)

    def device_step(hidden_in, loc_k, loc_v, glo_k, glo_v, loc_wq, loc_wk, loc_wv, loc_wo, loc_pre, loc_post, glo_wq, glo_wk, glo_wv, glo_wo, glo_pre, glo_post):
        d_model = hidden_in.shape[1]
        rows, heads, blk, hd = loc_k.shape
        q_cols, kv_cols = loc_wq.shape[1], loc_wk.shape[1]
        seq = n * blk
        slots = seq + CACHE_ROOM
        pad = 8 * ROW - d_model

        def tile(x):
            return jnp.pad(x.astype(jnp.float32).reshape(-1), (0, 8 * ROW - x.size)).reshape(8, ROW)

        cosine, sine = rope_tables(hd, seq)
        table = np.zeros((8, ROW), np.float32)
        table[0, :hd // 2], table[1, :hd // 2] = cosine, sine
        small = jnp.stack([tile(hidden_in), tile(loc_pre), tile(loc_post), tile(glo_pre), tile(glo_post), jnp.asarray(table)])

        vmem = pl.BlockSpec(memory_space=pltpu.VMEM)
        hbm = pl.BlockSpec(memory_space=pltpu.HBM)
        bf16, f32 = jnp.bfloat16, jnp.float32
        dma = pltpu.SemaphoreType.DMA
        return pl.pallas_call(
            Kernel(n, d_model, heads, blk, hd, slots),
            name="decode_step",
            out_shape=(
                jax.ShapeDtypeStruct(hidden_in.shape, bf16),
                pltpu.VMEM((rows, 1, WINDOW, hd), bf16),
                pltpu.VMEM((rows, 1, WINDOW, hd), bf16),
                pltpu.VMEM((rows, 1, slots, hd), bf16),
                pltpu.VMEM((rows, 1, slots, hd), bf16),
            ),
            in_specs=[vmem] + [hbm] * 12,
            out_specs=(vmem,) * 5,
            scratch_shapes=[
                pltpu.VMEM((2, d_model, q_cols), bf16),
                pltpu.VMEM((2, d_model, kv_cols), bf16),
                pltpu.VMEM((2, d_model, kv_cols), bf16),
                pltpu.VMEM((2, q_cols, d_model), bf16),
                pltpu.VMEM((2, 2, heads, blk, hd), bf16),
                pltpu.VMEM((2, 8, hd), f32),
                pltpu.VMEM((2, n, 8, hd), f32),
                pltpu.VMEM((2, n, 8, hd + 128), f32),
                pltpu.VMEM((2, n, 8, hd + 128), f32),
                pltpu.VMEM((2, n, 8, ROW), f32),
                dma((8, 2)), dma((4, 2)), dma((2, 2)), dma((2, 2)), dma((2, n)), dma((2, n)), dma((2, 4)), dma((2, 2)),
                dma((2, n - 1)), dma((2, n)), dma((2, n - 1)), dma((2, n)), dma((2, n - 1)), dma((2, n)),
            ],
            compiler_params=pltpu.CompilerParams(collective_id=0, has_side_effects=True, vmem_limit_bytes=48 * 2**20),
        )(small, loc_k, loc_v, glo_k, glo_v, loc_wq, loc_wk, loc_wv, loc_wo, glo_wq, glo_wk, glo_wv, glo_wo)

    return jax.shard_map(device_step, mesh=mesh, in_specs=in_specs, out_specs=out_specs, check_vma=False)
```

```python
import functools

import jax
import jax.numpy as jnp
import numpy as np
from jax import lax
from jax.experimental import pallas as pl
from jax.experimental.pallas import tpu as pltpu
from jax.sharding import PartitionSpec as P

SOFTCAP = 50.0
NORM_EPS = 1e-6
ROPE_BASE = 10000.0
WINDOW = 4096
CACHE_ROOM = 512
MESH = pl.DeviceIdType.MESH
CORES = 2
ROW = 512
STORE_PARTS = 4
NEG = -1e30


def rope_tables(head_dim, position):
    half = head_dim // 2
    inv = np.float32(ROPE_BASE) ** (np.float32(-2.0) * np.arange(half, dtype=np.float32) / np.float32(head_dim))
    ang = np.float32(position) * inv.astype(np.float32)
    return np.cos(ang).astype(np.float32), np.sin(ang).astype(np.float32)


def softcap(scores, scale):
    return SOFTCAP * jnp.tanh(scores * scale / SOFTCAP)


def rows_like(width):
    return lax.broadcasted_iota(jnp.int32, (8, width), 0)


def store_outputs(*refs):
    landed, outs, sem = refs[:5], refs[5:10], refs[10]
    copies = [pltpu.make_async_copy(landed[0], outs[0], sem.at[0, 0])]
    for j in range(1, 5):
        part = landed[j].shape[2] // STORE_PARTS
        for p in range(STORE_PARTS):
            rows = pl.ds(p * part, part)
            copies.append(pltpu.make_async_copy(landed[j].at[0, 0, rows], outs[j].at[0, 0, rows], sem.at[j, p]))
    for cp in copies:
        cp.start()
    for cp in copies:
        cp.wait()


class Kernel:
    def __init__(self, n, d_model, heads, blk, hd, slots):
        self.n, self.d_model, self.heads, self.blk, self.hd, self.slots = n, d_model, heads, blk, hd, slots
        self.seq = n * blk
        self.first_pos = self.seq - WINDOW + 1
        self.first_src = self.first_pos // blk
        self.chunks = d_model // ROW
        self.q_groups = 2

    def __call__(self, hid_in, table_in, loc_k, loc_v, glo_k, glo_v, lwq, lwk, lwv, lwo, lpre, lpost, gwq, gwk, gwv, gwo, gpre, gpost,
                 hid_out, lk_out, lv_out, gk_out, gv_out,
                 hid_b, table, gain_b, wq_b, wk_b, wv_b, wo_b, kv_b, q_msg, q_all, p_msg, p_all, y_all,
                 in_sem, f_sem, g_sem, d_sem, own_sem, glo_rsem, loc_rsem, w_sem, kv_sem,
                 qs_sem, qr_sem, ps_sem, pr_sem, ys_sem, yr_sem):
        n, blk, hd = self.n, self.blk, self.hd
        half = hd // 2
        me = lax.axis_index("a")
        chips = n // CORES
        chip, core = me // CORES, lax.rem(me, CORES)
        has_loc = me >= self.first_src
        right, left, opp = [lax.rem(chip + i, chips) for i in (1, chips - 1, chips // 2)]
        even = lax.rem(chip, 2) == 0
        near_f = jnp.where(even, right, left)
        near_g = jnp.where(even, left, right)

        barrier = pltpu.get_barrier_semaphore()
        for i in range(1, n):
            pl.semaphore_signal(barrier, inc=1, device_id={"a": lax.rem(me + i, n)}, device_id_type=MESH)

        weights = [((lwq, gwq), wq_b), ((lwk, gwk), wk_b), ((lwv, gwv), wv_b), ((lwo, gwo), wo_b)]
        w_cp = [[pltpu.make_async_copy(srcs[la], dst.at[la], w_sem.at[la, j]) for j, (srcs, dst) in enumerate(weights)] for la in range(2)]
        kv_cp = [[pltpu.make_async_copy(src.at[0], kv_b.at[la, j], kv_sem.at[la, j]) for j, src in enumerate(pair)]
                 for la, pair in enumerate(((loc_k, loc_v), (glo_k, glo_v)))]
        glo_pairs = ((glo_k, gk_out), (glo_v, gv_out))
        loc_pairs = ((loc_k, lk_out), (loc_v, lv_out))

        def glo_dst(out, src_dev):
            return out.at[0, 0, pl.ds(pl.multiple_of(src_dev * blk, blk), blk)]

        def loc_dst(out, src_dev):
            return out.at[0, 0, pl.ds(pl.multiple_of(lax.rem(src_dev * blk, WINDOW), blk), blk)]

        in_cp = [pltpu.make_async_copy(hid_in, hid_b, in_sem.at[0]), pltpu.make_async_copy(table_in, table, in_sem.at[1])]
        in_cp += [pltpu.make_async_copy(g, b, in_sem.at[2 + j]) for j, (g, b) in enumerate(zip((lpre, lpost, gpre, gpost), gain_b))]
        for cp in in_cp + w_cp[0][:3]:
            cp.start()

        @pl.when(has_loc)
        def _():
            for cp in kv_cp[0]:
                cp.start()

        w_cp[0][3].start()

        pl.semaphore_wait(barrier, n - 1)

        def glo_send(kv, dst, sem):
            src, out = glo_pairs[kv]
            return pltpu.make_async_remote_copy(src_ref=src.at[0, dst], dst_ref=glo_dst(out, me), send_sem=sem,
                                                recv_sem=glo_rsem.at[kv, me], device_id={"a": dst}, device_id_type=MESH)

        def loc_send(kv, dst, sem):
            src, out = loc_pairs[kv]
            return pltpu.make_async_remote_copy(src_ref=src.at[0, dst], dst_ref=loc_dst(out, me), send_sem=sem,
                                                recv_sem=loc_rsem.at[kv, me], device_id={"a": dst}, device_id_type=MESH)

        def step_items(step):
            dst_chip = near_f if step < 4 else opp
            part = step % 4
            items = [(part % 2, dst_chip * CORES + lax.rem(core + part // 2, CORES), f_sem, step)]
            if step < 4:
                items.append((part % 2, near_g * CORES + lax.rem(core + part // 2, CORES), g_sem, step))
            return items

        def bulk_start(step):
            items = step_items(step)
            for kv, dst, sem, s in items:
                glo_send(kv, dst, sem.at[s, 0]).start()

            @pl.when(has_loc)
            def _():
                for kv, dst, sem, s in items:
                    loc_send(kv, dst, sem.at[s, 1]).start()

        def bulk_wait(step):
            items = step_items(step)
            for kv, dst, sem, s in items:
                glo_send(kv, dst, sem.at[s, 0]).wait_send()

            @pl.when(has_loc)
            def _():
                for kv, dst, sem, s in items:
                    loc_send(kv, dst, sem.at[s, 1]).wait_send()

        bulk_start(0)
        mate = chip * CORES + (CORES - 1 - core)
        own_glo = [pltpu.make_async_copy(src.at[0, me], glo_dst(out, me), own_sem.at[0, kv]) for kv, (src, out) in enumerate(glo_pairs)]
        own_loc = [pltpu.make_async_copy(src.at[0, me], loc_dst(out, me), own_sem.at[1, kv]) for kv, (src, out) in enumerate(loc_pairs)]
        for kv in range(2):
            glo_send(kv, mate, d_sem.at[0, kv]).start()
            own_glo[kv].start()

        @pl.when(has_loc)
        def _():
            for kv in range(2):
                loc_send(kv, mate, d_sem.at[1, kv]).start()
                own_loc[kv].start()

        for cp in in_cp:
            cp.wait()

        def q_send(la, dst, i):
            return pltpu.make_async_remote_copy(src_ref=q_msg.at[la], dst_ref=q_all.at[la, me], send_sem=qs_sem.at[la, i - 1],
                                                recv_sem=qr_sem.at[la, me], device_id={"a": dst}, device_id_type=MESH)

        def p_send(la, dst, i):
            return pltpu.make_async_remote_copy(src_ref=p_msg.at[la, dst], dst_ref=p_all.at[la, me], send_sem=ps_sem.at[la, i - 1],
                                                recv_sem=pr_sem.at[la, me], device_id={"a": dst}, device_id_type=MESH)

        def y_send(la, dst, i):
            return pltpu.make_async_remote_copy(src_ref=y_all.at[la, me], dst_ref=y_all.at[la, me], send_sem=ys_sem.at[la, i - 1],
                                                recv_sem=yr_sem.at[la, me], device_id={"a": dst}, device_id_type=MESH)

        def q_arrival(la, src):
            return pltpu.make_async_remote_copy(src_ref=q_msg.at[la], dst_ref=q_all.at[la, src], send_sem=qs_sem.at[la, 0],
                                                recv_sem=qr_sem.at[la, src], device_id={"a": src}, device_id_type=MESH)

        def p_arrival(la, src):
            return pltpu.make_async_remote_copy(src_ref=p_msg.at[la, 0], dst_ref=p_all.at[la, src], send_sem=ps_sem.at[la, 0],
                                                recv_sem=pr_sem.at[la, src], device_id={"a": src}, device_id_type=MESH)

        def y_arrival(la, src):
            return pltpu.make_async_remote_copy(src_ref=y_all.at[la, src], dst_ref=y_all.at[la, src], send_sem=ys_sem.at[la, 0],
                                                recv_sem=yr_sem.at[la, src], device_id={"a": src}, device_id_type=MESH)

        def peers():
            return [(lax.rem(me + i, n), i) for i in range(1, n)]

        def norm(x):
            total = jnp.sum(jnp.sum(x * x, axis=1, keepdims=True), axis=0, keepdims=True)
            return x * lax.rsqrt(total / self.d_model + NORM_EPS)

        cosine, sine = table[0:1, :], table[1:2, :]

        def tiled(piece):
            row = rows_like(ROW)
            out = jnp.zeros((8, ROW), jnp.float32)
            for i in range(self.chunks):
                out = jnp.where(row == i, piece(i), out)
            return out

        def gain(j):
            return tiled(lambda i: gain_b[j][i * ROW:(i + 1) * ROW].astype(jnp.float32).reshape(1, ROW))

        def rope(x):
            first, second = x[:, :half], x[:, half:]
            return jnp.concatenate([first * cosine - second * sine, second * cosine + first * sine], axis=1)

        def round_bf16(x):
            return x.astype(jnp.bfloat16).astype(jnp.float32)

        def project(la, hidden, pre):
            a = norm(hidden) * (1.0 + pre)
            for j in range(3):
                w_cp[la][j].wait()
            q = k = v = None
            for i in range(self.chunks):
                lhs = jnp.broadcast_to(a[i:i + 1, :], (16, ROW)).astype(jnp.bfloat16)
                part = [jnp.dot(lhs, w[la, i * ROW:(i + 1) * ROW, :], preferred_element_type=jnp.float32) for w in (wq_b, wk_b, wv_b)]
                q, k, v = part if q is None else (q + part[0], k + part[1], v + part[2])
            q, k, v = q[:2], k[:2], v[:2]
            q0, q1 = rope(q[:, :hd]), rope(q[:, hd:])
            q = round_bf16(jnp.where(lax.broadcasted_iota(jnp.int32, (2, hd), 0) == 0, q0, q1))
            return q, round_bf16(rope(k)), round_bf16(v)

        def attend_block(la, h, masked):
            q = q_all[la, h].astype(jnp.bfloat16)
            s = lax.dot_general(q, kv_b[la, 0, h], (((1,), (1,)), ((), ())), preferred_element_type=jnp.float32)
            s = softcap(s, hd ** -0.5)
            if masked:
                pos = me * blk + lax.broadcasted_iota(jnp.int32, s.shape, 1)
                s = jnp.where(pos >= self.first_pos, s, NEG)
            top = jnp.max(s, axis=1, keepdims=True)
            e = jnp.exp(s - top)
            if masked:
                e = jnp.where(pos >= self.first_pos, e, 0.0)
            total = jnp.sum(e, axis=1, keepdims=True)
            o = jnp.dot(e.astype(jnp.bfloat16), kv_b[la, 1, h], preferred_element_type=jnp.float32)
            lane = lax.broadcasted_iota(jnp.int32, (2, 128), 1)
            p_msg[la, h, :, 0:hd] = o
            p_msg[la, h, :, hd:hd + 128] = jnp.where(lane < 64, top, total)

        def attend_all(la, masked):
            for cp in kv_cp[la]:
                cp.wait()

            def body(h, carry):
                attend_block(la, h, masked)
                return carry

            lax.fori_loop(0, n, body, 0)
            for dst, i in peers():
                p_send(la, dst, i).start()
            p_all[la, me] = p_msg[la, me]

        def combine(la, q, k_new, v_new, first_src):
            s_new = softcap(jnp.sum(q * k_new, axis=1, keepdims=True), hd ** -0.5)
            tops = [p_all[la, s, :, hd:hd + 1] for s in range(first_src, n)]
            sums = [p_all[la, s, :, hd + 64:hd + 65] for s in range(first_src, n)]
            top = s_new
            for t in tops:
                top = jnp.maximum(top, t)
            e_new = jnp.exp(s_new - top)
            denom = e_new
            o = round_bf16(e_new) * v_new
            for idx, s in enumerate(range(first_src, n)):
                w = jnp.exp(tops[idx] - top)
                denom = denom + w * sums[idx]
                o = o + w * p_all[la, s, :, 0:hd]
            return o / denom

        def out_project(la, o):
            w_cp[la][3].wait()
            lhs = [jnp.broadcast_to(o[g:g + 1, :], (16, hd)).astype(jnp.bfloat16) for g in range(self.q_groups)]
            row = rows_like(ROW)
            msg = jnp.zeros((8, ROW), jnp.float32)
            for i in range(self.chunks):
                y = None
                for g in range(self.q_groups):
                    part = jnp.dot(lhs[g], wo_b[la, g * hd:(g + 1) * hd, i * ROW:(i + 1) * ROW], preferred_element_type=jnp.float32)
                    y = part if y is None else y + part
                msg = jnp.where(row == i, y[:8], msg)
            y_all[la, me] = msg.astype(jnp.bfloat16)
            for dst, i in peers():
                y_send(la, dst, i).start()

        hidden = tiled(lambda i: hid_b[:, i * ROW:(i + 1) * ROW].astype(jnp.float32))
        fresh = []
        for la in range(2):
            pre, post = gain(2 * la), gain(2 * la + 1)
            q, k_new, v_new = project(la, hidden, pre)
            fresh.append((k_new, v_new))
            q_msg[la] = q
            q_all[la, me] = q
            for dst, i in peers():
                q_send(la, dst, i).start()
            step = 3 * la + 1
            bulk_start(step)
            bulk_wait(step - 1)
            if la == 0:
                for cp in w_cp[1] + kv_cp[1]:
                    cp.start()
            for src, i in peers():
                q_arrival(la, src).wait_recv()
            if la == 0:
                @pl.when(has_loc)
                def _():
                    attend_all(0, True)
            else:
                attend_all(1, False)
            bulk_start(step + 1)
            bulk_wait(step)
            first_src = self.first_src if la == 0 else 0
            for src, i in peers():
                if la == 0:
                    @pl.when(src >= first_src)
                    def _():
                        p_arrival(0, src).wait_recv()
                else:
                    p_arrival(la, src).wait_recv()
            out_project(la, combine(la, q, k_new, v_new, first_src))
            bulk_start(step + 2)
            bulk_wait(step + 1)
            for src, i in peers():
                y_arrival(la, src).wait_recv()
            y = y_all[la, 0].astype(jnp.float32)
            for s in range(1, n):
                y = y + y_all[la, s].astype(jnp.float32)
            hidden = round_bf16(hidden + norm(y) * (1.0 + post))
        for i in range(self.chunks):
            hid_out[:, i * ROW:(i + 1) * ROW] = hidden[i:i + 1, :].astype(jnp.bfloat16)

        bulk_start(7)
        row16 = lax.broadcasted_iota(jnp.int32, (16, hd), 0)
        for kv, out in enumerate((gk_out, gv_out)):
            new = jnp.broadcast_to(fresh[1][kv][0:1], (16, hd))
            out[0, 0, self.seq:self.seq + 16, :] = jnp.where(row16 == 0, new, 0.0).astype(jnp.bfloat16)
            out[0, 0, self.seq + 16:self.slots, :] = jnp.zeros((self.slots - self.seq - 16, hd), jnp.bfloat16)

        for la in range(2):
            for dst, i in peers():
                q_send(la, dst, i).wait_send()
                y_send(la, dst, i).wait_send()
        for dst, i in peers():
            p_send(1, dst, i).wait_send()

        @pl.when(has_loc)
        def _():
            for dst, i in peers():
                p_send(0, dst, i).wait_send()
            for kv in range(2):
                loc_send(kv, mate, d_sem.at[1, kv]).wait_send()
                own_loc[kv].wait()

        for kv in range(2):
            glo_send(kv, mate, d_sem.at[0, kv]).wait_send()
            own_glo[kv].wait()

        def glo_arrival(kv, src_dev):
            src, out = glo_pairs[kv]
            return pltpu.make_async_remote_copy(src_ref=src.at[0, 0], dst_ref=glo_dst(out, src_dev), send_sem=d_sem.at[0, kv],
                                                recv_sem=glo_rsem.at[kv, src_dev], device_id={"a": src_dev}, device_id_type=MESH)

        def loc_arrival(kv, src_dev):
            src, out = loc_pairs[kv]
            return pltpu.make_async_remote_copy(src_ref=src.at[0, 0], dst_ref=loc_dst(out, src_dev), send_sem=d_sem.at[1, kv],
                                                recv_sem=loc_rsem.at[kv, src_dev], device_id={"a": src_dev}, device_id_type=MESH)

        for src_dev, i in peers():
            @pl.when(src_dev >= self.first_src)
            def _():
                for kv in range(2):
                    loc_arrival(kv, src_dev).wait_recv()
        slot = (self.seq % WINDOW) // 16 * 16
        for kv, out in enumerate((lk_out, lv_out)):
            new = jnp.broadcast_to(fresh[0][kv][0:1], (16, hd))
            old = out[0, 0, slot:slot + 16, :].astype(jnp.float32)
            out[0, 0, slot:slot + 16, :] = jnp.where(row16 == self.seq % WINDOW - slot, new, old).astype(jnp.bfloat16)

        bulk_wait(6)
        bulk_wait(7)
        for src_dev, i in peers():
            for kv in range(2):
                glo_arrival(kv, src_dev).wait_recv()


def solution(mesh):
    n = mesh.shape["a"]
    cache_in = P("dp", None, "a", None)
    cache_out = P("dp", "a", None, None)
    rows_spec = P("dp", None)
    layer_specs = (P(None, "a"), P(None, "a"), P(None, "a"), P("a", None), P(None), P(None))
    in_specs = (rows_spec, cache_in, cache_in, cache_in, cache_in) + layer_specs + layer_specs
    out_specs = (rows_spec, cache_out, cache_out, cache_out, cache_out)

    def device_step(hidden_in, loc_k, loc_v, glo_k, glo_v, loc_wq, loc_wk, loc_wv, loc_wo, loc_pre, loc_post, glo_wq, glo_wk, glo_wv, glo_wo, glo_pre, glo_post):
        d_model = hidden_in.shape[1]
        rows, heads, blk, hd = loc_k.shape
        q_cols, kv_cols = loc_wq.shape[1], loc_wk.shape[1]
        seq = n * blk
        slots = seq + CACHE_ROOM
        table = jnp.asarray(np.stack(rope_tables(hd, seq)))

        vmem = pl.BlockSpec(memory_space=pltpu.VMEM)
        hbm = pl.BlockSpec(memory_space=pltpu.HBM)
        bf16, f32 = jnp.bfloat16, jnp.float32
        dma = pltpu.SemaphoreType.DMA
        landed = pl.pallas_call(
            Kernel(n, d_model, heads, blk, hd, slots),
            name="decode_step",
            out_shape=(
                pltpu.VMEM(hidden_in.shape, bf16),
                pltpu.VMEM((rows, 1, WINDOW, hd), bf16),
                pltpu.VMEM((rows, 1, WINDOW, hd), bf16),
                pltpu.VMEM((rows, 1, slots, hd), bf16),
                pltpu.VMEM((rows, 1, slots, hd), bf16),
            ),
            in_specs=[hbm] * 18,
            out_specs=(vmem,) * 5,
            scratch_shapes=[
                pltpu.VMEM(hidden_in.shape, bf16),
                pltpu.VMEM((2, hd // 2), f32),
                [pltpu.VMEM((d_model,), bf16)] * 4,
                pltpu.VMEM((2, d_model, q_cols), bf16),
                pltpu.VMEM((2, d_model, kv_cols), bf16),
                pltpu.VMEM((2, d_model, kv_cols), bf16),
                pltpu.VMEM((2, q_cols, d_model), bf16),
                pltpu.VMEM((2, 2, heads, blk, hd), bf16),
                pltpu.VMEM((2, 2, hd), f32),
                pltpu.VMEM((2, n, 2, hd), f32),
                pltpu.VMEM((2, n, 2, hd + 128), f32),
                pltpu.VMEM((2, n, 2, hd + 128), f32),
                pltpu.VMEM((2, n, 8, ROW), bf16),
                dma((6,)), dma((8, 2)), dma((4, 2)), dma((2, 2)), dma((2, 2)), dma((2, n)), dma((2, n)), dma((2, 4)), dma((2, 2)),
                dma((2, n - 1)), dma((2, n)), dma((2, n - 1)), dma((2, n)), dma((2, n - 1)), dma((2, n)),
            ],
            compiler_params=pltpu.CompilerParams(collective_id=0, has_side_effects=True, vmem_limit_bytes=48 * 2**20),
        )(hidden_in, table, loc_k, loc_v, glo_k, glo_v, loc_wq, loc_wk, loc_wv, loc_wo, loc_pre, loc_post, glo_wq, glo_wk, glo_wv, glo_wo, glo_pre, glo_post)
        return pl.pallas_call(
            store_outputs,
            name="store_outputs",
            out_shape=tuple(jax.ShapeDtypeStruct(x.shape, x.dtype) for x in landed),
            in_specs=[vmem] * 5,
            out_specs=(hbm,) * 5,
            scratch_shapes=[dma((5, STORE_PARTS))],
            compiler_params=pltpu.CompilerParams(vmem_limit_bytes=2**20),
        )(*landed)

    return jax.shard_map(device_step, mesh=mesh, in_specs=in_specs, out_specs=out_specs, check_vma=False)
```

```python
import functools

import jax
import jax.numpy as jnp
import numpy as np
from jax import lax
from jax.experimental import pallas as pl
from jax.experimental.pallas import tpu as pltpu
from jax.sharding import PartitionSpec as P

SOFTCAP = 50.0
NORM_EPS = 1e-6
ROPE_BASE = 10000.0
WINDOW = 4096
CACHE_ROOM = 512
MESH = pl.DeviceIdType.MESH
CORES = 2
ROW = 512
STORE_PARTS = 2
RELAY = 96
NEG = -1e30


def rope_tables(head_dim, position):
    half = head_dim // 2
    inv = np.float32(ROPE_BASE) ** (np.float32(-2.0) * np.arange(half, dtype=np.float32) / np.float32(head_dim))
    ang = np.float32(position) * inv.astype(np.float32)
    return np.cos(ang).astype(np.float32), np.sin(ang).astype(np.float32)


def softcap(scores, scale):
    return SOFTCAP * jnp.tanh(scores * scale / SOFTCAP)


def rows_like(width):
    return lax.broadcasted_iota(jnp.int32, (8, width), 0)


def store_outputs(*refs):
    landed, outs, sem = refs[:5], refs[5:10], refs[10]
    copies = [pltpu.make_async_copy(landed[0], outs[0], sem.at[0, 0])]
    for j in range(1, 5):
        part = landed[j].shape[2] // STORE_PARTS
        for p in range(STORE_PARTS):
            rows = pl.ds(p * part, part)
            copies.append(pltpu.make_async_copy(landed[j].at[0, 0, rows], outs[j].at[0, 0, rows], sem.at[j, p]))
    for cp in copies:
        cp.start()
    for cp in copies:
        cp.wait()


class Kernel:
    def __init__(self, n, d_model, heads, blk, hd, slots):
        self.n, self.d_model, self.heads, self.blk, self.hd, self.slots = n, d_model, heads, blk, hd, slots
        self.seq = n * blk
        self.first_pos = self.seq - WINDOW + 1
        self.first_src = self.first_pos // blk
        self.chunks = d_model // ROW
        self.q_groups = 2

    def __call__(self, hid_in, table_in, loc_k, loc_v, glo_k, glo_v, lwq, lwk, lwv, lwo, lpre, lpost, gwq, gwk, gwv, gwo, gpre, gpost,
                 hid_out, lk_out, lv_out, gk_out, gv_out,
                 hid_b, table, gain_b, wq_b, wk_b, wv_b, wo_b, kv_b, q_msg, q_all, p_msg, p_all, y_part, y_mate, y_chip, y_half, relay_b,
                 in_sem, f_sem, g_sem, d_sem, own_sem, glo_rsem, loc_rsem, w_sem, kv_sem,
                 qs_sem, qr_sem, ps_sem, pr_sem, m_sem, ys_sem, yr_sem, h_sem, r_sem):
        n, blk, hd = self.n, self.blk, self.hd
        half = hd // 2
        me = lax.axis_index("a")
        chips = n // CORES
        chip, core = me // CORES, lax.rem(me, CORES)
        has_loc = me >= self.first_src
        right, left, opp = [lax.rem(chip + i, chips) for i in (1, chips - 1, chips // 2)]
        even = lax.rem(chip, 2) == 0
        near_f = jnp.where(even, right, left)
        near_g = jnp.where(even, left, right)

        barrier = pltpu.get_barrier_semaphore()
        for i in range(1, n):
            pl.semaphore_signal(barrier, inc=1, device_id={"a": lax.rem(me + i, n)}, device_id_type=MESH)

        weights = [((lwq, gwq), wq_b), ((lwk, gwk), wk_b), ((lwv, gwv), wv_b), ((lwo, gwo), wo_b)]
        w_cp = [[pltpu.make_async_copy(srcs[la], dst.at[la], w_sem.at[la, j]) for j, (srcs, dst) in enumerate(weights)] for la in range(2)]
        kv_cp = [[pltpu.make_async_copy(src.at[0], kv_b.at[la, j], kv_sem.at[la, j]) for j, src in enumerate(pair)]
                 for la, pair in enumerate(((loc_k, loc_v), (glo_k, glo_v)))]
        glo_pairs = ((glo_k, gk_out), (glo_v, gv_out))
        loc_pairs = ((loc_k, lk_out), (loc_v, lv_out))

        def glo_dst(out, src_dev):
            return out.at[0, 0, pl.ds(pl.multiple_of(src_dev * blk, blk), blk)]

        def loc_dst(out, src_dev, lo=0):
            if lo == 0:
                return out.at[0, 0, pl.ds(pl.multiple_of(lax.rem(src_dev * blk, WINDOW), blk), blk)]
            return out.at[0, 0, pl.ds(pl.multiple_of(lax.rem(src_dev * blk, WINDOW) + lo, 32), blk - lo)]

        in_cp = [pltpu.make_async_copy(hid_in, hid_b, in_sem.at[0]), pltpu.make_async_copy(table_in, table, in_sem.at[1])]
        in_cp += [pltpu.make_async_copy(g, b, in_sem.at[2 + j]) for j, (g, b) in enumerate(zip((lpre, lpost, gpre, gpost), gain_b))]
        for cp in in_cp + w_cp[0][:3]:
            cp.start()

        @pl.when(has_loc)
        def _():
            for cp in kv_cp[0]:
                cp.start()

        w_cp[0][3].start()

        pl.semaphore_wait(barrier, n - 1)

        def glo_send(kv, dst, sem):
            src, out = glo_pairs[kv]
            return pltpu.make_async_remote_copy(src_ref=src.at[0, dst], dst_ref=glo_dst(out, me), send_sem=sem,
                                                recv_sem=glo_rsem.at[kv, me], device_id={"a": dst}, device_id_type=MESH)

        def loc_send(kv, dst, sem, lo=0):
            src, out = loc_pairs[kv]
            return pltpu.make_async_remote_copy(src_ref=src.at[0, dst, lo:], dst_ref=loc_dst(out, me, lo), send_sem=sem,
                                                recv_sem=loc_rsem.at[kv, me], device_id={"a": dst}, device_id_type=MESH)

        relay_from, relay_via = chips // 2, chips // 2 - 1
        relay_to = (relay_from + chips // 2) % chips

        def relay_send():
            dst = relay_to * CORES + (CORES - 1 - core)
            return pltpu.make_async_remote_copy(src_ref=loc_v.at[0, dst, pl.ds(0, RELAY)], dst_ref=relay_b, send_sem=r_sem.at[0],
                                                recv_sem=r_sem.at[1], device_id={"a": relay_via * CORES + core}, device_id_type=MESH)

        def relay_forward(src_core, dst_core):
            src_dev = relay_from * CORES + src_core
            dst_ref = lv_out.at[0, 0, pl.ds(pl.multiple_of(lax.rem(src_dev * blk, WINDOW), blk), RELAY)]
            return pltpu.make_async_remote_copy(src_ref=relay_b, dst_ref=dst_ref, send_sem=r_sem.at[2],
                                                recv_sem=r_sem.at[3], device_id={"a": relay_to * CORES + dst_core}, device_id_type=MESH)

        steps = 8

        def step_items(step):
            part = step % steps // 2
            kv, peer = part % 2, lax.rem(core + part // 2, CORES)
            if step >= steps:
                return kv, [(opp * CORES + peer, f_sem.at[step])]
            return kv, [(near_f * CORES + peer, f_sem.at[step]), (near_g * CORES + peer, g_sem.at[step])]

        def bulk(step, act):
            kv, items = step_items(step)
            if step % 2 == 0:
                for dst, sem in items:
                    act(glo_send(kv, dst, sem))
            elif step == 2 * steps - 1:
                (dst, sem), = items

                @pl.when(chip == relay_from)
                def _():
                    act(loc_send(kv, dst, sem, RELAY))

                @pl.when(jnp.logical_and(has_loc, chip != relay_from))
                def _():
                    act(loc_send(kv, dst, sem))
            else:
                @pl.when(has_loc)
                def _():
                    for dst, sem in items:
                        act(loc_send(kv, dst, sem))

        def bulk_start(step):
            bulk(step, lambda cp: cp.start())

        def bulk_wait(step):
            bulk(step, lambda cp: cp.wait_send())

        @pl.when(chip == relay_from)
        def _():
            relay_send().start()

        bulk_start(0)
        mate = chip * CORES + (CORES - 1 - core)
        own_glo = [pltpu.make_async_copy(src.at[0, me], glo_dst(out, me), own_sem.at[0, kv]) for kv, (src, out) in enumerate(glo_pairs)]
        own_loc = [pltpu.make_async_copy(src.at[0, me], loc_dst(out, me), own_sem.at[1, kv]) for kv, (src, out) in enumerate(loc_pairs)]
        for kv in range(2):
            glo_send(kv, mate, d_sem.at[0, kv]).start()
            own_glo[kv].start()

        @pl.when(has_loc)
        def _():
            for kv in range(2):
                loc_send(kv, mate, d_sem.at[1, kv]).start()
                own_loc[kv].start()

        for cp in in_cp:
            cp.wait()

        def q_send(la, dst, i):
            return pltpu.make_async_remote_copy(src_ref=q_msg.at[la], dst_ref=q_all.at[la, me], send_sem=qs_sem.at[la, i - 1],
                                                recv_sem=qr_sem.at[la, me], device_id={"a": dst}, device_id_type=MESH)

        def p_send(la, dst, i):
            return pltpu.make_async_remote_copy(src_ref=p_msg.at[la, dst], dst_ref=p_all.at[la, me], send_sem=ps_sem.at[la, i - 1],
                                                recv_sem=pr_sem.at[la, me], device_id={"a": dst}, device_id_type=MESH)

        def mate_send(la):
            return pltpu.make_async_remote_copy(src_ref=y_part.at[la, 1 - core], dst_ref=y_mate.at[la], send_sem=m_sem.at[la, 0],
                                                recv_sem=m_sem.at[la, 1], device_id={"a": mate}, device_id_type=MESH)

        def chip_copy(la, other, slot, i):
            return pltpu.make_async_remote_copy(src_ref=y_chip.at[la, slot], dst_ref=y_chip.at[la, slot], send_sem=ys_sem.at[la, i],
                                                recv_sem=yr_sem.at[la, slot], device_id={"a": other * CORES + core}, device_id_type=MESH)

        def half_copy(la, slot):
            return pltpu.make_async_remote_copy(src_ref=y_half.at[la, slot], dst_ref=y_half.at[la, slot], send_sem=h_sem.at[la, 0],
                                                recv_sem=h_sem.at[la, 1], device_id={"a": mate}, device_id_type=MESH)

        others = [(lax.rem(chip + i, chips), i - 1) for i in range(1, chips)]

        def q_arrival(la, src):
            return pltpu.make_async_remote_copy(src_ref=q_msg.at[la], dst_ref=q_all.at[la, src], send_sem=qs_sem.at[la, 0],
                                                recv_sem=qr_sem.at[la, src], device_id={"a": src}, device_id_type=MESH)

        def p_arrival(la, src):
            return pltpu.make_async_remote_copy(src_ref=p_msg.at[la, 0], dst_ref=p_all.at[la, src], send_sem=ps_sem.at[la, 0],
                                                recv_sem=pr_sem.at[la, src], device_id={"a": src}, device_id_type=MESH)

        def peers():
            return [(lax.rem(me + i, n), i) for i in range(1, n)]

        def norm(x):
            total = jnp.sum(jnp.sum(x * x, axis=1, keepdims=True), axis=0, keepdims=True)
            return x * lax.rsqrt(total / self.d_model + NORM_EPS)

        cosine, sine = table[0:1, :], table[1:2, :]

        def tiled(piece):
            row = rows_like(ROW)
            out = jnp.zeros((8, ROW), jnp.float32)
            for i in range(self.chunks):
                out = jnp.where(row == i, piece(i), out)
            return out

        def gain(j):
            return tiled(lambda i: gain_b[j][i * ROW:(i + 1) * ROW].astype(jnp.float32).reshape(1, ROW))

        def rope(x):
            first, second = x[:, :half], x[:, half:]
            return jnp.concatenate([first * cosine - second * sine, second * cosine + first * sine], axis=1)

        def round_bf16(x):
            return x.astype(jnp.bfloat16).astype(jnp.float32)

        def project(la, hidden, pre):
            a = norm(hidden) * (1.0 + pre)
            for j in range(3):
                w_cp[la][j].wait()
            q = k = v = None
            for i in range(self.chunks):
                lhs = jnp.broadcast_to(a[i:i + 1, :], (16, ROW)).astype(jnp.bfloat16)
                part = [jnp.dot(lhs, w[la, i * ROW:(i + 1) * ROW, :], preferred_element_type=jnp.float32) for w in (wq_b, wk_b, wv_b)]
                q, k, v = part if q is None else (q + part[0], k + part[1], v + part[2])
            q, k, v = q[:2], k[:2], v[:2]
            q0, q1 = rope(q[:, :hd]), rope(q[:, hd:])
            q = round_bf16(jnp.where(lax.broadcasted_iota(jnp.int32, (2, hd), 0) == 0, q0, q1))
            return q, round_bf16(rope(k)), round_bf16(v)

        def attend_block(la, h, masked):
            q = q_all[la, h].astype(jnp.bfloat16)
            s = lax.dot_general(q, kv_b[la, 0, h], (((1,), (1,)), ((), ())), preferred_element_type=jnp.float32)
            s = softcap(s, hd ** -0.5)
            if masked:
                pos = me * blk + lax.broadcasted_iota(jnp.int32, s.shape, 1)
                s = jnp.where(pos >= self.first_pos, s, NEG)
            top = jnp.max(s, axis=1, keepdims=True)
            e = jnp.exp(s - top)
            if masked:
                e = jnp.where(pos >= self.first_pos, e, 0.0)
            total = jnp.sum(e, axis=1, keepdims=True)
            o = jnp.dot(e.astype(jnp.bfloat16), kv_b[la, 1, h], preferred_element_type=jnp.float32)
            lane = lax.broadcasted_iota(jnp.int32, (2, 128), 1)
            p_msg[la, h, :, 0:hd] = o
            p_msg[la, h, :, hd:hd + 128] = jnp.where(lane < 64, top, total)

        def attend_all(la, masked):
            for cp in kv_cp[la]:
                cp.wait()

            def body(h, carry):
                attend_block(la, h, masked)
                return carry

            lax.fori_loop(0, n, body, 0)
            for dst, i in peers():
                p_send(la, dst, i).start()
            p_all[la, me] = p_msg[la, me]

        def combine(la, q, k_new, v_new, first_src):
            s_new = softcap(jnp.sum(q * k_new, axis=1, keepdims=True), hd ** -0.5)
            tops = [p_all[la, s, :, hd:hd + 1] for s in range(first_src, n)]
            sums = [p_all[la, s, :, hd + 64:hd + 65] for s in range(first_src, n)]
            top = s_new
            for t in tops:
                top = jnp.maximum(top, t)
            e_new = jnp.exp(s_new - top)
            denom = e_new
            o = round_bf16(e_new) * v_new
            for idx, s in enumerate(range(first_src, n)):
                w = jnp.exp(tops[idx] - top)
                denom = denom + w * sums[idx]
                o = o + w * p_all[la, s, :, 0:hd]
            return o / denom

        def out_project(la, o):
            w_cp[la][3].wait()
            lhs = [jnp.broadcast_to(o[g:g + 1, :], (16, hd)).astype(jnp.bfloat16) for g in range(self.q_groups)]
            row = rows_like(ROW)
            msg = jnp.zeros((8, ROW), jnp.float32)
            for i in range(self.chunks):
                y = None
                for g in range(self.q_groups):
                    part = jnp.dot(lhs[g], wo_b[la, g * hd:(g + 1) * hd, i * ROW:(i + 1) * ROW], preferred_element_type=jnp.float32)
                    y = part if y is None else y + part
                msg = jnp.where(row == i, y[:8], msg)
            y_part[la, 0] = msg[:4]
            y_part[la, 1] = msg[4:]
            mate_send(la).start()
            mate_send(la).wait_recv()
            y_chip[la, chip] = y_part[la, core] + y_mate[la]
            for other, i in others:
                chip_copy(la, other, chip, i).start()

        hidden = tiled(lambda i: hid_b[:, i * ROW:(i + 1) * ROW].astype(jnp.float32))
        fresh = []
        for la in range(2):
            pre, post = gain(2 * la), gain(2 * la + 1)
            q, k_new, v_new = project(la, hidden, pre)
            fresh.append((k_new, v_new))
            q_msg[la] = q
            q_all[la, me] = q
            for dst, i in peers():
                @pl.when(jnp.logical_or(la == 1, dst >= self.first_src))
                def _():
                    q_send(la, dst, i).start()
            step = 3 * la + 1
            bulk_start(step)
            bulk_wait(step - 1)
            if la == 0:
                for cp in w_cp[1] + kv_cp[1]:
                    cp.start()
            if la == 0:
                @pl.when(has_loc)
                def _():
                    for src, i in peers():
                        q_arrival(0, src).wait_recv()
                    attend_all(0, True)
            else:
                for src, i in peers():
                    q_arrival(1, src).wait_recv()
                attend_all(1, False)
            bulk_start(step + 1)
            bulk_wait(step)
            first_src = self.first_src if la == 0 else 0
            for src, i in peers():
                if la == 0:
                    @pl.when(src >= first_src)
                    def _():
                        p_arrival(0, src).wait_recv()
                else:
                    p_arrival(la, src).wait_recv()
            out_project(la, combine(la, q, k_new, v_new, first_src))
            bulk_start(step + 2)
            bulk_wait(step + 1)
            for other, i in others:
                chip_copy(la, other, other, i).wait_recv()
            total = y_chip[la, 0]
            for c in range(1, chips):
                total = total + y_chip[la, c]
            y_half[la, core] = total
            half_copy(la, core).start()
            half_copy(la, 1 - core).wait_recv()
            y = jnp.concatenate([y_half[la, 0], y_half[la, 1]], axis=0)
            hidden = round_bf16(hidden + norm(y) * (1.0 + post))
        for i in range(self.chunks):
            hid_out[:, i * ROW:(i + 1) * ROW] = hidden[i:i + 1, :].astype(jnp.bfloat16)

        for step in range(7, 2 * steps):
            bulk_start(step)

        @pl.when(chip == relay_via)
        def _():
            relay_send().wait_recv()
            relay_forward(core, CORES - 1 - core).start()

        row16 = lax.broadcasted_iota(jnp.int32, (16, hd), 0)
        for kv, out in enumerate((gk_out, gv_out)):
            new = jnp.broadcast_to(fresh[1][kv][0:1], (16, hd))
            out[0, 0, self.seq:self.seq + 16, :] = jnp.where(row16 == 0, new, 0.0).astype(jnp.bfloat16)
            out[0, 0, self.seq + 16:self.slots, :] = jnp.zeros((self.slots - self.seq - 16, hd), jnp.bfloat16)

        for la in range(2):
            for dst, i in peers():
                @pl.when(jnp.logical_or(la == 1, dst >= self.first_src))
                def _():
                    q_send(la, dst, i).wait_send()
            mate_send(la).wait_send()
            for other, i in others:
                chip_copy(la, other, chip, i).wait_send()
            half_copy(la, core).wait_send()
        for dst, i in peers():
            p_send(1, dst, i).wait_send()

        @pl.when(has_loc)
        def _():
            for dst, i in peers():
                p_send(0, dst, i).wait_send()
            for kv in range(2):
                loc_send(kv, mate, d_sem.at[1, kv]).wait_send()
                own_loc[kv].wait()

        for kv in range(2):
            glo_send(kv, mate, d_sem.at[0, kv]).wait_send()
            own_glo[kv].wait()

        def glo_arrival(kv, src_dev):
            src, out = glo_pairs[kv]
            return pltpu.make_async_remote_copy(src_ref=src.at[0, 0], dst_ref=glo_dst(out, src_dev), send_sem=d_sem.at[0, kv],
                                                recv_sem=glo_rsem.at[kv, src_dev], device_id={"a": src_dev}, device_id_type=MESH)

        def loc_arrival(kv, src_dev, lo=0):
            src, out = loc_pairs[kv]
            return pltpu.make_async_remote_copy(src_ref=src.at[0, 0, lo:], dst_ref=loc_dst(out, src_dev, lo), send_sem=d_sem.at[1, kv],
                                                recv_sem=loc_rsem.at[kv, src_dev], device_id={"a": src_dev}, device_id_type=MESH)

        for src_dev, i in peers():
            short = jnp.logical_and(chip == relay_to, src_dev == relay_from * CORES + (CORES - 1 - core))

            @pl.when(src_dev >= self.first_src)
            def _():
                loc_arrival(0, src_dev).wait_recv()

            @pl.when(jnp.logical_and(src_dev >= self.first_src, jnp.logical_not(short)))
            def _():
                loc_arrival(1, src_dev).wait_recv()

            @pl.when(short)
            def _():
                loc_arrival(1, src_dev, RELAY).wait_recv()

        @pl.when(chip == relay_from)
        def _():
            relay_send().wait_send()

        @pl.when(chip == relay_via)
        def _():
            relay_forward(core, CORES - 1 - core).wait_send()

        @pl.when(chip == relay_to)
        def _():
            relay_forward(CORES - 1 - core, core).wait_recv()

        slot = (self.seq % WINDOW) // 16 * 16
        for kv, out in enumerate((lk_out, lv_out)):
            new = jnp.broadcast_to(fresh[0][kv][0:1], (16, hd))
            old = out[0, 0, slot:slot + 16, :].astype(jnp.float32)
            out[0, 0, slot:slot + 16, :] = jnp.where(row16 == self.seq % WINDOW - slot, new, old).astype(jnp.bfloat16)

        for step in range(6, 2 * steps):
            bulk_wait(step)
        for src_dev, i in peers():
            for kv in range(2):
                glo_arrival(kv, src_dev).wait_recv()


def solution(mesh):
    n = mesh.shape["a"]
    cache_in = P("dp", None, "a", None)
    cache_out = P("dp", "a", None, None)
    rows_spec = P("dp", None)
    layer_specs = (P(None, "a"), P(None, "a"), P(None, "a"), P("a", None), P(None), P(None))
    in_specs = (rows_spec, cache_in, cache_in, cache_in, cache_in) + layer_specs + layer_specs
    out_specs = (rows_spec, cache_out, cache_out, cache_out, cache_out)

    def device_step(hidden_in, loc_k, loc_v, glo_k, glo_v, loc_wq, loc_wk, loc_wv, loc_wo, loc_pre, loc_post, glo_wq, glo_wk, glo_wv, glo_wo, glo_pre, glo_post):
        d_model = hidden_in.shape[1]
        rows, heads, blk, hd = loc_k.shape
        q_cols, kv_cols = loc_wq.shape[1], loc_wk.shape[1]
        seq = n * blk
        slots = seq + CACHE_ROOM
        table = jnp.asarray(np.stack(rope_tables(hd, seq)))

        vmem = pl.BlockSpec(memory_space=pltpu.VMEM)
        hbm = pl.BlockSpec(memory_space=pltpu.HBM)
        bf16, f32 = jnp.bfloat16, jnp.float32
        dma = pltpu.SemaphoreType.DMA
        landed = pl.pallas_call(
            Kernel(n, d_model, heads, blk, hd, slots),
            name="decode_step",
            out_shape=(
                pltpu.VMEM(hidden_in.shape, bf16),
                pltpu.VMEM((rows, 1, WINDOW, hd), bf16),
                pltpu.VMEM((rows, 1, WINDOW, hd), bf16),
                pltpu.VMEM((rows, 1, slots, hd), bf16),
                pltpu.VMEM((rows, 1, slots, hd), bf16),
            ),
            in_specs=[hbm] * 18,
            out_specs=(vmem,) * 5,
            scratch_shapes=[
                pltpu.VMEM(hidden_in.shape, bf16),
                pltpu.VMEM((2, hd // 2), f32),
                [pltpu.VMEM((d_model,), bf16)] * 4,
                pltpu.VMEM((2, d_model, q_cols), bf16),
                pltpu.VMEM((2, d_model, kv_cols), bf16),
                pltpu.VMEM((2, d_model, kv_cols), bf16),
                pltpu.VMEM((2, q_cols, d_model), bf16),
                pltpu.VMEM((2, 2, heads, blk, hd), bf16),
                pltpu.VMEM((2, 2, hd), f32),
                pltpu.VMEM((2, n, 2, hd), f32),
                pltpu.VMEM((2, n, 2, hd + 128), f32),
                pltpu.VMEM((2, n, 2, hd + 128), f32),
                pltpu.VMEM((2, CORES, 4, ROW), f32),
                pltpu.VMEM((2, 4, ROW), f32),
                pltpu.VMEM((2, n // CORES, 4, ROW), f32),
                pltpu.VMEM((2, CORES, 4, ROW), f32),
                pltpu.VMEM((RELAY, hd), bf16),
                dma((6,)), dma((16,)), dma((8,)), dma((2, 2)), dma((2, 2)), dma((2, n)), dma((2, n)), dma((2, 4)), dma((2, 2)),
                dma((2, n - 1)), dma((2, n)), dma((2, n - 1)), dma((2, n)), dma((2, 2)), dma((2, 3)), dma((2, n // CORES)), dma((2, 2)), dma((4,)),
            ],
            compiler_params=pltpu.CompilerParams(collective_id=0, has_side_effects=True, vmem_limit_bytes=48 * 2**20),
        )(hidden_in, table, loc_k, loc_v, glo_k, glo_v, loc_wq, loc_wk, loc_wv, loc_wo, loc_pre, loc_post, glo_wq, glo_wk, glo_wv, glo_wo, glo_pre, glo_post)
        return pl.pallas_call(
            store_outputs,
            name="store_outputs",
            out_shape=tuple(jax.ShapeDtypeStruct(x.shape, x.dtype) for x in landed),
            in_specs=[vmem] * 5,
            out_specs=(hbm,) * 5,
            scratch_shapes=[dma((5, STORE_PARTS))],
            compiler_params=pltpu.CompilerParams(vmem_limit_bytes=2**20),
        )(*landed)

    return jax.shard_map(device_step, mesh=mesh, in_specs=in_specs, out_specs=out_specs, check_vma=False)
```

```python
import functools

import jax
import jax.numpy as jnp
import numpy as np
from jax import lax
from jax.experimental import pallas as pl
from jax.experimental.pallas import tpu as pltpu
from jax.sharding import PartitionSpec as P

SOFTCAP = 50.0
NORM_EPS = 1e-6
ROPE_BASE = 10000.0
WINDOW = 4096
CACHE_ROOM = 512
MESH = pl.DeviceIdType.MESH
CORES = 2
ROW = 512
STORE_PARTS = 2
RELAY = 128
HOLD = 1
NEG = -1e30


def rope_tables(head_dim, position):
    half = head_dim // 2
    inv = np.float32(ROPE_BASE) ** (np.float32(-2.0) * np.arange(half, dtype=np.float32) / np.float32(head_dim))
    ang = np.float32(position) * inv.astype(np.float32)
    return np.cos(ang).astype(np.float32), np.sin(ang).astype(np.float32)


def softcap(scores, scale):
    return SOFTCAP * jnp.tanh(scores * scale / SOFTCAP)


def rows_like(width):
    return lax.broadcasted_iota(jnp.int32, (8, width), 0)


def store_outputs(*refs):
    landed, outs, sem = refs[:5], refs[5:10], refs[10]
    copies = [pltpu.make_async_copy(landed[0], outs[0], sem.at[0, 0])]
    for j in range(1, 5):
        part = landed[j].shape[2] // STORE_PARTS
        for p in range(STORE_PARTS):
            rows = pl.ds(p * part, part)
            copies.append(pltpu.make_async_copy(landed[j].at[0, 0, rows], outs[j].at[0, 0, rows], sem.at[j, p]))
    for cp in copies:
        cp.start()
    for cp in copies:
        cp.wait()


class Kernel:
    def __init__(self, n, d_model, heads, blk, hd, slots):
        self.n, self.d_model, self.heads, self.blk, self.hd, self.slots = n, d_model, heads, blk, hd, slots
        self.seq = n * blk
        self.first_pos = self.seq - WINDOW + 1
        self.first_src = self.first_pos // blk
        self.chunks = d_model // ROW
        self.q_groups = 2

    def __call__(self, hid_in, table_in, loc_k, loc_v, glo_k, glo_v, lwq, lwk, lwv, lwo, lpre, lpost, gwq, gwk, gwv, gwo, gpre, gpost,
                 hid_out, lk_out, lv_out, gk_out, gv_out,
                 hid_b, table, gain_b, wq_b, wk_b, wv_b, wo_b, kv_b, q_msg, q_all, p_msg, p_all, y_part, y_mate, y_chip, y_half, relay_b,
                 in_sem, f_sem, g_sem, d_sem, own_sem, glo_rsem, loc_rsem, w_sem, kv_sem,
                 qs_sem, qr_sem, ps_sem, pr_sem, m_sem, ys_sem, yr_sem, h_sem, r_sem, go_sem):
        n, blk, hd = self.n, self.blk, self.hd
        half = hd // 2
        me = lax.axis_index("a")
        chips = n // CORES
        chip, core = me // CORES, lax.rem(me, CORES)
        has_loc = me >= self.first_src
        right, left, opp = [lax.rem(chip + i, chips) for i in (1, chips - 1, chips // 2)]
        even = lax.rem(chip, 2) == 0
        near_f = jnp.where(even, right, left)
        near_g = jnp.where(even, left, right)

        mate = chip * CORES + (CORES - 1 - core)

        relay_from, relay_via = chips // 2, chips // 2 - 1
        relay_to = (relay_from + chips // 2) % chips

        barrier = pltpu.get_barrier_semaphore()

        def greet(devices):
            for dev in devices:
                pl.semaphore_signal(barrier, inc=1, device_id={"a": dev}, device_id_type=MESH)

        def cores_of(c):
            return [c * CORES + j for j in range(CORES)]

        def tell(c):
            pl.semaphore_signal(go_sem, inc=1, device_id={"a": c * CORES + core}, device_id_type=MESH)

        late = chips - 1
        early_devices = list(range(self.first_src))

        @pl.when(jnp.logical_not(has_loc))
        def _():
            greet([mate] + cores_of(near_f) + cores_of(near_g))

        @pl.when(chip == late)
        def _():
            greet([mate] + early_devices)

        weights = [((lwq, gwq), wq_b), ((lwk, gwk), wk_b), ((lwv, gwv), wv_b), ((lwo, gwo), wo_b)]
        w_cp = [[pltpu.make_async_copy(srcs[la], dst.at[la], w_sem.at[la, j]) for j, (srcs, dst) in enumerate(weights)] for la in range(2)]
        kv_cp = [[pltpu.make_async_copy(src.at[0], kv_b.at[la, j], kv_sem.at[la, j]) for j, src in enumerate(pair)]
                 for la, pair in enumerate(((loc_k, loc_v), (glo_k, glo_v)))]
        glo_pairs = ((glo_k, gk_out), (glo_v, gv_out))
        loc_pairs = ((loc_k, lk_out), (loc_v, lv_out))

        def glo_dst(out, src_dev):
            return out.at[0, 0, pl.ds(pl.multiple_of(src_dev * blk, blk), blk)]

        def loc_dst(out, src_dev, lo=0):
            if lo == 0:
                return out.at[0, 0, pl.ds(pl.multiple_of(lax.rem(src_dev * blk, WINDOW), blk), blk)]
            return out.at[0, 0, pl.ds(pl.multiple_of(lax.rem(src_dev * blk, WINDOW) + lo, 16), blk - lo)]

        in_cp = [pltpu.make_async_copy(hid_in, hid_b, in_sem.at[0]), pltpu.make_async_copy(table_in, table, in_sem.at[1])]
        in_cp += [pltpu.make_async_copy(g, b, in_sem.at[2 + j]) for j, (g, b) in enumerate(zip((lpre, lpost, gpre, gpost), gain_b))]
        for cp in in_cp + w_cp[0][:3]:
            cp.start()

        @pl.when(has_loc)
        def _():
            for cp in kv_cp[0]:
                cp.start()

        w_cp[0][3].start()

        @pl.when(jnp.logical_not(has_loc))
        def _():
            pl.semaphore_wait(barrier, n - 1)

        @pl.when(chip == late)
        def _():
            pl.semaphore_wait(barrier, 1 + 2 * CORES)
            tell(relay_from)

        def glo_send(kv, dst, sem):
            src, out = glo_pairs[kv]
            return pltpu.make_async_remote_copy(src_ref=src.at[0, dst], dst_ref=glo_dst(out, me), send_sem=sem,
                                                recv_sem=glo_rsem.at[kv, me], device_id={"a": dst}, device_id_type=MESH)

        def loc_send(kv, dst, sem, lo=0):
            src, out = loc_pairs[kv]
            return pltpu.make_async_remote_copy(src_ref=src.at[0, dst, lo:], dst_ref=loc_dst(out, me, lo), send_sem=sem,
                                                recv_sem=loc_rsem.at[kv, me], device_id={"a": dst}, device_id_type=MESH)

        def relay_send():
            dst = relay_to * CORES + (CORES - 1 - core)
            return pltpu.make_async_remote_copy(src_ref=loc_v.at[0, dst, pl.ds(0, RELAY)], dst_ref=relay_b, send_sem=r_sem.at[0],
                                                recv_sem=r_sem.at[1], device_id={"a": relay_via * CORES + core}, device_id_type=MESH)

        def relay_forward(src_core, dst_core):
            src_dev = relay_from * CORES + src_core
            dst_ref = lv_out.at[0, 0, pl.ds(pl.multiple_of(lax.rem(src_dev * blk, WINDOW), blk), RELAY)]
            return pltpu.make_async_remote_copy(src_ref=relay_b, dst_ref=dst_ref, send_sem=r_sem.at[2],
                                                recv_sem=r_sem.at[3], device_id={"a": relay_to * CORES + dst_core}, device_id_type=MESH)

        steps = 8

        def step_items(step):
            part = step // 2 if step < steps else step % 4
            kv, peer = part % 2, lax.rem(core + part // 2, CORES)
            if step >= steps:
                return kv, [(opp * CORES + peer, f_sem.at[step])]
            return kv, [(near_f * CORES + peer, f_sem.at[step]), (near_g * CORES + peer, g_sem.at[step])]

        def bulk(step, act, sides=slice(None)):
            kv, items = step_items(step)
            items = items[sides]
            if step >= 12 or (step < steps and step % 2 == 0):
                for dst, sem in items:
                    act(glo_send(kv, dst, sem))
            elif step == 11:
                (dst, sem), = items

                @pl.when(chip == relay_from)
                def _():
                    act(loc_send(kv, dst, sem, RELAY))

                @pl.when(jnp.logical_and(has_loc, chip != relay_from))
                def _():
                    act(loc_send(kv, dst, sem))
            else:
                @pl.when(has_loc)
                def _():
                    for dst, sem in items:
                        act(loc_send(kv, dst, sem))

        def bulk_start(step, sides=slice(None)):
            bulk(step, lambda cp: cp.start(), sides)

        def bulk_wait(step):
            bulk(step, lambda cp: cp.wait_send())

        @pl.when(chip == relay_from)
        def _():
            pl.semaphore_wait(barrier, CORES)
            greet(early_devices + cores_of(late))
            relay_send().start()
            bulk_start(0, slice(1, 2))
            pl.semaphore_wait(go_sem, 1)
            bulk_start(0, slice(0, 1))

        @pl.when(chip != relay_from)
        def _():
            bulk_start(0)

        own_glo = [pltpu.make_async_copy(src.at[0, me], glo_dst(out, me), own_sem.at[0, kv]) for kv, (src, out) in enumerate(glo_pairs)]
        own_loc = [pltpu.make_async_copy(src.at[0, me], loc_dst(out, me), own_sem.at[1, kv]) for kv, (src, out) in enumerate(loc_pairs)]
        for kv in range(2):
            glo_send(kv, mate, d_sem.at[0, kv]).start()
            own_glo[kv].start()

        @pl.when(has_loc)
        def _():
            for kv in range(2):
                loc_send(kv, mate, d_sem.at[1, kv]).start()
                own_loc[kv].start()

        for cp in in_cp:
            cp.wait()

        def q_send(la, dst, i):
            return pltpu.make_async_remote_copy(src_ref=q_msg.at[la], dst_ref=q_all.at[la, me], send_sem=qs_sem.at[la, i - 1],
                                                recv_sem=qr_sem.at[la, me], device_id={"a": dst}, device_id_type=MESH)

        def p_send(la, dst, i):
            return pltpu.make_async_remote_copy(src_ref=p_msg.at[la, dst], dst_ref=p_all.at[la, me], send_sem=ps_sem.at[la, i - 1],
                                                recv_sem=pr_sem.at[la, me], device_id={"a": dst}, device_id_type=MESH)

        def mate_send(la):
            return pltpu.make_async_remote_copy(src_ref=y_part.at[la, 1 - core], dst_ref=y_mate.at[la], send_sem=m_sem.at[la, 0],
                                                recv_sem=m_sem.at[la, 1], device_id={"a": mate}, device_id_type=MESH)

        def chip_copy(la, other, slot, i):
            return pltpu.make_async_remote_copy(src_ref=y_chip.at[la, slot], dst_ref=y_chip.at[la, slot], send_sem=ys_sem.at[la, i],
                                                recv_sem=yr_sem.at[la, slot], device_id={"a": other * CORES + core}, device_id_type=MESH)

        def half_copy(la, slot):
            return pltpu.make_async_remote_copy(src_ref=y_half.at[la, slot], dst_ref=y_half.at[la, slot], send_sem=h_sem.at[la, 0],
                                                recv_sem=h_sem.at[la, 1], device_id={"a": mate}, device_id_type=MESH)

        others = [(lax.rem(chip + i, chips), i - 1) for i in range(1, chips)]

        def q_arrival(la, src):
            return pltpu.make_async_remote_copy(src_ref=q_msg.at[la], dst_ref=q_all.at[la, src], send_sem=qs_sem.at[la, 0],
                                                recv_sem=qr_sem.at[la, src], device_id={"a": src}, device_id_type=MESH)

        def p_arrival(la, src):
            return pltpu.make_async_remote_copy(src_ref=p_msg.at[la, 0], dst_ref=p_all.at[la, src], send_sem=ps_sem.at[la, 0],
                                                recv_sem=pr_sem.at[la, src], device_id={"a": src}, device_id_type=MESH)

        def peers():
            return [(lax.rem(me + i, n), i) for i in range(1, n)]

        def norm(x):
            total = jnp.sum(jnp.sum(x * x, axis=1, keepdims=True), axis=0, keepdims=True)
            return x * lax.rsqrt(total / self.d_model + NORM_EPS)

        cosine, sine = table[0:1, :], table[1:2, :]

        def tiled(piece):
            row = rows_like(ROW)
            out = jnp.zeros((8, ROW), jnp.float32)
            for i in range(self.chunks):
                out = jnp.where(row == i, piece(i), out)
            return out

        def gain(j):
            return tiled(lambda i: gain_b[j][i * ROW:(i + 1) * ROW].astype(jnp.float32).reshape(1, ROW))

        def rope(x):
            first, second = x[:, :half], x[:, half:]
            return jnp.concatenate([first * cosine - second * sine, second * cosine + first * sine], axis=1)

        def round_bf16(x):
            return x.astype(jnp.bfloat16).astype(jnp.float32)

        def project(la, hidden, pre):
            a = norm(hidden) * (1.0 + pre)
            for j in range(3):
                w_cp[la][j].wait()
            q = k = v = None
            for i in range(self.chunks):
                lhs = jnp.broadcast_to(a[i:i + 1, :], (16, ROW)).astype(jnp.bfloat16)
                part = [jnp.dot(lhs, w[la, i * ROW:(i + 1) * ROW, :], preferred_element_type=jnp.float32) for w in (wq_b, wk_b, wv_b)]
                q, k, v = part if q is None else (q + part[0], k + part[1], v + part[2])
            q, k, v = q[:2], k[:2], v[:2]
            q0, q1 = rope(q[:, :hd]), rope(q[:, hd:])
            q = round_bf16(jnp.where(lax.broadcasted_iota(jnp.int32, (2, hd), 0) == 0, q0, q1))
            return q, round_bf16(rope(k)), round_bf16(v)

        def attend_block(la, h, masked):
            q = q_all[la, h].astype(jnp.bfloat16)
            s = lax.dot_general(q, kv_b[la, 0, h], (((1,), (1,)), ((), ())), preferred_element_type=jnp.float32)
            s = softcap(s, hd ** -0.5)
            if masked:
                pos = me * blk + lax.broadcasted_iota(jnp.int32, s.shape, 1)
                s = jnp.where(pos >= self.first_pos, s, NEG)
            top = jnp.max(s, axis=1, keepdims=True)
            e = jnp.exp(s - top)
            if masked:
                e = jnp.where(pos >= self.first_pos, e, 0.0)
            total = jnp.sum(e, axis=1, keepdims=True)
            o = jnp.dot(e.astype(jnp.bfloat16), kv_b[la, 1, h], preferred_element_type=jnp.float32)
            lane = lax.broadcasted_iota(jnp.int32, (2, 128), 1)
            p_msg[la, h, :, 0:hd] = o
            p_msg[la, h, :, hd:hd + 128] = jnp.where(lane < 64, top, total)

        def attend_all(la, masked):
            for cp in kv_cp[la]:
                cp.wait()

            def body(h, carry):
                attend_block(la, h, masked)
                return carry

            lax.fori_loop(0, n, body, 0)
            for dst, i in peers():
                p_send(la, dst, i).start()
            p_all[la, me] = p_msg[la, me]

        def combine(la, q, k_new, v_new, first_src):
            s_new = softcap(jnp.sum(q * k_new, axis=1, keepdims=True), hd ** -0.5)
            tops = [p_all[la, s, :, hd:hd + 1] for s in range(first_src, n)]
            sums = [p_all[la, s, :, hd + 64:hd + 65] for s in range(first_src, n)]
            top = s_new
            for t in tops:
                top = jnp.maximum(top, t)
            e_new = jnp.exp(s_new - top)
            denom = e_new
            o = round_bf16(e_new) * v_new
            for idx, s in enumerate(range(first_src, n)):
                w = jnp.exp(tops[idx] - top)
                denom = denom + w * sums[idx]
                o = o + w * p_all[la, s, :, 0:hd]
            return o / denom

        def out_project(la, o):
            w_cp[la][3].wait()
            lhs = [jnp.broadcast_to(o[g:g + 1, :], (16, hd)).astype(jnp.bfloat16) for g in range(self.q_groups)]
            row = rows_like(ROW)
            msg = jnp.zeros((8, ROW), jnp.float32)
            for i in range(self.chunks):
                y = None
                for g in range(self.q_groups):
                    part = jnp.dot(lhs[g], wo_b[la, g * hd:(g + 1) * hd, i * ROW:(i + 1) * ROW], preferred_element_type=jnp.float32)
                    y = part if y is None else y + part
                msg = jnp.where(row == i, y[:8], msg)
            y_part[la, 0] = msg[:4]
            y_part[la, 1] = msg[4:]
            mate_send(la).start()
            mate_send(la).wait_recv()
            y_chip[la, chip] = y_part[la, core] + y_mate[la]
            for other, i in others:
                chip_copy(la, other, chip, i).start()

        hidden = tiled(lambda i: hid_b[:, i * ROW:(i + 1) * ROW].astype(jnp.float32))
        fresh = []
        for la in range(2):
            pre, post = gain(2 * la), gain(2 * la + 1)
            q, k_new, v_new = project(la, hidden, pre)
            fresh.append((k_new, v_new))
            q_msg[la] = q
            q_all[la, me] = q
            for dst, i in peers():
                @pl.when(jnp.logical_or(la == 1, dst >= self.first_src))
                def _():
                    q_send(la, dst, i).start()
            step = 3 * la + 1
            bulk_start(step)
            bulk_wait(step - 1)
            if la == 0:
                for cp in w_cp[1] + kv_cp[1]:
                    cp.start()
            if la == 0:
                @pl.when(has_loc)
                def _():
                    for src, i in peers():
                        q_arrival(0, src).wait_recv()
                    attend_all(0, True)
            else:
                for src, i in peers():
                    q_arrival(1, src).wait_recv()
                attend_all(1, False)
            bulk_start(step + 1)
            bulk_wait(step)
            first_src = self.first_src if la == 0 else 0
            for src, i in peers():
                if la == 0:
                    @pl.when(src >= first_src)
                    def _():
                        p_arrival(0, src).wait_recv()
                else:
                    p_arrival(la, src).wait_recv()
            out_project(la, combine(la, q, k_new, v_new, first_src))
            if la == 0:
                bulk_start(step + 2)
                bulk_wait(step + 1)
            else:
                for later in range(step + 2, steps - HOLD):
                    bulk_start(later)
                for later in range(steps - HOLD, steps):
                    bulk_start(later, slice(1, 2))
                for later in range(steps, 2 * steps):
                    bulk_start(later)
                for later in range(steps - HOLD, steps):
                    bulk_start(later, slice(0, 1))

                @pl.when(chip == relay_via)
                def _():
                    relay_send().wait_recv()
                    relay_forward(core, CORES - 1 - core).start()

            for other, i in others:
                chip_copy(la, other, other, i).wait_recv()
            total = y_chip[la, 0]
            for c in range(1, chips):
                total = total + y_chip[la, c]
            y_half[la, core] = total
            half_copy(la, core).start()
            half_copy(la, 1 - core).wait_recv()
            y = jnp.concatenate([y_half[la, 0], y_half[la, 1]], axis=0)
            hidden = round_bf16(hidden + norm(y) * (1.0 + post))
        for i in range(self.chunks):
            hid_out[:, i * ROW:(i + 1) * ROW] = hidden[i:i + 1, :].astype(jnp.bfloat16)

        row16 = lax.broadcasted_iota(jnp.int32, (16, hd), 0)
        for kv, out in enumerate((gk_out, gv_out)):
            new = jnp.broadcast_to(fresh[1][kv][0:1], (16, hd))
            out[0, 0, self.seq:self.seq + 16, :] = jnp.where(row16 == 0, new, 0.0).astype(jnp.bfloat16)
            out[0, 0, self.seq + 16:self.slots, :] = jnp.zeros((self.slots - self.seq - 16, hd), jnp.bfloat16)

        for la in range(2):
            for dst, i in peers():
                @pl.when(jnp.logical_or(la == 1, dst >= self.first_src))
                def _():
                    q_send(la, dst, i).wait_send()
            mate_send(la).wait_send()
            for other, i in others:
                chip_copy(la, other, chip, i).wait_send()
            half_copy(la, core).wait_send()
        for dst, i in peers():
            p_send(1, dst, i).wait_send()

        @pl.when(has_loc)
        def _():
            for dst, i in peers():
                p_send(0, dst, i).wait_send()
            for kv in range(2):
                loc_send(kv, mate, d_sem.at[1, kv]).wait_send()
                own_loc[kv].wait()

        for kv in range(2):
            glo_send(kv, mate, d_sem.at[0, kv]).wait_send()
            own_glo[kv].wait()

        def glo_arrival(kv, src_dev):
            src, out = glo_pairs[kv]
            return pltpu.make_async_remote_copy(src_ref=src.at[0, 0], dst_ref=glo_dst(out, src_dev), send_sem=d_sem.at[0, kv],
                                                recv_sem=glo_rsem.at[kv, src_dev], device_id={"a": src_dev}, device_id_type=MESH)

        def loc_arrival(kv, src_dev, lo=0):
            src, out = loc_pairs[kv]
            return pltpu.make_async_remote_copy(src_ref=src.at[0, 0, lo:], dst_ref=loc_dst(out, src_dev, lo), send_sem=d_sem.at[1, kv],
                                                recv_sem=loc_rsem.at[kv, src_dev], device_id={"a": src_dev}, device_id_type=MESH)

        for src_dev, i in peers():
            short = jnp.logical_and(chip == relay_to, src_dev == relay_from * CORES + (CORES - 1 - core))

            @pl.when(src_dev >= self.first_src)
            def _():
                loc_arrival(0, src_dev).wait_recv()

            @pl.when(jnp.logical_and(src_dev >= self.first_src, jnp.logical_not(short)))
            def _():
                loc_arrival(1, src_dev).wait_recv()

            @pl.when(short)
            def _():
                loc_arrival(1, src_dev, RELAY).wait_recv()

        @pl.when(chip == relay_from)
        def _():
            relay_send().wait_send()

        @pl.when(chip == relay_via)
        def _():
            relay_forward(core, CORES - 1 - core).wait_send()

        @pl.when(chip == relay_to)
        def _():
            relay_forward(CORES - 1 - core, core).wait_recv()

        slot = (self.seq % WINDOW) // 16 * 16
        for kv, out in enumerate((lk_out, lv_out)):
            new = jnp.broadcast_to(fresh[0][kv][0:1], (16, hd))
            old = out[0, 0, slot:slot + 16, :].astype(jnp.float32)
            out[0, 0, slot:slot + 16, :] = jnp.where(row16 == self.seq % WINDOW - slot, new, old).astype(jnp.bfloat16)

        for step in range(5, 2 * steps):
            bulk_wait(step)
        for src_dev, i in peers():
            for kv in range(2):
                glo_arrival(kv, src_dev).wait_recv()


def solution(mesh):
    n = mesh.shape["a"]
    cache_in = P("dp", None, "a", None)
    cache_out = P("dp", "a", None, None)
    rows_spec = P("dp", None)
    layer_specs = (P(None, "a"), P(None, "a"), P(None, "a"), P("a", None), P(None), P(None))
    in_specs = (rows_spec, cache_in, cache_in, cache_in, cache_in) + layer_specs + layer_specs
    out_specs = (rows_spec, cache_out, cache_out, cache_out, cache_out)

    def device_step(hidden_in, loc_k, loc_v, glo_k, glo_v, loc_wq, loc_wk, loc_wv, loc_wo, loc_pre, loc_post, glo_wq, glo_wk, glo_wv, glo_wo, glo_pre, glo_post):
        d_model = hidden_in.shape[1]
        rows, heads, blk, hd = loc_k.shape
        q_cols, kv_cols = loc_wq.shape[1], loc_wk.shape[1]
        seq = n * blk
        slots = seq + CACHE_ROOM
        table = jnp.asarray(np.stack(rope_tables(hd, seq)))

        vmem = pl.BlockSpec(memory_space=pltpu.VMEM)
        hbm = pl.BlockSpec(memory_space=pltpu.HBM)
        bf16, f32 = jnp.bfloat16, jnp.float32
        dma = pltpu.SemaphoreType.DMA
        landed = pl.pallas_call(
            Kernel(n, d_model, heads, blk, hd, slots),
            name="decode_step",
            out_shape=(
                pltpu.VMEM(hidden_in.shape, bf16),
                pltpu.VMEM((rows, 1, WINDOW, hd), bf16),
                pltpu.VMEM((rows, 1, WINDOW, hd), bf16),
                pltpu.VMEM((rows, 1, slots, hd), bf16),
                pltpu.VMEM((rows, 1, slots, hd), bf16),
            ),
            in_specs=[hbm] * 18,
            out_specs=(vmem,) * 5,
            scratch_shapes=[
                pltpu.VMEM(hidden_in.shape, bf16),
                pltpu.VMEM((2, hd // 2), f32),
                [pltpu.VMEM((d_model,), bf16)] * 4,
                pltpu.VMEM((2, d_model, q_cols), bf16),
                pltpu.VMEM((2, d_model, kv_cols), bf16),
                pltpu.VMEM((2, d_model, kv_cols), bf16),
                pltpu.VMEM((2, q_cols, d_model), bf16),
                pltpu.VMEM((2, 2, heads, blk, hd), bf16),
                pltpu.VMEM((2, 2, hd), f32),
                pltpu.VMEM((2, n, 2, hd), f32),
                pltpu.VMEM((2, n, 2, hd + 128), f32),
                pltpu.VMEM((2, n, 2, hd + 128), f32),
                pltpu.VMEM((2, CORES, 4, ROW), f32),
                pltpu.VMEM((2, 4, ROW), f32),
                pltpu.VMEM((2, n // CORES, 4, ROW), f32),
                pltpu.VMEM((2, CORES, 4, ROW), f32),
                pltpu.VMEM((RELAY, hd), bf16),
                dma((6,)), dma((16,)), dma((8,)), dma((2, 2)), dma((2, 2)), dma((2, n)), dma((2, n)), dma((2, 4)), dma((2, 2)),
                dma((2, n - 1)), dma((2, n)), dma((2, n - 1)), dma((2, n)), dma((2, 2)), dma((2, 3)), dma((2, n // CORES)), dma((2, 2)), dma((4,)), pltpu.SemaphoreType.REGULAR,
            ],
            compiler_params=pltpu.CompilerParams(collective_id=0, has_side_effects=True, vmem_limit_bytes=48 * 2**20),
        )(hidden_in, table, loc_k, loc_v, glo_k, glo_v, loc_wq, loc_wk, loc_wv, loc_wo, loc_pre, loc_post, glo_wq, glo_wk, glo_wv, glo_wo, glo_pre, glo_post)
        return pl.pallas_call(
            store_outputs,
            name="store_outputs",
            out_shape=tuple(jax.ShapeDtypeStruct(x.shape, x.dtype) for x in landed),
            in_specs=[vmem] * 5,
            out_specs=(hbm,) * 5,
            scratch_shapes=[dma((5, STORE_PARTS))],
            compiler_params=pltpu.CompilerParams(vmem_limit_bytes=2**20),
        )(*landed)

    return jax.shard_map(device_step, mesh=mesh, in_specs=in_specs, out_specs=out_specs, check_vma=False)
```

```python
import functools

import jax
import jax.numpy as jnp
import numpy as np
from jax import lax
from jax.experimental import pallas as pl
from jax.experimental.pallas import tpu as pltpu
from jax.sharding import PartitionSpec as P

SOFTCAP = 50.0
NORM_EPS = 1e-6
ROPE_BASE = 10000.0
WINDOW = 4096
CACHE_ROOM = 512
MESH = pl.DeviceIdType.MESH
CORES = 2
ROW = 512
STORE_PARTS = 2
RELAY = 112
HOLD = 1
SCHEDULE = (1, 2, 3, 4, 5, 6)
NEG = -1e30


def rope_tables(head_dim, position):
    half = head_dim // 2
    inv = np.float32(ROPE_BASE) ** (np.float32(-2.0) * np.arange(half, dtype=np.float32) / np.float32(head_dim))
    ang = np.float32(position) * inv.astype(np.float32)
    return np.cos(ang).astype(np.float32), np.sin(ang).astype(np.float32)


def softcap(scores, scale):
    return SOFTCAP * jnp.tanh(scores * scale / SOFTCAP)


def rows_like(width):
    return lax.broadcasted_iota(jnp.int32, (8, width), 0)


def store_outputs(*refs):
    landed, outs, sem = refs[:5], refs[5:10], refs[10]
    copies = [pltpu.make_async_copy(landed[0], outs[0], sem.at[0, 0])]
    for j in range(1, 5):
        part = landed[j].shape[2] // STORE_PARTS
        for p in range(STORE_PARTS):
            rows = pl.ds(p * part, part)
            copies.append(pltpu.make_async_copy(landed[j].at[0, 0, rows], outs[j].at[0, 0, rows], sem.at[j, p]))
    for cp in copies:
        cp.start()
    for cp in copies:
        cp.wait()


class Kernel:
    def __init__(self, n, d_model, heads, blk, hd, slots):
        self.n, self.d_model, self.heads, self.blk, self.hd, self.slots = n, d_model, heads, blk, hd, slots
        self.seq = n * blk
        self.first_pos = self.seq - WINDOW + 1
        self.first_src = self.first_pos // blk
        self.chunks = d_model // ROW
        self.q_groups = 2

    def __call__(self, hid_in, table_in, loc_k, loc_v, glo_k, glo_v, lwq, lwk, lwv, lwo, lpre, lpost, gwq, gwk, gwv, gwo, gpre, gpost,
                 hid_out, lk_out, lv_out, gk_out, gv_out,
                 hid_b, table, gain_b, wq_b, wk_b, wv_b, wo_b, kv_b, q_msg, q_all, p_msg, p_all, y_part, y_mate, y_chip, y_half, relay_b,
                 in_sem, f_sem, g_sem, d_sem, own_sem, glo_rsem, loc_rsem, w_sem, kv_sem,
                 qs_sem, qr_sem, ps_sem, pr_sem, m_sem, ys_sem, yr_sem, h_sem, r_sem, go_sem):
        n, blk, hd = self.n, self.blk, self.hd
        half = hd // 2
        me = lax.axis_index("a")
        chips = n // CORES
        chip, core = me // CORES, lax.rem(me, CORES)
        has_loc = me >= self.first_src
        right, left, opp = [lax.rem(chip + i, chips) for i in (1, chips - 1, chips // 2)]
        even = lax.rem(chip, 2) == 0
        near_f = jnp.where(even, right, left)
        near_g = jnp.where(even, left, right)

        mate = chip * CORES + (CORES - 1 - core)

        relay_from, relay_via = chips // 2, chips // 2 - 1
        relay_to = (relay_from + chips // 2) % chips

        barrier = pltpu.get_barrier_semaphore()

        def greet(devices):
            for dev in devices:
                pl.semaphore_signal(barrier, inc=1, device_id={"a": dev}, device_id_type=MESH)

        def cores_of(c):
            return [c * CORES + j for j in range(CORES)]

        def tell(c):
            pl.semaphore_signal(go_sem, inc=1, device_id={"a": c * CORES + core}, device_id_type=MESH)

        late = chips - 1
        early_devices = list(range(self.first_src))

        @pl.when(jnp.logical_not(has_loc))
        def _():
            greet([mate] + cores_of(near_f) + cores_of(near_g))

        @pl.when(chip == late)
        def _():
            greet([mate] + early_devices)

        @pl.when(chip == relay_from)
        def _():
            greet(cores_of(late) + early_devices)

        weights = [((lwq, gwq), wq_b), ((lwk, gwk), wk_b), ((lwv, gwv), wv_b), ((lwo, gwo), wo_b)]
        w_cp = [[pltpu.make_async_copy(srcs[la], dst.at[la], w_sem.at[la, j]) for j, (srcs, dst) in enumerate(weights)] for la in range(2)]
        kv_cp = [[pltpu.make_async_copy(src.at[0], kv_b.at[la, j], kv_sem.at[la, j]) for j, src in enumerate(pair)]
                 for la, pair in enumerate(((loc_k, loc_v), (glo_k, glo_v)))]
        glo_pairs = ((glo_k, gk_out), (glo_v, gv_out))
        loc_pairs = ((loc_k, lk_out), (loc_v, lv_out))

        def glo_dst(out, src_dev):
            return out.at[0, 0, pl.ds(pl.multiple_of(src_dev * blk, blk), blk)]

        def loc_dst(out, src_dev, lo=0):
            if lo == 0:
                return out.at[0, 0, pl.ds(pl.multiple_of(lax.rem(src_dev * blk, WINDOW), blk), blk)]
            return out.at[0, 0, pl.ds(pl.multiple_of(lax.rem(src_dev * blk, WINDOW) + lo, 16), blk - lo)]

        in_cp = [pltpu.make_async_copy(hid_in, hid_b, in_sem.at[0]), pltpu.make_async_copy(table_in, table, in_sem.at[1])]
        in_cp += [pltpu.make_async_copy(g, b, in_sem.at[2 + j]) for j, (g, b) in enumerate(zip((lpre, lpost, gpre, gpost), gain_b))]
        for cp in in_cp + w_cp[0][:3]:
            cp.start()

        @pl.when(has_loc)
        def _():
            for cp in kv_cp[0]:
                cp.start()

        w_cp[0][3].start()

        @pl.when(jnp.logical_not(has_loc))
        def _():
            pl.semaphore_wait(barrier, n - 1)

        @pl.when(chip == late)
        def _():
            pl.semaphore_wait(barrier, 1 + 2 * CORES)
            tell(relay_from)

        def glo_send(kv, dst, sem):
            src, out = glo_pairs[kv]
            return pltpu.make_async_remote_copy(src_ref=src.at[0, dst], dst_ref=glo_dst(out, me), send_sem=sem,
                                                recv_sem=glo_rsem.at[kv, me], device_id={"a": dst}, device_id_type=MESH)

        def loc_send(kv, dst, sem, lo=0):
            src, out = loc_pairs[kv]
            return pltpu.make_async_remote_copy(src_ref=src.at[0, dst, lo:], dst_ref=loc_dst(out, me, lo), send_sem=sem,
                                                recv_sem=loc_rsem.at[kv, me], device_id={"a": dst}, device_id_type=MESH)

        def relay_send():
            dst = relay_to * CORES + (CORES - 1 - core)
            return pltpu.make_async_remote_copy(src_ref=loc_v.at[0, dst, pl.ds(0, RELAY)], dst_ref=relay_b, send_sem=r_sem.at[0],
                                                recv_sem=r_sem.at[1], device_id={"a": relay_via * CORES + core}, device_id_type=MESH)

        def relay_forward(src_core, dst_core):
            src_dev = relay_from * CORES + src_core
            dst_ref = lv_out.at[0, 0, pl.ds(pl.multiple_of(lax.rem(src_dev * blk, WINDOW), blk), RELAY)]
            return pltpu.make_async_remote_copy(src_ref=relay_b, dst_ref=dst_ref, send_sem=r_sem.at[2],
                                                recv_sem=r_sem.at[3], device_id={"a": relay_to * CORES + dst_core}, device_id_type=MESH)

        steps = 8

        def step_items(step):
            part = step // 2 if step < steps else step % 4
            kv, peer = part % 2, lax.rem(core + part // 2, CORES)
            if step >= steps:
                return kv, [(opp * CORES + peer, f_sem.at[step])]
            return kv, [(near_f * CORES + peer, f_sem.at[step]), (near_g * CORES + peer, g_sem.at[step])]

        def bulk(step, act, sides=slice(None)):
            kv, items = step_items(step)
            items = items[sides]
            if step >= 12 or (step < steps and step % 2 == 0):
                for dst, sem in items:
                    act(glo_send(kv, dst, sem))
            elif step == 11:
                (dst, sem), = items

                @pl.when(chip == relay_from)
                def _():
                    act(loc_send(kv, dst, sem, RELAY))

                @pl.when(jnp.logical_and(has_loc, chip != relay_from))
                def _():
                    act(loc_send(kv, dst, sem))
            else:
                @pl.when(has_loc)
                def _():
                    for dst, sem in items:
                        act(loc_send(kv, dst, sem))

        def bulk_start(step, sides=slice(None)):
            bulk(step, lambda cp: cp.start(), sides)

        def bulk_wait(step):
            bulk(step, lambda cp: cp.wait_send())

        @pl.when(chip == relay_from)
        def _():
            pl.semaphore_wait(barrier, CORES)
            relay_send().start()
            bulk_start(0, slice(1, 2))
            pl.semaphore_wait(go_sem, 1)
            tell(late)
            bulk_start(0, slice(0, 1))

        @pl.when(chip != relay_from)
        def _():
            bulk_start(0)

        own_glo = [pltpu.make_async_copy(src.at[0, me], glo_dst(out, me), own_sem.at[0, kv]) for kv, (src, out) in enumerate(glo_pairs)]
        own_loc = [pltpu.make_async_copy(src.at[0, me], loc_dst(out, me), own_sem.at[1, kv]) for kv, (src, out) in enumerate(loc_pairs)]
        for kv in range(2):
            glo_send(kv, mate, d_sem.at[0, kv]).start()
            own_glo[kv].start()

        @pl.when(has_loc)
        def _():
            for kv in range(2):
                loc_send(kv, mate, d_sem.at[1, kv]).start()
                own_loc[kv].start()

        for cp in in_cp:
            cp.wait()

        def q_send(la, dst, i):
            return pltpu.make_async_remote_copy(src_ref=q_msg.at[la], dst_ref=q_all.at[la, me], send_sem=qs_sem.at[la, i - 1],
                                                recv_sem=qr_sem.at[la, me], device_id={"a": dst}, device_id_type=MESH)

        def p_send(la, dst, i):
            return pltpu.make_async_remote_copy(src_ref=p_msg.at[la, dst], dst_ref=p_all.at[la, me], send_sem=ps_sem.at[la, i - 1],
                                                recv_sem=pr_sem.at[la, me], device_id={"a": dst}, device_id_type=MESH)

        def mate_send(la):
            return pltpu.make_async_remote_copy(src_ref=y_part.at[la, 1 - core], dst_ref=y_mate.at[la], send_sem=m_sem.at[la, 0],
                                                recv_sem=m_sem.at[la, 1], device_id={"a": mate}, device_id_type=MESH)

        def chip_copy(la, other, slot, i):
            return pltpu.make_async_remote_copy(src_ref=y_chip.at[la, slot], dst_ref=y_chip.at[la, slot], send_sem=ys_sem.at[la, i],
                                                recv_sem=yr_sem.at[la, slot], device_id={"a": other * CORES + core}, device_id_type=MESH)

        def half_copy(la, slot):
            return pltpu.make_async_remote_copy(src_ref=y_half.at[la, slot], dst_ref=y_half.at[la, slot], send_sem=h_sem.at[la, 0],
                                                recv_sem=h_sem.at[la, 1], device_id={"a": mate}, device_id_type=MESH)

        others = [(lax.rem(chip + i, chips), i - 1) for i in range(1, chips)]

        def q_arrival(la, src):
            return pltpu.make_async_remote_copy(src_ref=q_msg.at[la], dst_ref=q_all.at[la, src], send_sem=qs_sem.at[la, 0],
                                                recv_sem=qr_sem.at[la, src], device_id={"a": src}, device_id_type=MESH)

        def p_arrival(la, src):
            return pltpu.make_async_remote_copy(src_ref=p_msg.at[la, 0], dst_ref=p_all.at[la, src], send_sem=ps_sem.at[la, 0],
                                                recv_sem=pr_sem.at[la, src], device_id={"a": src}, device_id_type=MESH)

        def peers():
            return [(lax.rem(me + i, n), i) for i in range(1, n)]

        def norm(x):
            total = jnp.sum(jnp.sum(x * x, axis=1, keepdims=True), axis=0, keepdims=True)
            return x * lax.rsqrt(total / self.d_model + NORM_EPS)

        cosine, sine = table[0:1, :], table[1:2, :]

        def tiled(piece):
            row = rows_like(ROW)
            out = jnp.zeros((8, ROW), jnp.float32)
            for i in range(self.chunks):
                out = jnp.where(row == i, piece(i), out)
            return out

        def gain(j):
            return tiled(lambda i: gain_b[j][i * ROW:(i + 1) * ROW].astype(jnp.float32).reshape(1, ROW))

        def rope(x):
            first, second = x[:, :half], x[:, half:]
            return jnp.concatenate([first * cosine - second * sine, second * cosine + first * sine], axis=1)

        def round_bf16(x):
            return x.astype(jnp.bfloat16).astype(jnp.float32)

        def project(la, hidden, pre):
            a = norm(hidden) * (1.0 + pre)
            for j in range(3):
                w_cp[la][j].wait()
            q = k = v = None
            for i in range(self.chunks):
                lhs = jnp.broadcast_to(a[i:i + 1, :], (16, ROW)).astype(jnp.bfloat16)
                part = [jnp.dot(lhs, w[la, i * ROW:(i + 1) * ROW, :], preferred_element_type=jnp.float32) for w in (wq_b, wk_b, wv_b)]
                q, k, v = part if q is None else (q + part[0], k + part[1], v + part[2])
            q, k, v = q[:2], k[:2], v[:2]
            q0, q1 = rope(q[:, :hd]), rope(q[:, hd:])
            q = round_bf16(jnp.where(lax.broadcasted_iota(jnp.int32, (2, hd), 0) == 0, q0, q1))
            return q, round_bf16(rope(k)), round_bf16(v)

        def attend_block(la, h, masked):
            q = q_all[la, h].astype(jnp.bfloat16)
            s = lax.dot_general(q, kv_b[la, 0, h], (((1,), (1,)), ((), ())), preferred_element_type=jnp.float32)
            s = softcap(s, hd ** -0.5)
            if masked:
                pos = me * blk + lax.broadcasted_iota(jnp.int32, s.shape, 1)
                s = jnp.where(pos >= self.first_pos, s, NEG)
            top = jnp.max(s, axis=1, keepdims=True)
            e = jnp.exp(s - top)
            if masked:
                e = jnp.where(pos >= self.first_pos, e, 0.0)
            total = jnp.sum(e, axis=1, keepdims=True)
            o = jnp.dot(e.astype(jnp.bfloat16), kv_b[la, 1, h], preferred_element_type=jnp.float32)
            lane = lax.broadcasted_iota(jnp.int32, (2, 128), 1)
            p_msg[la, h, :, 0:hd] = o
            p_msg[la, h, :, hd:hd + 128] = jnp.where(lane < 64, top, total)

        def attend_all(la, masked):
            for cp in kv_cp[la]:
                cp.wait()

            def body(h, carry):
                attend_block(la, h, masked)
                return carry

            lax.fori_loop(0, n, body, 0)
            for dst, i in peers():
                p_send(la, dst, i).start()
            p_all[la, me] = p_msg[la, me]

        def combine(la, q, k_new, v_new, first_src):
            s_new = softcap(jnp.sum(q * k_new, axis=1, keepdims=True), hd ** -0.5)
            tops = [p_all[la, s, :, hd:hd + 1] for s in range(first_src, n)]
            sums = [p_all[la, s, :, hd + 64:hd + 65] for s in range(first_src, n)]
            top = s_new
            for t in tops:
                top = jnp.maximum(top, t)
            e_new = jnp.exp(s_new - top)
            denom = e_new
            o = round_bf16(e_new) * v_new
            for idx, s in enumerate(range(first_src, n)):
                w = jnp.exp(tops[idx] - top)
                denom = denom + w * sums[idx]
                o = o + w * p_all[la, s, :, 0:hd]
            return o / denom

        def out_project(la, o):
            w_cp[la][3].wait()
            lhs = [jnp.broadcast_to(o[g:g + 1, :], (16, hd)).astype(jnp.bfloat16) for g in range(self.q_groups)]
            row = rows_like(ROW)
            msg = jnp.zeros((8, ROW), jnp.float32)
            for i in range(self.chunks):
                y = None
                for g in range(self.q_groups):
                    part = jnp.dot(lhs[g], wo_b[la, g * hd:(g + 1) * hd, i * ROW:(i + 1) * ROW], preferred_element_type=jnp.float32)
                    y = part if y is None else y + part
                msg = jnp.where(row == i, y[:8], msg)
            y_part[la, 0] = msg[:4]
            y_part[la, 1] = msg[4:]
            mate_send(la).start()
            mate_send(la).wait_recv()
            y_chip[la, chip] = y_part[la, core] + y_mate[la]
            for other, i in others:
                chip_copy(la, other, chip, i).start()

        def stage(k):
            for step in range(SCHEDULE[k], SCHEDULE[k + 1]):
                bulk_start(step)
            for step in range(SCHEDULE[k - 1] if k else 0, SCHEDULE[k]):
                bulk_wait(step)

        hidden = tiled(lambda i: hid_b[:, i * ROW:(i + 1) * ROW].astype(jnp.float32))
        fresh = []
        for la in range(2):
            pre, post = gain(2 * la), gain(2 * la + 1)
            q, k_new, v_new = project(la, hidden, pre)
            fresh.append((k_new, v_new))
            q_msg[la] = q
            q_all[la, me] = q
            for dst, i in peers():
                @pl.when(jnp.logical_or(la == 1, dst >= self.first_src))
                def _():
                    q_send(la, dst, i).start()
            stage(3 * la)
            if la == 0:
                for cp in w_cp[1] + kv_cp[1]:
                    cp.start()
            if la == 0:
                @pl.when(has_loc)
                def _():
                    @pl.when(chip == late)
                    def _():
                        pl.semaphore_wait(go_sem, 1)

                    for src, i in peers():
                        q_arrival(0, src).wait_recv()
                    attend_all(0, True)
            else:
                for src, i in peers():
                    q_arrival(1, src).wait_recv()
                attend_all(1, False)
            stage(3 * la + 1)
            first_src = self.first_src if la == 0 else 0
            for src, i in peers():
                if la == 0:
                    @pl.when(src >= first_src)
                    def _():
                        p_arrival(0, src).wait_recv()
                else:
                    p_arrival(la, src).wait_recv()
            out_project(la, combine(la, q, k_new, v_new, first_src))
            if la == 0:
                stage(2)
            else:
                for later in range(SCHEDULE[5], steps - HOLD):
                    bulk_start(later)
                for later in range(steps - HOLD, steps):
                    bulk_start(later, slice(1, 2))
                for later in range(steps, 2 * steps):
                    bulk_start(later)
                for later in range(steps - HOLD, steps):
                    bulk_start(later, slice(0, 1))

                @pl.when(chip == relay_via)
                def _():
                    relay_send().wait_recv()
                    relay_forward(core, CORES - 1 - core).start()

            for other, i in others:
                chip_copy(la, other, other, i).wait_recv()
            total = y_chip[la, 0]
            for c in range(1, chips):
                total = total + y_chip[la, c]
            y_half[la, core] = total
            half_copy(la, core).start()
            half_copy(la, 1 - core).wait_recv()
            y = jnp.concatenate([y_half[la, 0], y_half[la, 1]], axis=0)
            hidden = round_bf16(hidden + norm(y) * (1.0 + post))
        for i in range(self.chunks):
            hid_out[:, i * ROW:(i + 1) * ROW] = hidden[i:i + 1, :].astype(jnp.bfloat16)

        row16 = lax.broadcasted_iota(jnp.int32, (16, hd), 0)
        for kv, out in enumerate((gk_out, gv_out)):
            new = jnp.broadcast_to(fresh[1][kv][0:1], (16, hd))
            out[0, 0, self.seq:self.seq + 16, :] = jnp.where(row16 == 0, new, 0.0).astype(jnp.bfloat16)
            out[0, 0, self.seq + 16:self.slots, :] = jnp.zeros((self.slots - self.seq - 16, hd), jnp.bfloat16)

        for la in range(2):
            for dst, i in peers():
                @pl.when(jnp.logical_or(la == 1, dst >= self.first_src))
                def _():
                    q_send(la, dst, i).wait_send()
            mate_send(la).wait_send()
            for other, i in others:
                chip_copy(la, other, chip, i).wait_send()
            half_copy(la, core).wait_send()
        for dst, i in peers():
            p_send(1, dst, i).wait_send()

        @pl.when(has_loc)
        def _():
            for dst, i in peers():
                p_send(0, dst, i).wait_send()
            for kv in range(2):
                loc_send(kv, mate, d_sem.at[1, kv]).wait_send()
                own_loc[kv].wait()

        for kv in range(2):
            glo_send(kv, mate, d_sem.at[0, kv]).wait_send()
            own_glo[kv].wait()

        def glo_arrival(kv, src_dev):
            src, out = glo_pairs[kv]
            return pltpu.make_async_remote_copy(src_ref=src.at[0, 0], dst_ref=glo_dst(out, src_dev), send_sem=d_sem.at[0, kv],
                                                recv_sem=glo_rsem.at[kv, src_dev], device_id={"a": src_dev}, device_id_type=MESH)

        def loc_arrival(kv, src_dev, lo=0):
            src, out = loc_pairs[kv]
            return pltpu.make_async_remote_copy(src_ref=src.at[0, 0, lo:], dst_ref=loc_dst(out, src_dev, lo), send_sem=d_sem.at[1, kv],
                                                recv_sem=loc_rsem.at[kv, src_dev], device_id={"a": src_dev}, device_id_type=MESH)

        for src_dev, i in peers():
            short = jnp.logical_and(chip == relay_to, src_dev == relay_from * CORES + (CORES - 1 - core))

            @pl.when(src_dev >= self.first_src)
            def _():
                loc_arrival(0, src_dev).wait_recv()

            @pl.when(jnp.logical_and(src_dev >= self.first_src, jnp.logical_not(short)))
            def _():
                loc_arrival(1, src_dev).wait_recv()

            @pl.when(short)
            def _():
                loc_arrival(1, src_dev, RELAY).wait_recv()

        @pl.when(chip == relay_from)
        def _():
            relay_send().wait_send()

        @pl.when(chip == relay_via)
        def _():
            relay_forward(core, CORES - 1 - core).wait_send()

        @pl.when(chip == relay_to)
        def _():
            relay_forward(CORES - 1 - core, core).wait_recv()

        slot = (self.seq % WINDOW) // 16 * 16
        for kv, out in enumerate((lk_out, lv_out)):
            new = jnp.broadcast_to(fresh[0][kv][0:1], (16, hd))
            old = out[0, 0, slot:slot + 16, :].astype(jnp.float32)
            out[0, 0, slot:slot + 16, :] = jnp.where(row16 == self.seq % WINDOW - slot, new, old).astype(jnp.bfloat16)

        for step in range(SCHEDULE[4], 2 * steps):
            bulk_wait(step)
        for src_dev, i in peers():
            for kv in range(2):
                glo_arrival(kv, src_dev).wait_recv()


def solution(mesh):
    n = mesh.shape["a"]
    cache_in = P("dp", None, "a", None)
    cache_out = P("dp", "a", None, None)
    rows_spec = P("dp", None)
    layer_specs = (P(None, "a"), P(None, "a"), P(None, "a"), P("a", None), P(None), P(None))
    in_specs = (rows_spec, cache_in, cache_in, cache_in, cache_in) + layer_specs + layer_specs
    out_specs = (rows_spec, cache_out, cache_out, cache_out, cache_out)

    def device_step(hidden_in, loc_k, loc_v, glo_k, glo_v, loc_wq, loc_wk, loc_wv, loc_wo, loc_pre, loc_post, glo_wq, glo_wk, glo_wv, glo_wo, glo_pre, glo_post):
        d_model = hidden_in.shape[1]
        rows, heads, blk, hd = loc_k.shape
        q_cols, kv_cols = loc_wq.shape[1], loc_wk.shape[1]
        seq = n * blk
        slots = seq + CACHE_ROOM
        table = jnp.asarray(np.stack(rope_tables(hd, seq)))

        vmem = pl.BlockSpec(memory_space=pltpu.VMEM)
        hbm = pl.BlockSpec(memory_space=pltpu.HBM)
        bf16, f32 = jnp.bfloat16, jnp.float32
        dma = pltpu.SemaphoreType.DMA
        landed = pl.pallas_call(
            Kernel(n, d_model, heads, blk, hd, slots),
            name="decode_step",
            out_shape=(
                pltpu.VMEM(hidden_in.shape, bf16),
                pltpu.VMEM((rows, 1, WINDOW, hd), bf16),
                pltpu.VMEM((rows, 1, WINDOW, hd), bf16),
                pltpu.VMEM((rows, 1, slots, hd), bf16),
                pltpu.VMEM((rows, 1, slots, hd), bf16),
            ),
            in_specs=[hbm] * 18,
            out_specs=(vmem,) * 5,
            scratch_shapes=[
                pltpu.VMEM(hidden_in.shape, bf16),
                pltpu.VMEM((2, hd // 2), f32),
                [pltpu.VMEM((d_model,), bf16)] * 4,
                pltpu.VMEM((2, d_model, q_cols), bf16),
                pltpu.VMEM((2, d_model, kv_cols), bf16),
                pltpu.VMEM((2, d_model, kv_cols), bf16),
                pltpu.VMEM((2, q_cols, d_model), bf16),
                pltpu.VMEM((2, 2, heads, blk, hd), bf16),
                pltpu.VMEM((2, 2, hd), f32),
                pltpu.VMEM((2, n, 2, hd), f32),
                pltpu.VMEM((2, n, 2, hd + 128), f32),
                pltpu.VMEM((2, n, 2, hd + 128), f32),
                pltpu.VMEM((2, CORES, 4, ROW), f32),
                pltpu.VMEM((2, 4, ROW), f32),
                pltpu.VMEM((2, n // CORES, 4, ROW), f32),
                pltpu.VMEM((2, CORES, 4, ROW), f32),
                pltpu.VMEM((RELAY, hd), bf16),
                dma((6,)), dma((16,)), dma((8,)), dma((2, 2)), dma((2, 2)), dma((2, n)), dma((2, n)), dma((2, 4)), dma((2, 2)),
                dma((2, n - 1)), dma((2, n)), dma((2, n - 1)), dma((2, n)), dma((2, 2)), dma((2, 3)), dma((2, n // CORES)), dma((2, 2)), dma((4,)), pltpu.SemaphoreType.REGULAR,
            ],
            compiler_params=pltpu.CompilerParams(collective_id=0, has_side_effects=True, vmem_limit_bytes=48 * 2**20),
        )(hidden_in, table, loc_k, loc_v, glo_k, glo_v, loc_wq, loc_wk, loc_wv, loc_wo, loc_pre, loc_post, glo_wq, glo_wk, glo_wv, glo_wo, glo_pre, glo_post)
        return pl.pallas_call(
            store_outputs,
            name="store_outputs",
            out_shape=tuple(jax.ShapeDtypeStruct(x.shape, x.dtype) for x in landed),
            in_specs=[vmem] * 5,
            out_specs=(hbm,) * 5,
            scratch_shapes=[dma((5, STORE_PARTS))],
            compiler_params=pltpu.CompilerParams(vmem_limit_bytes=2**20),
        )(*landed)

    return jax.shard_map(device_step, mesh=mesh, in_specs=in_specs, out_specs=out_specs, check_vma=False)
```

```python
import functools

import jax
import jax.numpy as jnp
import numpy as np
from jax import lax
from jax.experimental import pallas as pl
from jax.experimental.pallas import tpu as pltpu
from jax.sharding import PartitionSpec as P

SOFTCAP = 50.0
NORM_EPS = 1e-6
ROPE_BASE = 10000.0
WINDOW = 4096
CACHE_ROOM = 512
MESH = pl.DeviceIdType.MESH
CORES = 2
ROW = 512
STORE_PARTS = 2
RELAY = 112
HOLD = 1
SCHEDULE = (1, 2, 3, 4, 5, 6)
NEG = -1e30


def rope_tables(head_dim, position):
    half = head_dim // 2
    inv = np.float32(ROPE_BASE) ** (np.float32(-2.0) * np.arange(half, dtype=np.float32) / np.float32(head_dim))
    ang = np.float32(position) * inv.astype(np.float32)
    return np.cos(ang).astype(np.float32), np.sin(ang).astype(np.float32)


def softcap(scores, scale):
    return SOFTCAP * jnp.tanh(scores * scale / SOFTCAP)


def rows_like(width):
    return lax.broadcasted_iota(jnp.int32, (8, width), 0)


def store_outputs(*refs):
    landed, outs, sem = refs[:5], refs[5:10], refs[10]
    copies = [pltpu.make_async_copy(landed[0], outs[0], sem.at[0, 0])]
    for j in range(1, 5):
        part = landed[j].shape[2] // STORE_PARTS
        for p in range(STORE_PARTS):
            rows = pl.ds(p * part, part)
            copies.append(pltpu.make_async_copy(landed[j].at[0, 0, rows], outs[j].at[0, 0, rows], sem.at[j, p]))
    for cp in copies:
        cp.start()
    for cp in copies:
        cp.wait()


class Kernel:
    def __init__(self, n, d_model, heads, blk, hd, slots):
        self.n, self.d_model, self.heads, self.blk, self.hd, self.slots = n, d_model, heads, blk, hd, slots
        self.seq = n * blk
        self.first_pos = self.seq - WINDOW + 1
        self.first_src = self.first_pos // blk
        self.chunks = d_model // ROW
        self.q_groups = 2

    def __call__(self, hid_in, table_in, loc_k, loc_v, glo_k, glo_v, lwq, lwk, lwv, lwo, lpre, lpost, gwq, gwk, gwv, gwo, gpre, gpost,
                 hid_out, lk_out, lv_out, gk_out, gv_out,
                 hid_b, table, gain_b, wq_b, wk_b, wv_b, wo_b, kv_b, q_msg, q_all, p_msg, p_mate, p_out, p_all, y_part, y_mate, y_chip, y_half, relay_b,
                 in_sem, f_sem, g_sem, d_sem, own_sem, glo_rsem, loc_rsem, w_sem, kv_sem,
                 qs_sem, qr_sem, pm_sem, ps_sem, pr_sem, m_sem, ys_sem, yr_sem, h_sem, r_sem, go_sem):
        n, blk, hd = self.n, self.blk, self.hd
        half = hd // 2
        me = lax.axis_index("a")
        chips = n // CORES
        chip, core = me // CORES, lax.rem(me, CORES)
        has_loc = me >= self.first_src
        right, left, opp = [lax.rem(chip + i, chips) for i in (1, chips - 1, chips // 2)]
        even = lax.rem(chip, 2) == 0
        near_f = jnp.where(even, right, left)
        near_g = jnp.where(even, left, right)

        mate = chip * CORES + (CORES - 1 - core)

        relay_from, relay_via = chips // 2, chips // 2 - 1
        relay_to = (relay_from + chips // 2) % chips

        barrier = pltpu.get_barrier_semaphore()

        def greet(devices):
            for dev in devices:
                pl.semaphore_signal(barrier, inc=1, device_id={"a": dev}, device_id_type=MESH)

        def cores_of(c):
            return [c * CORES + j for j in range(CORES)]

        def tell(c):
            pl.semaphore_signal(go_sem, inc=1, device_id={"a": c * CORES + core}, device_id_type=MESH)

        late = chips - 1
        early_devices = list(range(self.first_src))

        @pl.when(jnp.logical_not(has_loc))
        def _():
            greet([mate] + cores_of(near_f) + cores_of(near_g))

        @pl.when(chip == late)
        def _():
            greet([mate] + early_devices)

        @pl.when(chip == relay_from)
        def _():
            greet(cores_of(late) + early_devices)

        weights = [((lwq, gwq), wq_b), ((lwk, gwk), wk_b), ((lwv, gwv), wv_b), ((lwo, gwo), wo_b)]
        w_cp = [[pltpu.make_async_copy(srcs[la], dst.at[la], w_sem.at[la, j]) for j, (srcs, dst) in enumerate(weights)] for la in range(2)]
        kv_cp = [[pltpu.make_async_copy(src.at[0], kv_b.at[la, j], kv_sem.at[la, j]) for j, src in enumerate(pair)]
                 for la, pair in enumerate(((loc_k, loc_v), (glo_k, glo_v)))]
        glo_pairs = ((glo_k, gk_out), (glo_v, gv_out))
        loc_pairs = ((loc_k, lk_out), (loc_v, lv_out))

        def glo_dst(out, src_dev):
            return out.at[0, 0, pl.ds(pl.multiple_of(src_dev * blk, blk), blk)]

        def loc_dst(out, src_dev, lo=0):
            if lo == 0:
                return out.at[0, 0, pl.ds(pl.multiple_of(lax.rem(src_dev * blk, WINDOW), blk), blk)]
            return out.at[0, 0, pl.ds(pl.multiple_of(lax.rem(src_dev * blk, WINDOW) + lo, 16), blk - lo)]

        in_cp = [pltpu.make_async_copy(hid_in, hid_b, in_sem.at[0]), pltpu.make_async_copy(table_in, table, in_sem.at[1])]
        in_cp += [pltpu.make_async_copy(g, b, in_sem.at[2 + j]) for j, (g, b) in enumerate(zip((lpre, lpost, gpre, gpost), gain_b))]
        for cp in in_cp + w_cp[0][:3]:
            cp.start()

        @pl.when(has_loc)
        def _():
            for cp in kv_cp[0]:
                cp.start()

        w_cp[0][3].start()

        @pl.when(jnp.logical_not(has_loc))
        def _():
            pl.semaphore_wait(barrier, n - 1)

        @pl.when(chip == late)
        def _():
            pl.semaphore_wait(barrier, 1 + 2 * CORES)
            tell(relay_from)

        def glo_send(kv, dst, sem):
            src, out = glo_pairs[kv]
            return pltpu.make_async_remote_copy(src_ref=src.at[0, dst], dst_ref=glo_dst(out, me), send_sem=sem,
                                                recv_sem=glo_rsem.at[kv, me], device_id={"a": dst}, device_id_type=MESH)

        def loc_send(kv, dst, sem, lo=0):
            src, out = loc_pairs[kv]
            return pltpu.make_async_remote_copy(src_ref=src.at[0, dst, lo:], dst_ref=loc_dst(out, me, lo), send_sem=sem,
                                                recv_sem=loc_rsem.at[kv, me], device_id={"a": dst}, device_id_type=MESH)

        def relay_send():
            dst = relay_to * CORES + (CORES - 1 - core)
            return pltpu.make_async_remote_copy(src_ref=loc_v.at[0, dst, pl.ds(0, RELAY)], dst_ref=relay_b, send_sem=r_sem.at[0],
                                                recv_sem=r_sem.at[1], device_id={"a": relay_via * CORES + core}, device_id_type=MESH)

        def relay_forward(src_core, dst_core):
            src_dev = relay_from * CORES + src_core
            dst_ref = lv_out.at[0, 0, pl.ds(pl.multiple_of(lax.rem(src_dev * blk, WINDOW), blk), RELAY)]
            return pltpu.make_async_remote_copy(src_ref=relay_b, dst_ref=dst_ref, send_sem=r_sem.at[2],
                                                recv_sem=r_sem.at[3], device_id={"a": relay_to * CORES + dst_core}, device_id_type=MESH)

        steps = 8

        def step_items(step):
            part = step // 2 if step < steps else step % 4
            kv, peer = part % 2, lax.rem(core + part // 2, CORES)
            if step >= steps:
                return kv, [(opp * CORES + peer, f_sem.at[step])]
            return kv, [(near_f * CORES + peer, f_sem.at[step]), (near_g * CORES + peer, g_sem.at[step])]

        def bulk(step, act, sides=slice(None)):
            kv, items = step_items(step)
            items = items[sides]
            if step >= 12 or (step < steps and step % 2 == 1):
                for dst, sem in items:
                    act(glo_send(kv, dst, sem))
            elif step == 11:
                (dst, sem), = items

                @pl.when(chip == relay_from)
                def _():
                    act(loc_send(kv, dst, sem, RELAY))

                @pl.when(jnp.logical_and(has_loc, chip != relay_from))
                def _():
                    act(loc_send(kv, dst, sem))
            else:
                @pl.when(has_loc)
                def _():
                    for dst, sem in items:
                        act(loc_send(kv, dst, sem))

        def bulk_start(step, sides=slice(None)):
            bulk(step, lambda cp: cp.start(), sides)

        def bulk_wait(step):
            bulk(step, lambda cp: cp.wait_send())

        @pl.when(chip == relay_from)
        def _():
            pl.semaphore_wait(barrier, CORES)
            relay_send().start()
            bulk_start(0, slice(1, 2))
            pl.semaphore_wait(go_sem, 1)
            tell(late)
            bulk_start(0, slice(0, 1))

        @pl.when(chip != relay_from)
        def _():
            bulk_start(0)

        own_glo = [pltpu.make_async_copy(src.at[0, me], glo_dst(out, me), own_sem.at[0, kv]) for kv, (src, out) in enumerate(glo_pairs)]
        own_loc = [pltpu.make_async_copy(src.at[0, me], loc_dst(out, me), own_sem.at[1, kv]) for kv, (src, out) in enumerate(loc_pairs)]
        for kv in range(2):
            glo_send(kv, mate, d_sem.at[0, kv]).start()
            own_glo[kv].start()

        @pl.when(has_loc)
        def _():
            for kv in range(2):
                loc_send(kv, mate, d_sem.at[1, kv]).start()
                own_loc[kv].start()

        for cp in in_cp:
            cp.wait()

        def q_send(la, dst, i):
            return pltpu.make_async_remote_copy(src_ref=q_msg.at[la], dst_ref=q_all.at[la, me], send_sem=qs_sem.at[la, i - 1],
                                                recv_sem=qr_sem.at[la, me], device_id={"a": dst}, device_id_type=MESH)

        def p_mate_send(la):
            return pltpu.make_async_remote_copy(src_ref=p_msg.at[la, 1 - core], dst_ref=p_mate.at[la], send_sem=pm_sem.at[la, 0],
                                                recv_sem=pm_sem.at[la, 1], device_id={"a": mate}, device_id_type=MESH)

        def p_send(la, other, i):
            return pltpu.make_async_remote_copy(src_ref=p_out.at[la, other], dst_ref=p_all.at[la, chip], send_sem=ps_sem.at[la, i],
                                                recv_sem=pr_sem.at[la, chip], device_id={"a": other * CORES + core}, device_id_type=MESH)

        def mate_send(la):
            return pltpu.make_async_remote_copy(src_ref=y_part.at[la, 1 - core], dst_ref=y_mate.at[la], send_sem=m_sem.at[la, 0],
                                                recv_sem=m_sem.at[la, 1], device_id={"a": mate}, device_id_type=MESH)

        def chip_copy(la, other, slot, i):
            return pltpu.make_async_remote_copy(src_ref=y_chip.at[la, slot], dst_ref=y_chip.at[la, slot], send_sem=ys_sem.at[la, i],
                                                recv_sem=yr_sem.at[la, slot], device_id={"a": other * CORES + core}, device_id_type=MESH)

        def half_copy(la, slot):
            return pltpu.make_async_remote_copy(src_ref=y_half.at[la, slot], dst_ref=y_half.at[la, slot], send_sem=h_sem.at[la, 0],
                                                recv_sem=h_sem.at[la, 1], device_id={"a": mate}, device_id_type=MESH)

        others = [(lax.rem(chip + i, chips), i - 1) for i in range(1, chips)]

        def q_arrival(la, src):
            return pltpu.make_async_remote_copy(src_ref=q_msg.at[la], dst_ref=q_all.at[la, src], send_sem=qs_sem.at[la, 0],
                                                recv_sem=qr_sem.at[la, src], device_id={"a": src}, device_id_type=MESH)

        def p_arrival(la, other):
            return pltpu.make_async_remote_copy(src_ref=p_out.at[la, other], dst_ref=p_all.at[la, other], send_sem=ps_sem.at[la, 0],
                                                recv_sem=pr_sem.at[la, other], device_id={"a": other * CORES + core}, device_id_type=MESH)

        def peers():
            return [(lax.rem(me + i, n), i) for i in range(1, n)]

        def norm(x):
            total = jnp.sum(jnp.sum(x * x, axis=1, keepdims=True), axis=0, keepdims=True)
            return x * lax.rsqrt(total / self.d_model + NORM_EPS)

        cosine, sine = table[0:1, :], table[1:2, :]

        def tiled(piece):
            row = rows_like(ROW)
            out = jnp.zeros((8, ROW), jnp.float32)
            for i in range(self.chunks):
                out = jnp.where(row == i, piece(i), out)
            return out

        def gain(j):
            return tiled(lambda i: gain_b[j][i * ROW:(i + 1) * ROW].astype(jnp.float32).reshape(1, ROW))

        def rope(x):
            first, second = x[:, :half], x[:, half:]
            return jnp.concatenate([first * cosine - second * sine, second * cosine + first * sine], axis=1)

        def round_bf16(x):
            return x.astype(jnp.bfloat16).astype(jnp.float32)

        def project(la, hidden, pre):
            a = norm(hidden) * (1.0 + pre)
            for j in range(3):
                w_cp[la][j].wait()
            q = k = v = None
            for i in range(self.chunks):
                lhs = jnp.broadcast_to(a[i:i + 1, :], (16, ROW)).astype(jnp.bfloat16)
                part = [jnp.dot(lhs, w[la, i * ROW:(i + 1) * ROW, :], preferred_element_type=jnp.float32) for w in (wq_b, wk_b, wv_b)]
                q, k, v = part if q is None else (q + part[0], k + part[1], v + part[2])
            q, k, v = q[:2], k[:2], v[:2]
            q0, q1 = rope(q[:, :hd]), rope(q[:, hd:])
            q = round_bf16(jnp.where(lax.broadcasted_iota(jnp.int32, (2, hd), 0) == 0, q0, q1))
            return q, round_bf16(rope(k)), round_bf16(v)

        def attend_block(la, h, masked):
            q = q_all[la, h]
            s = lax.dot_general(q, kv_b[la, 0, h], (((1,), (1,)), ((), ())), preferred_element_type=jnp.float32)
            s = softcap(s, hd ** -0.5)
            if masked:
                pos = me * blk + lax.broadcasted_iota(jnp.int32, s.shape, 1)
                s = jnp.where(pos >= self.first_pos, s, NEG)
            top = jnp.max(s, axis=1, keepdims=True)
            e = jnp.exp(s - top)
            if masked:
                e = jnp.where(pos >= self.first_pos, e, 0.0)
            total = jnp.sum(e, axis=1, keepdims=True)
            o = jnp.dot(e.astype(jnp.bfloat16), kv_b[la, 1, h], preferred_element_type=jnp.float32)
            lane = lax.broadcasted_iota(jnp.int32, (2, 128), 1)
            p_msg[la, lax.rem(h, CORES), h // CORES, :, 0:hd] = o
            p_msg[la, lax.rem(h, CORES), h // CORES, :, hd:hd + 128] = jnp.where(lane < 64, top, total)

        def attend_all(la, masked):
            for cp in kv_cp[la]:
                cp.wait()

            def body(h, carry):
                attend_block(la, h, masked)
                return carry

            lax.fori_loop(0, n, body, 0)
            p_mate_send(la).start()
            p_mate_send(la).wait_recv()
            lane = lax.broadcasted_iota(jnp.int32, (2, 128), 1)
            for c in range(chips):
                top, total, o = merge([p_msg[la, core, c], p_mate[la, c]])
                p_out[la, c, :, 0:hd] = o
                p_out[la, c, :, hd:hd + 128] = jnp.where(lane < 64, top, total)
            for other, i in others:
                p_send(la, other, i).start()
            p_all[la, chip] = p_out[la, chip]

        def merge(parts):
            tops = [p[:, hd:hd + 1] for p in parts]
            top = functools.reduce(jnp.maximum, tops)
            weights = [jnp.exp(t - top) for t in tops]
            total = sum(w * p[:, hd + 64:hd + 65] for w, p in zip(weights, parts))
            return top, total, sum(w * p[:, 0:hd] for w, p in zip(weights, parts))

        def combine(la, q, k_new, v_new, first_chip):
            s_new = softcap(jnp.sum(q * k_new, axis=1, keepdims=True), hd ** -0.5)
            old_top, old_total, old_o = merge([p_all[la, c] for c in range(first_chip, chips)])
            top = jnp.maximum(s_new, old_top)
            e_new, w = jnp.exp(s_new - top), jnp.exp(old_top - top)
            return (round_bf16(e_new) * v_new + w * old_o) / (e_new + w * old_total)

        def out_project(la, o):
            w_cp[la][3].wait()
            lhs = [jnp.broadcast_to(o[g:g + 1, :], (16, hd)).astype(jnp.bfloat16) for g in range(self.q_groups)]
            row = rows_like(ROW)
            msg = jnp.zeros((8, ROW), jnp.float32)
            for i in range(self.chunks):
                y = None
                for g in range(self.q_groups):
                    part = jnp.dot(lhs[g], wo_b[la, g * hd:(g + 1) * hd, i * ROW:(i + 1) * ROW], preferred_element_type=jnp.float32)
                    y = part if y is None else y + part
                msg = jnp.where(row == i, y[:8], msg)
            y_part[la, 0] = msg[:4]
            y_part[la, 1] = msg[4:]
            mate_send(la).start()
            mate_send(la).wait_recv()
            y_chip[la, chip] = y_part[la, core] + y_mate[la]
            for other, i in others:
                chip_copy(la, other, chip, i).start()

        def stage(k):
            for step in range(SCHEDULE[k], SCHEDULE[k + 1]):
                bulk_start(step)
            for step in range(SCHEDULE[k - 1] if k else 0, SCHEDULE[k]):
                bulk_wait(step)

        hidden = tiled(lambda i: hid_b[:, i * ROW:(i + 1) * ROW].astype(jnp.float32))
        fresh = []
        for la in range(2):
            pre, post = gain(2 * la), gain(2 * la + 1)
            q, k_new, v_new = project(la, hidden, pre)
            fresh.append((k_new, v_new))
            q_msg[la] = q.astype(jnp.bfloat16)
            q_all[la, me] = q.astype(jnp.bfloat16)
            for dst, i in peers():
                @pl.when(jnp.logical_or(la == 1, dst >= self.first_src))
                def _():
                    q_send(la, dst, i).start()
            stage(3 * la)
            if la == 0:
                for cp in w_cp[1] + kv_cp[1]:
                    cp.start()
            if la == 0:
                @pl.when(has_loc)
                def _():
                    @pl.when(chip == late)
                    def _():
                        pl.semaphore_wait(go_sem, 1)

                    for src, i in peers():
                        q_arrival(0, src).wait_recv()
                    attend_all(0, True)
            else:
                for src, i in peers():
                    q_arrival(1, src).wait_recv()
                attend_all(1, False)
            stage(3 * la + 1)
            first_chip = self.first_src // CORES if la == 0 else 0
            for other, i in others:
                @pl.when(other >= first_chip)
                def _():
                    p_arrival(la, other).wait_recv()
            out_project(la, combine(la, q, k_new, v_new, first_chip))
            if la == 0:
                stage(2)
            else:
                for later in range(SCHEDULE[5], steps - HOLD):
                    bulk_start(later)
                for later in range(steps - HOLD, steps):
                    bulk_start(later, slice(1, 2))
                for later in range(steps, 2 * steps):
                    bulk_start(later)
                for later in range(steps - HOLD, steps):
                    bulk_start(later, slice(0, 1))

                @pl.when(chip == relay_via)
                def _():
                    relay_send().wait_recv()
                    relay_forward(core, CORES - 1 - core).start()

            for other, i in others:
                chip_copy(la, other, other, i).wait_recv()
            total = y_chip[la, 0]
            for c in range(1, chips):
                total = total + y_chip[la, c]
            y_half[la, core] = total
            half_copy(la, core).start()
            half_copy(la, 1 - core).wait_recv()
            y = jnp.concatenate([y_half[la, 0], y_half[la, 1]], axis=0)
            hidden = round_bf16(hidden + norm(y) * (1.0 + post))
        for i in range(self.chunks):
            hid_out[:, i * ROW:(i + 1) * ROW] = hidden[i:i + 1, :].astype(jnp.bfloat16)

        row16 = lax.broadcasted_iota(jnp.int32, (16, hd), 0)
        for kv, out in enumerate((gk_out, gv_out)):
            new = jnp.broadcast_to(fresh[1][kv][0:1], (16, hd))
            out[0, 0, self.seq:self.seq + 16, :] = jnp.where(row16 == 0, new, 0.0).astype(jnp.bfloat16)
            out[0, 0, self.seq + 16:self.slots, :] = jnp.zeros((self.slots - self.seq - 16, hd), jnp.bfloat16)

        for la in range(2):
            for dst, i in peers():
                @pl.when(jnp.logical_or(la == 1, dst >= self.first_src))
                def _():
                    q_send(la, dst, i).wait_send()
            mate_send(la).wait_send()
            for other, i in others:
                chip_copy(la, other, chip, i).wait_send()
            half_copy(la, core).wait_send()
        p_mate_send(1).wait_send()
        for other, i in others:
            p_send(1, other, i).wait_send()

        @pl.when(has_loc)
        def _():
            p_mate_send(0).wait_send()
            for other, i in others:
                p_send(0, other, i).wait_send()
            for kv in range(2):
                loc_send(kv, mate, d_sem.at[1, kv]).wait_send()
                own_loc[kv].wait()

        for kv in range(2):
            glo_send(kv, mate, d_sem.at[0, kv]).wait_send()
            own_glo[kv].wait()

        def glo_arrival(kv, src_dev):
            src, out = glo_pairs[kv]
            return pltpu.make_async_remote_copy(src_ref=src.at[0, 0], dst_ref=glo_dst(out, src_dev), send_sem=d_sem.at[0, kv],
                                                recv_sem=glo_rsem.at[kv, src_dev], device_id={"a": src_dev}, device_id_type=MESH)

        def loc_arrival(kv, src_dev, lo=0):
            src, out = loc_pairs[kv]
            return pltpu.make_async_remote_copy(src_ref=src.at[0, 0, lo:], dst_ref=loc_dst(out, src_dev, lo), send_sem=d_sem.at[1, kv],
                                                recv_sem=loc_rsem.at[kv, src_dev], device_id={"a": src_dev}, device_id_type=MESH)

        for src_dev, i in peers():
            short = jnp.logical_and(chip == relay_to, src_dev == relay_from * CORES + (CORES - 1 - core))

            @pl.when(src_dev >= self.first_src)
            def _():
                loc_arrival(0, src_dev).wait_recv()

            @pl.when(jnp.logical_and(src_dev >= self.first_src, jnp.logical_not(short)))
            def _():
                loc_arrival(1, src_dev).wait_recv()

            @pl.when(short)
            def _():
                loc_arrival(1, src_dev, RELAY).wait_recv()

        @pl.when(chip == relay_from)
        def _():
            relay_send().wait_send()

        @pl.when(chip == relay_via)
        def _():
            relay_forward(core, CORES - 1 - core).wait_send()

        @pl.when(chip == relay_to)
        def _():
            relay_forward(CORES - 1 - core, core).wait_recv()

        slot = (self.seq % WINDOW) // 16 * 16
        for kv, out in enumerate((lk_out, lv_out)):
            new = jnp.broadcast_to(fresh[0][kv][0:1], (16, hd))
            old = out[0, 0, slot:slot + 16, :].astype(jnp.float32)
            out[0, 0, slot:slot + 16, :] = jnp.where(row16 == self.seq % WINDOW - slot, new, old).astype(jnp.bfloat16)

        for step in range(SCHEDULE[4], 2 * steps):
            bulk_wait(step)
        for c in (chip, near_f, opp, near_g):
            for src_dev in ([mate] if c is chip else cores_of(c)):
                for kv in range(2):
                    glo_arrival(kv, src_dev).wait_recv()


def solution(mesh):
    n = mesh.shape["a"]
    cache_in = P("dp", None, "a", None)
    cache_out = P("dp", "a", None, None)
    rows_spec = P("dp", None)
    layer_specs = (P(None, "a"), P(None, "a"), P(None, "a"), P("a", None), P(None), P(None))
    in_specs = (rows_spec, cache_in, cache_in, cache_in, cache_in) + layer_specs + layer_specs
    out_specs = (rows_spec, cache_out, cache_out, cache_out, cache_out)

    def device_step(hidden_in, loc_k, loc_v, glo_k, glo_v, loc_wq, loc_wk, loc_wv, loc_wo, loc_pre, loc_post, glo_wq, glo_wk, glo_wv, glo_wo, glo_pre, glo_post):
        d_model = hidden_in.shape[1]
        rows, heads, blk, hd = loc_k.shape
        q_cols, kv_cols = loc_wq.shape[1], loc_wk.shape[1]
        seq = n * blk
        slots = seq + CACHE_ROOM
        table = jnp.asarray(np.stack(rope_tables(hd, seq)))

        vmem = pl.BlockSpec(memory_space=pltpu.VMEM)
        hbm = pl.BlockSpec(memory_space=pltpu.HBM)
        bf16, f32 = jnp.bfloat16, jnp.float32
        dma = pltpu.SemaphoreType.DMA
        landed = pl.pallas_call(
            Kernel(n, d_model, heads, blk, hd, slots),
            name="decode_step",
            out_shape=(
                pltpu.VMEM(hidden_in.shape, bf16),
                pltpu.VMEM((rows, 1, WINDOW, hd), bf16),
                pltpu.VMEM((rows, 1, WINDOW, hd), bf16),
                pltpu.VMEM((rows, 1, slots, hd), bf16),
                pltpu.VMEM((rows, 1, slots, hd), bf16),
            ),
            in_specs=[hbm] * 18,
            out_specs=(vmem,) * 5,
            scratch_shapes=[
                pltpu.VMEM(hidden_in.shape, bf16),
                pltpu.VMEM((2, hd // 2), f32),
                [pltpu.VMEM((d_model,), bf16)] * 4,
                pltpu.VMEM((2, d_model, q_cols), bf16),
                pltpu.VMEM((2, d_model, kv_cols), bf16),
                pltpu.VMEM((2, d_model, kv_cols), bf16),
                pltpu.VMEM((2, q_cols, d_model), bf16),
                pltpu.VMEM((2, 2, heads, blk, hd), bf16),
                pltpu.VMEM((2, 2, hd), bf16),
                pltpu.VMEM((2, n, 2, hd), bf16),
                pltpu.VMEM((2, CORES, n // CORES, 2, hd + 128), f32),
                pltpu.VMEM((2, n // CORES, 2, hd + 128), f32),
                pltpu.VMEM((2, n // CORES, 2, hd + 128), f32),
                pltpu.VMEM((2, n // CORES, 2, hd + 128), f32),
                pltpu.VMEM((2, CORES, 4, ROW), f32),
                pltpu.VMEM((2, 4, ROW), f32),
                pltpu.VMEM((2, n // CORES, 4, ROW), f32),
                pltpu.VMEM((2, CORES, 4, ROW), f32),
                pltpu.VMEM((RELAY, hd), bf16),
                dma((6,)), dma((16,)), dma((8,)), dma((2, 2)), dma((2, 2)), dma((2, n)), dma((2, n)), dma((2, 4)), dma((2, 2)),
                dma((2, n - 1)), dma((2, n)), dma((2, 2)), dma((2, 3)), dma((2, n // CORES)), dma((2, 2)), dma((2, 3)), dma((2, n // CORES)), dma((2, 2)), dma((4,)), pltpu.SemaphoreType.REGULAR,
            ],
            compiler_params=pltpu.CompilerParams(collective_id=0, has_side_effects=True, vmem_limit_bytes=48 * 2**20),
        )(hidden_in, table, loc_k, loc_v, glo_k, glo_v, loc_wq, loc_wk, loc_wv, loc_wo, loc_pre, loc_post, glo_wq, glo_wk, glo_wv, glo_wo, glo_pre, glo_post)
        return pl.pallas_call(
            store_outputs,
            name="store_outputs",
            out_shape=tuple(jax.ShapeDtypeStruct(x.shape, x.dtype) for x in landed),
            in_specs=[vmem] * 5,
            out_specs=(hbm,) * 5,
            scratch_shapes=[dma((5, STORE_PARTS))],
            compiler_params=pltpu.CompilerParams(vmem_limit_bytes=2**20),
        )(*landed)

    return jax.shard_map(device_step, mesh=mesh, in_specs=in_specs, out_specs=out_specs, check_vma=False)
```

```python
import functools

import jax
import jax.numpy as jnp
import numpy as np
from jax import lax
from jax.experimental import pallas as pl
from jax.experimental.pallas import tpu as pltpu
from jax.sharding import PartitionSpec as P

SOFTCAP = 50.0
NORM_EPS = 1e-6
ROPE_BASE = 10000.0
WINDOW = 4096
CACHE_ROOM = 512
MESH = pl.DeviceIdType.MESH
CORES = 2
ROW = 512
STORE_PARTS = 2
RELAY = 112
HOLD = 1
SCHEDULE = (1, 2, 3, 4, 5, 6, 7)
NEG = -1e30


def rope_tables(head_dim, position):
    half = head_dim // 2
    inv = np.float32(ROPE_BASE) ** (np.float32(-2.0) * np.arange(half, dtype=np.float32) / np.float32(head_dim))
    ang = np.float32(position) * inv.astype(np.float32)
    return np.cos(ang).astype(np.float32), np.sin(ang).astype(np.float32)


def softcap(scores, scale):
    return SOFTCAP * jnp.tanh(scores * scale / SOFTCAP)


def rows_like(width):
    return lax.broadcasted_iota(jnp.int32, (8, width), 0)


def store_outputs(*refs):
    landed, outs, sem = refs[:5], refs[5:10], refs[10]
    copies = [pltpu.make_async_copy(landed[0], outs[0], sem.at[0, 0])]
    for j in range(1, 5):
        part = landed[j].shape[2] // STORE_PARTS
        for p in range(STORE_PARTS):
            rows = pl.ds(p * part, part)
            copies.append(pltpu.make_async_copy(landed[j].at[0, 0, rows], outs[j].at[0, 0, rows], sem.at[j, p]))
    for cp in copies:
        cp.start()
    for cp in copies:
        cp.wait()


class Kernel:
    def __init__(self, n, d_model, heads, blk, hd, slots):
        self.n, self.d_model, self.heads, self.blk, self.hd, self.slots = n, d_model, heads, blk, hd, slots
        self.seq = n * blk
        self.first_pos = self.seq - WINDOW + 1
        self.first_src = self.first_pos // blk
        self.chunks = d_model // ROW
        self.q_groups = 2

    def __call__(self, hid_in, table_in, loc_k, loc_v, glo_k, glo_v, lwq, lwk, lwv, lwo, lpre, lpost, gwq, gwk, gwv, gwo, gpre, gpost,
                 hid_out, lk_out, lv_out, gk_out, gv_out,
                 hid_b, table, gain_b, wq_b, wk_b, wv_b, wo_b, kv_b, q_msg, q_all, p_msg, p_mate, p_out, p_all, y_part, y_mate, y_chip, y_half, relay_b,
                 in_sem, f_sem, g_sem, d_sem, own_sem, glo_rsem, loc_rsem, w_sem, kv_sem,
                 qs_sem, qr_sem, pm_sem, ps_sem, pr_sem, m_sem, ys_sem, yr_sem, h_sem, r_sem, go_sem):
        n, blk, hd = self.n, self.blk, self.hd
        half = hd // 2
        me = lax.axis_index("a")
        chips = n // CORES
        chip, core = me // CORES, lax.rem(me, CORES)
        has_loc = me >= self.first_src
        right, left, opp = [lax.rem(chip + i, chips) for i in (1, chips - 1, chips // 2)]
        even = lax.rem(chip, 2) == 0
        near_f = jnp.where(even, right, left)
        near_g = jnp.where(even, left, right)

        mate = chip * CORES + (CORES - 1 - core)

        relay_from, relay_via = chips // 2, chips // 2 - 1
        relay_to = (relay_from + chips // 2) % chips

        barrier = pltpu.get_barrier_semaphore()

        def greet(devices):
            for dev in devices:
                pl.semaphore_signal(barrier, inc=1, device_id={"a": dev}, device_id_type=MESH)

        def cores_of(c):
            return [c * CORES + j for j in range(CORES)]

        def tell(c):
            pl.semaphore_signal(go_sem, inc=1, device_id={"a": c * CORES + core}, device_id_type=MESH)

        late = chips - 1
        early_devices = list(range(self.first_src))

        @pl.when(jnp.logical_not(has_loc))
        def _():
            greet([mate] + cores_of(near_f) + cores_of(near_g))

        @pl.when(chip == late)
        def _():
            greet([mate] + early_devices)

        @pl.when(chip == relay_from)
        def _():
            greet(cores_of(late) + early_devices)

        weights = [((lwq, gwq), wq_b), ((lwk, gwk), wk_b), ((lwv, gwv), wv_b), ((lwo, gwo), wo_b)]
        w_cp = [[pltpu.make_async_copy(srcs[la], dst.at[la], w_sem.at[la, j]) for j, (srcs, dst) in enumerate(weights)] for la in range(2)]
        kv_cp = [[pltpu.make_async_copy(src.at[0], kv_b.at[la, j], kv_sem.at[la, j]) for j, src in enumerate(pair)]
                 for la, pair in enumerate(((loc_k, loc_v), (glo_k, glo_v)))]
        glo_pairs = ((glo_k, gk_out), (glo_v, gv_out))
        loc_pairs = ((loc_k, lk_out), (loc_v, lv_out))

        def glo_dst(out, src_dev):
            return out.at[0, 0, pl.ds(pl.multiple_of(src_dev * blk, blk), blk)]

        def loc_dst(out, src_dev, lo=0):
            if lo == 0:
                return out.at[0, 0, pl.ds(pl.multiple_of(lax.rem(src_dev * blk, WINDOW), blk), blk)]
            return out.at[0, 0, pl.ds(pl.multiple_of(lax.rem(src_dev * blk, WINDOW) + lo, 16), blk - lo)]

        in_cp = [pltpu.make_async_copy(hid_in, hid_b, in_sem.at[0]), pltpu.make_async_copy(table_in, table, in_sem.at[1])]
        in_cp += [pltpu.make_async_copy(g, b, in_sem.at[2 + j]) for j, (g, b) in enumerate(zip((lpre, lpost, gpre, gpost), gain_b))]
        for cp in in_cp + w_cp[0][:3]:
            cp.start()

        @pl.when(has_loc)
        def _():
            for cp in kv_cp[0]:
                cp.start()

        w_cp[0][3].start()

        @pl.when(jnp.logical_not(has_loc))
        def _():
            pl.semaphore_wait(barrier, n - 1)

        @pl.when(chip == late)
        def _():
            pl.semaphore_wait(barrier, 1 + 2 * CORES)
            tell(relay_from)

        def glo_send(kv, dst, sem):
            src, out = glo_pairs[kv]
            return pltpu.make_async_remote_copy(src_ref=src.at[0, dst], dst_ref=glo_dst(out, me), send_sem=sem,
                                                recv_sem=glo_rsem.at[kv, me], device_id={"a": dst}, device_id_type=MESH)

        def loc_send(kv, dst, sem, lo=0):
            src, out = loc_pairs[kv]
            return pltpu.make_async_remote_copy(src_ref=src.at[0, dst, lo:], dst_ref=loc_dst(out, me, lo), send_sem=sem,
                                                recv_sem=loc_rsem.at[kv, me], device_id={"a": dst}, device_id_type=MESH)

        def relay_send():
            dst = relay_to * CORES + (CORES - 1 - core)
            return pltpu.make_async_remote_copy(src_ref=loc_v.at[0, dst, pl.ds(0, RELAY)], dst_ref=relay_b, send_sem=r_sem.at[0],
                                                recv_sem=r_sem.at[1], device_id={"a": relay_via * CORES + core}, device_id_type=MESH)

        def relay_forward(src_core, dst_core):
            src_dev = relay_from * CORES + src_core
            dst_ref = lv_out.at[0, 0, pl.ds(pl.multiple_of(lax.rem(src_dev * blk, WINDOW), blk), RELAY)]
            return pltpu.make_async_remote_copy(src_ref=relay_b, dst_ref=dst_ref, send_sem=r_sem.at[2],
                                                recv_sem=r_sem.at[3], device_id={"a": relay_to * CORES + dst_core}, device_id_type=MESH)

        steps = 8

        def step_items(step):
            part = step // 2 if step < steps else step % 4
            kv, peer = part % 2, lax.rem(core + part // 2, CORES)
            if step >= steps:
                return kv, [(opp * CORES + peer, f_sem.at[step])]
            return kv, [(near_f * CORES + peer, f_sem.at[step]), (near_g * CORES + peer, g_sem.at[step])]

        def bulk(step, act, sides=slice(None)):
            kv, items = step_items(step)
            items = items[sides]
            if step >= 12 or (step < steps and step % 2 == 1):
                for dst, sem in items:
                    act(glo_send(kv, dst, sem))
            elif step == 11:
                (dst, sem), = items

                @pl.when(chip == relay_from)
                def _():
                    act(loc_send(kv, dst, sem, RELAY))

                @pl.when(jnp.logical_and(has_loc, chip != relay_from))
                def _():
                    act(loc_send(kv, dst, sem))
            else:
                @pl.when(has_loc)
                def _():
                    for dst, sem in items:
                        act(loc_send(kv, dst, sem))

        def bulk_start(step, sides=slice(None)):
            bulk(step, lambda cp: cp.start(), sides)

        def bulk_wait(step):
            bulk(step, lambda cp: cp.wait_send())

        @pl.when(chip == relay_from)
        def _():
            pl.semaphore_wait(barrier, CORES)
            relay_send().start()
            bulk_start(0, slice(1, 2))
            pl.semaphore_wait(go_sem, 1)
            tell(late)
            bulk_start(0, slice(0, 1))

        @pl.when(chip != relay_from)
        def _():
            bulk_start(0)

        own_glo = [pltpu.make_async_copy(src.at[0, me], glo_dst(out, me), own_sem.at[0, kv]) for kv, (src, out) in enumerate(glo_pairs)]
        own_loc = [pltpu.make_async_copy(src.at[0, me], loc_dst(out, me), own_sem.at[1, kv]) for kv, (src, out) in enumerate(loc_pairs)]
        for kv in range(2):
            glo_send(kv, mate, d_sem.at[0, kv]).start()
            own_glo[kv].start()

        @pl.when(has_loc)
        def _():
            for kv in range(2):
                loc_send(kv, mate, d_sem.at[1, kv]).start()
                own_loc[kv].start()

        for cp in in_cp:
            cp.wait()

        def q_send(la, dst, i):
            return pltpu.make_async_remote_copy(src_ref=q_msg.at[la], dst_ref=q_all.at[la, me], send_sem=qs_sem.at[la, i - 1],
                                                recv_sem=qr_sem.at[la, me], device_id={"a": dst}, device_id_type=MESH)

        def p_mate_send(la):
            return pltpu.make_async_remote_copy(src_ref=p_msg.at[la, 1 - core], dst_ref=p_mate.at[la], send_sem=pm_sem.at[la, 0],
                                                recv_sem=pm_sem.at[la, 1], device_id={"a": mate}, device_id_type=MESH)

        def p_send(la, other, i):
            return pltpu.make_async_remote_copy(src_ref=p_out.at[la, other], dst_ref=p_all.at[la, chip], send_sem=ps_sem.at[la, i],
                                                recv_sem=pr_sem.at[la, chip], device_id={"a": other * CORES + core}, device_id_type=MESH)

        def mate_send(la):
            return pltpu.make_async_remote_copy(src_ref=y_part.at[la, 1 - core], dst_ref=y_mate.at[la], send_sem=m_sem.at[la, 0],
                                                recv_sem=m_sem.at[la, 1], device_id={"a": mate}, device_id_type=MESH)

        def chip_copy(la, other, slot, i):
            return pltpu.make_async_remote_copy(src_ref=y_chip.at[la, slot], dst_ref=y_chip.at[la, slot], send_sem=ys_sem.at[la, i],
                                                recv_sem=yr_sem.at[la, slot], device_id={"a": other * CORES + core}, device_id_type=MESH)

        def pair_copy(side):
            near = near_g if side else near_f
            return pltpu.make_async_remote_copy(src_ref=y_chip.at[0, 2 * side], dst_ref=y_chip.at[0, 2 * side + 1], send_sem=ys_sem.at[0, side],
                                                recv_sem=yr_sem.at[0, side], device_id={"a": near * CORES + core}, device_id_type=MESH)

        def half_copy(la, slot):
            return pltpu.make_async_remote_copy(src_ref=y_half.at[la, slot], dst_ref=y_half.at[la, slot], send_sem=h_sem.at[la, 0],
                                                recv_sem=h_sem.at[la, 1], device_id={"a": mate}, device_id_type=MESH)

        others = [(lax.rem(chip + i, chips), i - 1) for i in range(1, chips)]

        def q_arrival(la, src):
            return pltpu.make_async_remote_copy(src_ref=q_msg.at[la], dst_ref=q_all.at[la, src], send_sem=qs_sem.at[la, 0],
                                                recv_sem=qr_sem.at[la, src], device_id={"a": src}, device_id_type=MESH)

        def p_arrival(la, other):
            return pltpu.make_async_remote_copy(src_ref=p_out.at[la, other], dst_ref=p_all.at[la, other], send_sem=ps_sem.at[la, 0],
                                                recv_sem=pr_sem.at[la, other], device_id={"a": other * CORES + core}, device_id_type=MESH)

        def peers():
            return [(lax.rem(me + i, n), i) for i in range(1, n)]

        def norm(x):
            total = jnp.sum(jnp.sum(x * x, axis=1, keepdims=True), axis=0, keepdims=True)
            return x * lax.rsqrt(total / self.d_model + NORM_EPS)

        cosine, sine = table[0:1, :], table[1:2, :]

        def tiled(piece):
            row = rows_like(ROW)
            out = jnp.zeros((8, ROW), jnp.float32)
            for i in range(self.chunks):
                out = jnp.where(row == i, piece(i), out)
            return out

        def gain(j):
            return tiled(lambda i: gain_b[j][i * ROW:(i + 1) * ROW].astype(jnp.float32).reshape(1, ROW))

        def rope(x):
            first, second = x[:, :half], x[:, half:]
            return jnp.concatenate([first * cosine - second * sine, second * cosine + first * sine], axis=1)

        def round_bf16(x):
            return x.astype(jnp.bfloat16).astype(jnp.float32)

        def project(la, hidden, pre):
            a = norm(hidden) * (1.0 + pre)
            for j in range(3):
                w_cp[la][j].wait()
            q = k = v = None
            for i in range(self.chunks):
                lhs = jnp.broadcast_to(a[i:i + 1, :], (16, ROW)).astype(jnp.bfloat16)
                part = [jnp.dot(lhs, w[la, i * ROW:(i + 1) * ROW, :], preferred_element_type=jnp.float32) for w in (wq_b, wk_b, wv_b)]
                q, k, v = part if q is None else (q + part[0], k + part[1], v + part[2])
            q, k, v = q[:2], k[:2], v[:2]
            q0, q1 = rope(q[:, :hd]), rope(q[:, hd:])
            q = round_bf16(jnp.where(lax.broadcasted_iota(jnp.int32, (2, hd), 0) == 0, q0, q1))
            return q, round_bf16(rope(k)), round_bf16(v)

        def attend_block(la, h, masked):
            q = q_all[la, h]
            s = lax.dot_general(q, kv_b[la, 0, h], (((1,), (1,)), ((), ())), preferred_element_type=jnp.float32)
            s = softcap(s, hd ** -0.5)
            if masked:
                pos = me * blk + lax.broadcasted_iota(jnp.int32, s.shape, 1)
                s = jnp.where(pos >= self.first_pos, s, NEG)
            top = jnp.max(s, axis=1, keepdims=True)
            e = jnp.exp(s - top)
            if masked:
                e = jnp.where(pos >= self.first_pos, e, 0.0)
            total = jnp.sum(e, axis=1, keepdims=True)
            o = jnp.dot(e.astype(jnp.bfloat16), kv_b[la, 1, h], preferred_element_type=jnp.float32)
            lane = lax.broadcasted_iota(jnp.int32, (2, 128), 1)
            p_msg[la, lax.rem(h, CORES), h // CORES, :, 0:hd] = o
            p_msg[la, lax.rem(h, CORES), h // CORES, :, hd:hd + 128] = jnp.where(lane < 64, top, total)

        def attend_all(la, masked):
            for cp in kv_cp[la]:
                cp.wait()

            def body(h, carry):
                attend_block(la, h, masked)
                return carry

            lax.fori_loop(0, n, body, 0)
            p_mate_send(la).start()
            p_mate_send(la).wait_recv()
            lane = lax.broadcasted_iota(jnp.int32, (2, 128), 1)
            for c in range(chips):
                top, total, o = merge([p_msg[la, core, c], p_mate[la, c]])
                p_out[la, c, :, 0:hd] = o
                p_out[la, c, :, hd:hd + 128] = jnp.where(lane < 64, top, total)
            for other, i in others:
                p_send(la, other, i).start()
            p_all[la, chip] = p_out[la, chip]

        def merge(parts):
            tops = [p[:, hd:hd + 1] for p in parts]
            top = functools.reduce(jnp.maximum, tops)
            weights = [jnp.exp(t - top) for t in tops]
            total = sum(w * p[:, hd + 64:hd + 65] for w, p in zip(weights, parts))
            return top, total, sum(w * p[:, 0:hd] for w, p in zip(weights, parts))

        def combine(la, q, k_new, v_new, first_chip):
            s_new = softcap(jnp.sum(q * k_new, axis=1, keepdims=True), hd ** -0.5)
            old_top, old_total, old_o = merge([p_all[la, c] for c in range(first_chip, chips)])
            top = jnp.maximum(s_new, old_top)
            e_new, w = jnp.exp(s_new - top), jnp.exp(old_top - top)
            return (round_bf16(e_new) * v_new + w * old_o) / (e_new + w * old_total)

        def out_project(la, o):
            w_cp[la][3].wait()
            lhs = [jnp.broadcast_to(o[g:g + 1, :], (16, hd)).astype(jnp.bfloat16) for g in range(self.q_groups)]
            row = rows_like(ROW)
            msg = jnp.zeros((8, ROW), jnp.float32)
            for i in range(self.chunks):
                y = None
                for g in range(self.q_groups):
                    part = jnp.dot(lhs[g], wo_b[la, g * hd:(g + 1) * hd, i * ROW:(i + 1) * ROW], preferred_element_type=jnp.float32)
                    y = part if y is None else y + part
                msg = jnp.where(row == i, y[:8], msg)
            y_part[la, 0] = msg[:4]
            y_part[la, 1] = msg[4:]
            mate_send(la).start()
            mate_send(la).wait_recv()
            if la == 0:
                y_chip[0, 0] = y_part[0, core] + y_mate[0]
                pair_copy(0).start()
                return
            y_chip[la, chip] = y_part[la, core] + y_mate[la]
            for other, i in others:
                chip_copy(la, other, chip, i).start()

        def stage(k):
            for step in range(SCHEDULE[k], SCHEDULE[k + 1]):
                bulk_start(step)
            for step in range(SCHEDULE[k - 1] if k else 0, SCHEDULE[k]):
                bulk_wait(step)

        hidden = tiled(lambda i: hid_b[:, i * ROW:(i + 1) * ROW].astype(jnp.float32))
        fresh = []
        for la in range(2):
            pre, post = gain(2 * la), gain(2 * la + 1)
            q, k_new, v_new = project(la, hidden, pre)
            fresh.append((k_new, v_new))
            q_msg[la] = q.astype(jnp.bfloat16)
            q_all[la, me] = q.astype(jnp.bfloat16)
            for dst, i in peers():
                @pl.when(jnp.logical_or(la == 1, dst >= self.first_src))
                def _():
                    q_send(la, dst, i).start()
            stage(4 * la)
            if la == 0:
                for cp in w_cp[1] + kv_cp[1]:
                    cp.start()
            if la == 0:
                @pl.when(has_loc)
                def _():
                    @pl.when(chip == late)
                    def _():
                        pl.semaphore_wait(go_sem, 1)

                    for src, i in peers():
                        q_arrival(0, src).wait_recv()
                    attend_all(0, True)
            else:
                for src, i in peers():
                    q_arrival(1, src).wait_recv()
                attend_all(1, False)
            stage(4 * la + 1)
            first_chip = self.first_src // CORES if la == 0 else 0
            for other, i in others:
                @pl.when(other >= first_chip)
                def _():
                    p_arrival(la, other).wait_recv()
            out_project(la, combine(la, q, k_new, v_new, first_chip))
            if la == 0:
                stage(2)
                pair_copy(0).wait_recv()
                y_chip[0, 2] = y_chip[0, 0] + y_chip[0, 1]
                pair_copy(1).start()
                stage(3)
            else:
                for later in range(SCHEDULE[6], steps - HOLD):
                    bulk_start(later)
                for later in range(steps - HOLD, steps):
                    bulk_start(later, slice(1, 2))
                for later in range(steps, 2 * steps):
                    bulk_start(later)
                for later in range(steps - HOLD, steps):
                    bulk_start(later, slice(0, 1))

                @pl.when(chip == relay_via)
                def _():
                    relay_send().wait_recv()
                    relay_forward(core, CORES - 1 - core).start()

            if la == 0:
                pair_copy(1).wait_recv()
                total = y_chip[0, 2] + y_chip[0, 3]
            else:
                for other, i in others:
                    chip_copy(la, other, other, i).wait_recv()
                total = y_chip[la, 0]
                for c in range(1, chips):
                    total = total + y_chip[la, c]
            y_half[la, core] = total
            half_copy(la, core).start()
            half_copy(la, 1 - core).wait_recv()
            y = jnp.concatenate([y_half[la, 0], y_half[la, 1]], axis=0)
            hidden = round_bf16(hidden + norm(y) * (1.0 + post))
        for i in range(self.chunks):
            hid_out[:, i * ROW:(i + 1) * ROW] = hidden[i:i + 1, :].astype(jnp.bfloat16)

        row16 = lax.broadcasted_iota(jnp.int32, (16, hd), 0)
        for kv, out in enumerate((gk_out, gv_out)):
            new = jnp.broadcast_to(fresh[1][kv][0:1], (16, hd))
            out[0, 0, self.seq:self.seq + 16, :] = jnp.where(row16 == 0, new, 0.0).astype(jnp.bfloat16)
            out[0, 0, self.seq + 16:self.slots, :] = jnp.zeros((self.slots - self.seq - 16, hd), jnp.bfloat16)

        for la in range(2):
            for dst, i in peers():
                @pl.when(jnp.logical_or(la == 1, dst >= self.first_src))
                def _():
                    q_send(la, dst, i).wait_send()
            mate_send(la).wait_send()
            if la == 0:
                pair_copy(0).wait_send()
                pair_copy(1).wait_send()
            else:
                for other, i in others:
                    chip_copy(la, other, chip, i).wait_send()
            half_copy(la, core).wait_send()
        p_mate_send(1).wait_send()
        for other, i in others:
            p_send(1, other, i).wait_send()

        @pl.when(has_loc)
        def _():
            p_mate_send(0).wait_send()
            for other, i in others:
                p_send(0, other, i).wait_send()
            for kv in range(2):
                loc_send(kv, mate, d_sem.at[1, kv]).wait_send()
                own_loc[kv].wait()

        for kv in range(2):
            glo_send(kv, mate, d_sem.at[0, kv]).wait_send()
            own_glo[kv].wait()

        def glo_arrival(kv, src_dev):
            src, out = glo_pairs[kv]
            return pltpu.make_async_remote_copy(src_ref=src.at[0, 0], dst_ref=glo_dst(out, src_dev), send_sem=d_sem.at[0, kv],
                                                recv_sem=glo_rsem.at[kv, src_dev], device_id={"a": src_dev}, device_id_type=MESH)

        def loc_arrival(kv, src_dev, lo=0):
            src, out = loc_pairs[kv]
            return pltpu.make_async_remote_copy(src_ref=src.at[0, 0, lo:], dst_ref=loc_dst(out, src_dev, lo), send_sem=d_sem.at[1, kv],
                                                recv_sem=loc_rsem.at[kv, src_dev], device_id={"a": src_dev}, device_id_type=MESH)

        for src_dev, i in peers():
            short = jnp.logical_and(chip == relay_to, src_dev == relay_from * CORES + (CORES - 1 - core))

            @pl.when(src_dev >= self.first_src)
            def _():
                loc_arrival(0, src_dev).wait_recv()

            @pl.when(jnp.logical_and(src_dev >= self.first_src, jnp.logical_not(short)))
            def _():
                loc_arrival(1, src_dev).wait_recv()

            @pl.when(short)
            def _():
                loc_arrival(1, src_dev, RELAY).wait_recv()

        @pl.when(chip == relay_from)
        def _():
            relay_send().wait_send()

        @pl.when(chip == relay_via)
        def _():
            relay_forward(core, CORES - 1 - core).wait_send()

        @pl.when(chip == relay_to)
        def _():
            relay_forward(CORES - 1 - core, core).wait_recv()

        slot = (self.seq % WINDOW) // 16 * 16
        for kv, out in enumerate((lk_out, lv_out)):
            new = jnp.broadcast_to(fresh[0][kv][0:1], (16, hd))
            old = out[0, 0, slot:slot + 16, :].astype(jnp.float32)
            out[0, 0, slot:slot + 16, :] = jnp.where(row16 == self.seq % WINDOW - slot, new, old).astype(jnp.bfloat16)

        for step in range(SCHEDULE[5], 2 * steps):
            bulk_wait(step)
        for c in (chip, near_f, opp, near_g):
            for src_dev in ([mate] if c is chip else cores_of(c)):
                for kv in range(2):
                    glo_arrival(kv, src_dev).wait_recv()


def solution(mesh):
    n = mesh.shape["a"]
    cache_in = P("dp", None, "a", None)
    cache_out = P("dp", "a", None, None)
    rows_spec = P("dp", None)
    layer_specs = (P(None, "a"), P(None, "a"), P(None, "a"), P("a", None), P(None), P(None))
    in_specs = (rows_spec, cache_in, cache_in, cache_in, cache_in) + layer_specs + layer_specs
    out_specs = (rows_spec, cache_out, cache_out, cache_out, cache_out)

    def device_step(hidden_in, loc_k, loc_v, glo_k, glo_v, loc_wq, loc_wk, loc_wv, loc_wo, loc_pre, loc_post, glo_wq, glo_wk, glo_wv, glo_wo, glo_pre, glo_post):
        d_model = hidden_in.shape[1]
        rows, heads, blk, hd = loc_k.shape
        q_cols, kv_cols = loc_wq.shape[1], loc_wk.shape[1]
        seq = n * blk
        slots = seq + CACHE_ROOM
        table = jnp.asarray(np.stack(rope_tables(hd, seq)))

        vmem = pl.BlockSpec(memory_space=pltpu.VMEM)
        hbm = pl.BlockSpec(memory_space=pltpu.HBM)
        bf16, f32 = jnp.bfloat16, jnp.float32
        dma = pltpu.SemaphoreType.DMA
        landed = pl.pallas_call(
            Kernel(n, d_model, heads, blk, hd, slots),
            name="decode_step",
            out_shape=(
                pltpu.VMEM(hidden_in.shape, bf16),
                pltpu.VMEM((rows, 1, WINDOW, hd), bf16),
                pltpu.VMEM((rows, 1, WINDOW, hd), bf16),
                pltpu.VMEM((rows, 1, slots, hd), bf16),
                pltpu.VMEM((rows, 1, slots, hd), bf16),
            ),
            in_specs=[hbm] * 18,
            out_specs=(vmem,) * 5,
            scratch_shapes=[
                pltpu.VMEM(hidden_in.shape, bf16),
                pltpu.VMEM((2, hd // 2), f32),
                [pltpu.VMEM((d_model,), bf16)] * 4,
                pltpu.VMEM((2, d_model, q_cols), bf16),
                pltpu.VMEM((2, d_model, kv_cols), bf16),
                pltpu.VMEM((2, d_model, kv_cols), bf16),
                pltpu.VMEM((2, q_cols, d_model), bf16),
                pltpu.VMEM((2, 2, heads, blk, hd), bf16),
                pltpu.VMEM((2, 2, hd), bf16),
                pltpu.VMEM((2, n, 2, hd), bf16),
                pltpu.VMEM((2, CORES, n // CORES, 2, hd + 128), f32),
                pltpu.VMEM((2, n // CORES, 2, hd + 128), f32),
                pltpu.VMEM((2, n // CORES, 2, hd + 128), f32),
                pltpu.VMEM((2, n // CORES, 2, hd + 128), f32),
                pltpu.VMEM((2, CORES, 4, ROW), f32),
                pltpu.VMEM((2, 4, ROW), f32),
                pltpu.VMEM((2, 4, 4, ROW), f32),
                pltpu.VMEM((2, CORES, 4, ROW), f32),
                pltpu.VMEM((RELAY, hd), bf16),
                dma((6,)), dma((16,)), dma((8,)), dma((2, 2)), dma((2, 2)), dma((2, n)), dma((2, n)), dma((2, 4)), dma((2, 2)),
                dma((2, n - 1)), dma((2, n)), dma((2, 2)), dma((2, 3)), dma((2, n // CORES)), dma((2, 2)), dma((2, 3)), dma((2, n // CORES)), dma((2, 2)), dma((4,)), pltpu.SemaphoreType.REGULAR,
            ],
            compiler_params=pltpu.CompilerParams(collective_id=0, has_side_effects=True, vmem_limit_bytes=48 * 2**20),
        )(hidden_in, table, loc_k, loc_v, glo_k, glo_v, loc_wq, loc_wk, loc_wv, loc_wo, loc_pre, loc_post, glo_wq, glo_wk, glo_wv, glo_wo, glo_pre, glo_post)
        return pl.pallas_call(
            store_outputs,
            name="store_outputs",
            out_shape=tuple(jax.ShapeDtypeStruct(x.shape, x.dtype) for x in landed),
            in_specs=[vmem] * 5,
            out_specs=(hbm,) * 5,
            scratch_shapes=[dma((5, STORE_PARTS))],
            compiler_params=pltpu.CompilerParams(vmem_limit_bytes=2**20),
        )(*landed)

    return jax.shard_map(device_step, mesh=mesh, in_specs=in_specs, out_specs=out_specs, check_vma=False)
```

```python
import functools

import jax
import jax.numpy as jnp
import numpy as np
from jax import lax
from jax.experimental import pallas as pl
from jax.experimental.pallas import tpu as pltpu
from jax.sharding import PartitionSpec as P

SOFTCAP = 50.0
NORM_EPS = 1e-6
ROPE_BASE = 10000.0
WINDOW = 4096
CACHE_ROOM = 512
MESH = pl.DeviceIdType.MESH
CORES = 2
ROW = 512
STORE_PARTS = 2
RELAY = 112
SCHEDULE = (1, 2, 3, 4, 5, 6, 7)
NEG = -1e30


def rope_tables(head_dim, position):
    half = head_dim // 2
    inv = np.float32(ROPE_BASE) ** (np.float32(-2.0) * np.arange(half, dtype=np.float32) / np.float32(head_dim))
    ang = np.float32(position) * inv.astype(np.float32)
    return np.cos(ang).astype(np.float32), np.sin(ang).astype(np.float32)


def softcap(scores, scale):
    return SOFTCAP * jnp.tanh(scores * scale / SOFTCAP)


def rows_like(width):
    return lax.broadcasted_iota(jnp.int32, (8, width), 0)


def store_outputs(*refs):
    landed, outs, sem = refs[:5], refs[5:10], refs[10]
    copies = [pltpu.make_async_copy(landed[0], outs[0], sem.at[0, 0])]
    for j in range(1, 5):
        part = landed[j].shape[2] // STORE_PARTS
        for p in range(STORE_PARTS):
            rows = pl.ds(p * part, part)
            copies.append(pltpu.make_async_copy(landed[j].at[0, 0, rows], outs[j].at[0, 0, rows], sem.at[j, p]))
    for cp in copies:
        cp.start()
    for cp in copies:
        cp.wait()


class Kernel:
    def __init__(self, n, d_model, heads, blk, hd, slots):
        self.n, self.d_model, self.heads, self.blk, self.hd, self.slots = n, d_model, heads, blk, hd, slots
        self.seq = n * blk
        self.first_pos = self.seq - WINDOW + 1
        self.first_src = self.first_pos // blk
        self.chunks = d_model // ROW
        self.q_groups = 2

    def __call__(self, hid_in, table_in, loc_k, loc_v, glo_k, glo_v, lwq, lwk, lwv, lwo, lpre, lpost, gwq, gwk, gwv, gwo, gpre, gpost,
                 hid_out, lk_out, lv_out, gk_out, gv_out,
                 hid_b, table, gain_b, wq_b, wk_b, wv_b, wo_b, kv_b, q_msg, q_all, p_msg, p_mate, p_out, p_all, y_part, y_mate, y_chip, y_half, relay_b,
                 in_sem, f_sem, g_sem, d_sem, own_sem, glo_rsem, loc_rsem, w_sem, kv_sem,
                 qs_sem, qr_sem, pm_sem, ps_sem, pr_sem, m_sem, ys_sem, yr_sem, h_sem, r_sem, go_sem):
        n, blk, hd = self.n, self.blk, self.hd
        half = hd // 2
        me = lax.axis_index("a")
        chips = n // CORES
        chip, core = me // CORES, lax.rem(me, CORES)
        has_loc = me >= self.first_src
        right, left, opp = [lax.rem(chip + i, chips) for i in (1, chips - 1, chips // 2)]
        even = lax.rem(chip, 2) == 0
        near_f = jnp.where(even, right, left)
        near_g = jnp.where(even, left, right)

        mate = chip * CORES + (CORES - 1 - core)

        relay_from, relay_via = chips // 2, chips // 2 - 1
        relay_to = (relay_from + chips // 2) % chips

        barrier = pltpu.get_barrier_semaphore()

        def greet(devices):
            for dev in devices:
                pl.semaphore_signal(barrier, inc=1, device_id={"a": dev}, device_id_type=MESH)

        def cores_of(c):
            return [c * CORES + j for j in range(CORES)]

        def tell(c):
            pl.semaphore_signal(go_sem, inc=1, device_id={"a": c * CORES + core}, device_id_type=MESH)

        late = chips - 1
        early_devices = list(range(self.first_src))

        @pl.when(jnp.logical_not(has_loc))
        def _():
            greet([mate] + cores_of(near_f) + cores_of(near_g))

        @pl.when(chip == late)
        def _():
            greet([mate] + early_devices)

        @pl.when(chip == relay_from)
        def _():
            greet(cores_of(late) + early_devices)

        weights = [((lwq, gwq), wq_b), ((lwk, gwk), wk_b), ((lwv, gwv), wv_b), ((lwo, gwo), wo_b)]
        w_cp = [[pltpu.make_async_copy(srcs[la], dst.at[la], w_sem.at[la, j]) for j, (srcs, dst) in enumerate(weights)] for la in range(2)]
        kv_cp = [[pltpu.make_async_copy(src.at[0], kv_b.at[la, j], kv_sem.at[la, j]) for j, src in enumerate(pair)]
                 for la, pair in enumerate(((loc_k, loc_v), (glo_k, glo_v)))]
        glo_pairs = ((glo_k, gk_out), (glo_v, gv_out))
        loc_pairs = ((loc_k, lk_out), (loc_v, lv_out))

        def glo_dst(out, src_dev):
            return out.at[0, 0, pl.ds(pl.multiple_of(src_dev * blk, blk), blk)]

        def loc_dst(out, src_dev, lo=0):
            if lo == 0:
                return out.at[0, 0, pl.ds(pl.multiple_of(lax.rem(src_dev * blk, WINDOW), blk), blk)]
            return out.at[0, 0, pl.ds(pl.multiple_of(lax.rem(src_dev * blk, WINDOW) + lo, 16), blk - lo)]

        in_cp = [pltpu.make_async_copy(hid_in, hid_b, in_sem.at[0]), pltpu.make_async_copy(table_in, table, in_sem.at[1])]
        in_cp += [pltpu.make_async_copy(g, b, in_sem.at[2 + j]) for j, (g, b) in enumerate(zip((lpre, lpost, gpre, gpost), gain_b))]
        for cp in in_cp + w_cp[0][:3]:
            cp.start()

        @pl.when(has_loc)
        def _():
            for cp in kv_cp[0]:
                cp.start()

        w_cp[0][3].start()

        @pl.when(jnp.logical_not(has_loc))
        def _():
            pl.semaphore_wait(barrier, n - 1)

        @pl.when(chip == late)
        def _():
            pl.semaphore_wait(barrier, 1 + 2 * CORES)
            tell(relay_from)

        def glo_send(kv, dst, sem):
            src, out = glo_pairs[kv]
            return pltpu.make_async_remote_copy(src_ref=src.at[0, dst], dst_ref=glo_dst(out, me), send_sem=sem,
                                                recv_sem=glo_rsem.at[kv, me], device_id={"a": dst}, device_id_type=MESH)

        def loc_send(kv, dst, sem, lo=0):
            src, out = loc_pairs[kv]
            return pltpu.make_async_remote_copy(src_ref=src.at[0, dst, lo:], dst_ref=loc_dst(out, me, lo), send_sem=sem,
                                                recv_sem=loc_rsem.at[kv, me], device_id={"a": dst}, device_id_type=MESH)

        def relay_send():
            dst = relay_to * CORES + (CORES - 1 - core)
            return pltpu.make_async_remote_copy(src_ref=loc_v.at[0, dst, pl.ds(0, RELAY)], dst_ref=relay_b, send_sem=r_sem.at[0],
                                                recv_sem=r_sem.at[1], device_id={"a": relay_via * CORES + core}, device_id_type=MESH)

        def relay_forward(src_core, dst_core):
            src_dev = relay_from * CORES + src_core
            dst_ref = lv_out.at[0, 0, pl.ds(pl.multiple_of(lax.rem(src_dev * blk, WINDOW), blk), RELAY)]
            return pltpu.make_async_remote_copy(src_ref=relay_b, dst_ref=dst_ref, send_sem=r_sem.at[2],
                                                recv_sem=r_sem.at[3], device_id={"a": relay_to * CORES + dst_core}, device_id_type=MESH)

        steps = 8

        def step_items(step):
            part = step // 2 if step < steps else step % 4
            kv, peer = part % 2, lax.rem(core + part // 2, CORES)
            if step >= steps:
                return kv, [(opp * CORES + peer, f_sem.at[step])]
            return kv, [(near_f * CORES + peer, f_sem.at[step]), (near_g * CORES + peer, g_sem.at[step])]

        def bulk(step, act, sides=slice(None)):
            kv, items = step_items(step)
            items = items[sides]
            if step >= 12 or (step < steps and step % 2 == 1):
                for dst, sem in items:
                    act(glo_send(kv, dst, sem))
            elif step == 11:
                (dst, sem), = items

                @pl.when(chip == relay_from)
                def _():
                    act(loc_send(kv, dst, sem, RELAY))

                @pl.when(jnp.logical_and(has_loc, chip != relay_from))
                def _():
                    act(loc_send(kv, dst, sem))
            else:
                @pl.when(has_loc)
                def _():
                    for dst, sem in items:
                        act(loc_send(kv, dst, sem))

        def bulk_start(step, sides=slice(None)):
            bulk(step, lambda cp: cp.start(), sides)

        def bulk_wait(step):
            bulk(step, lambda cp: cp.wait_send())

        @pl.when(chip == relay_from)
        def _():
            pl.semaphore_wait(barrier, CORES)
            relay_send().start()
            bulk_start(0, slice(1, 2))
            pl.semaphore_wait(go_sem, 1)
            tell(late)
            bulk_start(0, slice(0, 1))

        @pl.when(chip != relay_from)
        def _():
            bulk_start(0)

        own_glo = [pltpu.make_async_copy(src.at[0, me], glo_dst(out, me), own_sem.at[0, kv]) for kv, (src, out) in enumerate(glo_pairs)]
        own_loc = [pltpu.make_async_copy(src.at[0, me], loc_dst(out, me), own_sem.at[1, kv]) for kv, (src, out) in enumerate(loc_pairs)]
        for kv in range(2):
            glo_send(kv, mate, d_sem.at[0, kv]).start()
            own_glo[kv].start()

        @pl.when(has_loc)
        def _():
            for kv in range(2):
                loc_send(kv, mate, d_sem.at[1, kv]).start()
                own_loc[kv].start()

        for cp in in_cp:
            cp.wait()

        def q_send(la, dst, i):
            return pltpu.make_async_remote_copy(src_ref=q_msg.at[la], dst_ref=q_all.at[la, me], send_sem=qs_sem.at[la, i - 1],
                                                recv_sem=qr_sem.at[la, me], device_id={"a": dst}, device_id_type=MESH)

        def p_mate_send(la):
            return pltpu.make_async_remote_copy(src_ref=p_msg.at[la, 1 - core], dst_ref=p_mate.at[la], send_sem=pm_sem.at[la, 0],
                                                recv_sem=pm_sem.at[la, 1], device_id={"a": mate}, device_id_type=MESH)

        def p_send(la, other, i):
            return pltpu.make_async_remote_copy(src_ref=p_out.at[la, other], dst_ref=p_all.at[la, chip], send_sem=ps_sem.at[la, i],
                                                recv_sem=pr_sem.at[la, chip], device_id={"a": other * CORES + core}, device_id_type=MESH)

        def mate_send(la):
            return pltpu.make_async_remote_copy(src_ref=y_part.at[la, 1 - core], dst_ref=y_mate.at[la], send_sem=m_sem.at[la, 0],
                                                recv_sem=m_sem.at[la, 1], device_id={"a": mate}, device_id_type=MESH)

        def pair_copy(la, turn):
            near = near_f if turn else near_g
            return pltpu.make_async_remote_copy(src_ref=y_chip.at[la, 2 * turn], dst_ref=y_chip.at[la, 2 * turn + 1], send_sem=ys_sem.at[la, turn],
                                                recv_sem=yr_sem.at[la, turn], device_id={"a": near * CORES + core}, device_id_type=MESH)

        def half_copy(la, slot):
            return pltpu.make_async_remote_copy(src_ref=y_half.at[la, slot], dst_ref=y_half.at[la, slot], send_sem=h_sem.at[la, 0],
                                                recv_sem=h_sem.at[la, 1], device_id={"a": mate}, device_id_type=MESH)

        others = [(lax.rem(chip + i, chips), i - 1) for i in range(1, chips)]

        def q_arrival(la, src):
            return pltpu.make_async_remote_copy(src_ref=q_msg.at[la], dst_ref=q_all.at[la, src], send_sem=qs_sem.at[la, 0],
                                                recv_sem=qr_sem.at[la, src], device_id={"a": src}, device_id_type=MESH)

        def p_arrival(la, other):
            return pltpu.make_async_remote_copy(src_ref=p_out.at[la, other], dst_ref=p_all.at[la, other], send_sem=ps_sem.at[la, 0],
                                                recv_sem=pr_sem.at[la, other], device_id={"a": other * CORES + core}, device_id_type=MESH)

        def peers():
            return [(lax.rem(me + i, n), i) for i in range(1, n)]

        def norm(x):
            total = jnp.sum(jnp.sum(x * x, axis=1, keepdims=True), axis=0, keepdims=True)
            return x * lax.rsqrt(total / self.d_model + NORM_EPS)

        cosine, sine = table[0:1, :], table[1:2, :]

        def tiled(piece):
            row = rows_like(ROW)
            out = jnp.zeros((8, ROW), jnp.float32)
            for i in range(self.chunks):
                out = jnp.where(row == i, piece(i), out)
            return out

        def gain(j):
            return tiled(lambda i: gain_b[j][i * ROW:(i + 1) * ROW].astype(jnp.float32).reshape(1, ROW))

        def rope(x):
            first, second = x[:, :half], x[:, half:]
            return jnp.concatenate([first * cosine - second * sine, second * cosine + first * sine], axis=1)

        def round_bf16(x):
            return x.astype(jnp.bfloat16).astype(jnp.float32)

        def project(la, hidden, pre):
            a = norm(hidden) * (1.0 + pre)
            for j in range(3):
                w_cp[la][j].wait()
            q = k = v = None
            for i in range(self.chunks):
                lhs = jnp.broadcast_to(a[i:i + 1, :], (16, ROW)).astype(jnp.bfloat16)
                part = [jnp.dot(lhs, w[la, i * ROW:(i + 1) * ROW, :], preferred_element_type=jnp.float32) for w in (wq_b, wk_b, wv_b)]
                q, k, v = part if q is None else (q + part[0], k + part[1], v + part[2])
            q, k, v = q[:2], k[:2], v[:2]
            q0, q1 = rope(q[:, :hd]), rope(q[:, hd:])
            q = round_bf16(jnp.where(lax.broadcasted_iota(jnp.int32, (2, hd), 0) == 0, q0, q1))
            return q, round_bf16(rope(k)), round_bf16(v)

        def attend_block(la, h, masked):
            q = q_all[la, h]
            s = lax.dot_general(q, kv_b[la, 0, h], (((1,), (1,)), ((), ())), preferred_element_type=jnp.float32)
            s = softcap(s, hd ** -0.5)
            if masked:
                pos = me * blk + lax.broadcasted_iota(jnp.int32, s.shape, 1)
                s = jnp.where(pos >= self.first_pos, s, NEG)
            top = jnp.max(s, axis=1, keepdims=True)
            e = jnp.exp(s - top)
            if masked:
                e = jnp.where(pos >= self.first_pos, e, 0.0)
            total = jnp.sum(e, axis=1, keepdims=True)
            o = jnp.dot(e.astype(jnp.bfloat16), kv_b[la, 1, h], preferred_element_type=jnp.float32)
            lane = lax.broadcasted_iota(jnp.int32, (2, 128), 1)
            p_msg[la, lax.rem(h, CORES), h // CORES, :, 0:hd] = o
            p_msg[la, lax.rem(h, CORES), h // CORES, :, hd:hd + 128] = jnp.where(lane < 64, top, total)

        def attend_all(la, masked):
            for cp in kv_cp[la]:
                cp.wait()

            def body(h, carry):
                attend_block(la, h, masked)
                return carry

            lax.fori_loop(0, n, body, 0)
            p_mate_send(la).start()
            p_mate_send(la).wait_recv()
            lane = lax.broadcasted_iota(jnp.int32, (2, 128), 1)
            for c in range(chips):
                top, total, o = merge([p_msg[la, core, c], p_mate[la, c]])
                p_out[la, c, :, 0:hd] = o
                p_out[la, c, :, hd:hd + 128] = jnp.where(lane < 64, top, total)
            for other, i in others:
                p_send(la, other, i).start()
            p_all[la, chip] = p_out[la, chip]

        def merge(parts):
            tops = [p[:, hd:hd + 1] for p in parts]
            top = functools.reduce(jnp.maximum, tops)
            weights = [jnp.exp(t - top) for t in tops]
            total = sum(w * p[:, hd + 64:hd + 65] for w, p in zip(weights, parts))
            return top, total, sum(w * p[:, 0:hd] for w, p in zip(weights, parts))

        def combine(la, q, k_new, v_new, first_chip):
            s_new = softcap(jnp.sum(q * k_new, axis=1, keepdims=True), hd ** -0.5)
            old_top, old_total, old_o = merge([p_all[la, c] for c in range(first_chip, chips)])
            top = jnp.maximum(s_new, old_top)
            e_new, w = jnp.exp(s_new - top), jnp.exp(old_top - top)
            return (round_bf16(e_new) * v_new + w * old_o) / (e_new + w * old_total)

        def out_project(la, o):
            w_cp[la][3].wait()
            lhs = [jnp.broadcast_to(o[g:g + 1, :], (16, hd)).astype(jnp.bfloat16) for g in range(self.q_groups)]
            row = rows_like(ROW)
            msg = jnp.zeros((8, ROW), jnp.float32)
            for i in range(self.chunks):
                y = None
                for g in range(self.q_groups):
                    part = jnp.dot(lhs[g], wo_b[la, g * hd:(g + 1) * hd, i * ROW:(i + 1) * ROW], preferred_element_type=jnp.float32)
                    y = part if y is None else y + part
                msg = jnp.where(row == i, y[:8], msg)
            y_part[la, 0] = msg[:4]
            y_part[la, 1] = msg[4:]
            mate_send(la).start()
            mate_send(la).wait_recv()
            y_chip[la, 0] = y_part[la, core] + y_mate[la]
            pair_copy(la, 0).start()

        def stage(k):
            for step in range(SCHEDULE[k], SCHEDULE[k + 1]):
                bulk_start(step)
            for step in range(SCHEDULE[k - 1] if k else 0, SCHEDULE[k]):
                bulk_wait(step)

        hidden = tiled(lambda i: hid_b[:, i * ROW:(i + 1) * ROW].astype(jnp.float32))
        fresh = []
        for la in range(2):
            pre, post = gain(2 * la), gain(2 * la + 1)
            q, k_new, v_new = project(la, hidden, pre)
            fresh.append((k_new, v_new))
            q_msg[la] = q.astype(jnp.bfloat16)
            q_all[la, me] = q.astype(jnp.bfloat16)
            for dst, i in peers():
                @pl.when(jnp.logical_or(la == 1, dst >= self.first_src))
                def _():
                    q_send(la, dst, i).start()
            stage(4 * la)
            if la == 0:
                for cp in w_cp[1] + kv_cp[1]:
                    cp.start()
            if la == 0:
                @pl.when(has_loc)
                def _():
                    @pl.when(chip == late)
                    def _():
                        pl.semaphore_wait(go_sem, 1)

                    for src, i in peers():
                        q_arrival(0, src).wait_recv()
                    attend_all(0, True)
            else:
                for src, i in peers():
                    q_arrival(1, src).wait_recv()
                attend_all(1, False)
            stage(4 * la + 1)
            first_chip = self.first_src // CORES if la == 0 else 0
            for other, i in others:
                @pl.when(other >= first_chip)
                def _():
                    p_arrival(la, other).wait_recv()
            out_project(la, combine(la, q, k_new, v_new, first_chip))
            if la == 0:
                stage(2)
            else:
                bulk_start(steps - 1, slice(1, 2))
                for later in range(steps, 2 * steps):
                    bulk_start(later)
            pair_copy(la, 0).wait_recv()
            y_chip[la, 2] = y_chip[la, 0] + y_chip[la, 1]
            pair_copy(la, 1).start()
            if la == 0:
                stage(3)
            else:
                bulk_start(steps - 1, slice(0, 1))

                @pl.when(chip == relay_via)
                def _():
                    relay_send().wait_recv()
                    relay_forward(core, CORES - 1 - core).start()

            pair_copy(la, 1).wait_recv()
            total = y_chip[la, 2] + y_chip[la, 3]
            y_half[la, core] = total
            half_copy(la, core).start()
            half_copy(la, 1 - core).wait_recv()
            y = jnp.concatenate([y_half[la, 0], y_half[la, 1]], axis=0)
            hidden = round_bf16(hidden + norm(y) * (1.0 + post))
        for i in range(self.chunks):
            hid_out[:, i * ROW:(i + 1) * ROW] = hidden[i:i + 1, :].astype(jnp.bfloat16)

        row16 = lax.broadcasted_iota(jnp.int32, (16, hd), 0)
        for kv, out in enumerate((gk_out, gv_out)):
            new = jnp.broadcast_to(fresh[1][kv][0:1], (16, hd))
            out[0, 0, self.seq:self.seq + 16, :] = jnp.where(row16 == 0, new, 0.0).astype(jnp.bfloat16)
            out[0, 0, self.seq + 16:self.slots, :] = jnp.zeros((self.slots - self.seq - 16, hd), jnp.bfloat16)

        for la in range(2):
            for dst, i in peers():
                @pl.when(jnp.logical_or(la == 1, dst >= self.first_src))
                def _():
                    q_send(la, dst, i).wait_send()
            mate_send(la).wait_send()
            for turn in range(2):
                pair_copy(la, turn).wait_send()
            half_copy(la, core).wait_send()
        p_mate_send(1).wait_send()
        for other, i in others:
            p_send(1, other, i).wait_send()

        @pl.when(has_loc)
        def _():
            p_mate_send(0).wait_send()
            for other, i in others:
                p_send(0, other, i).wait_send()
            for kv in range(2):
                loc_send(kv, mate, d_sem.at[1, kv]).wait_send()
                own_loc[kv].wait()

        for kv in range(2):
            glo_send(kv, mate, d_sem.at[0, kv]).wait_send()
            own_glo[kv].wait()

        def glo_arrival(kv, src_dev):
            src, out = glo_pairs[kv]
            return pltpu.make_async_remote_copy(src_ref=src.at[0, 0], dst_ref=glo_dst(out, src_dev), send_sem=d_sem.at[0, kv],
                                                recv_sem=glo_rsem.at[kv, src_dev], device_id={"a": src_dev}, device_id_type=MESH)

        def loc_arrival(kv, src_dev, lo=0):
            src, out = loc_pairs[kv]
            return pltpu.make_async_remote_copy(src_ref=src.at[0, 0, lo:], dst_ref=loc_dst(out, src_dev, lo), send_sem=d_sem.at[1, kv],
                                                recv_sem=loc_rsem.at[kv, src_dev], device_id={"a": src_dev}, device_id_type=MESH)

        for src_dev, i in peers():
            short = jnp.logical_and(chip == relay_to, src_dev == relay_from * CORES + (CORES - 1 - core))

            @pl.when(src_dev >= self.first_src)
            def _():
                loc_arrival(0, src_dev).wait_recv()

            @pl.when(jnp.logical_and(src_dev >= self.first_src, jnp.logical_not(short)))
            def _():
                loc_arrival(1, src_dev).wait_recv()

            @pl.when(short)
            def _():
                loc_arrival(1, src_dev, RELAY).wait_recv()

        @pl.when(chip == relay_from)
        def _():
            relay_send().wait_send()

        @pl.when(chip == relay_via)
        def _():
            relay_forward(core, CORES - 1 - core).wait_send()

        @pl.when(chip == relay_to)
        def _():
            relay_forward(CORES - 1 - core, core).wait_recv()

        slot = (self.seq % WINDOW) // 16 * 16
        for kv, out in enumerate((lk_out, lv_out)):
            new = jnp.broadcast_to(fresh[0][kv][0:1], (16, hd))
            old = out[0, 0, slot:slot + 16, :].astype(jnp.float32)
            out[0, 0, slot:slot + 16, :] = jnp.where(row16 == self.seq % WINDOW - slot, new, old).astype(jnp.bfloat16)

        for step in range(SCHEDULE[5], 2 * steps):
            bulk_wait(step)
        for c in (chip, near_f, opp, near_g):
            for src_dev in ([mate] if c is chip else cores_of(c)):
                for kv in range(2):
                    glo_arrival(kv, src_dev).wait_recv()


def solution(mesh):
    n = mesh.shape["a"]
    cache_in = P("dp", None, "a", None)
    cache_out = P("dp", "a", None, None)
    rows_spec = P("dp", None)
    layer_specs = (P(None, "a"), P(None, "a"), P(None, "a"), P("a", None), P(None), P(None))
    in_specs = (rows_spec, cache_in, cache_in, cache_in, cache_in) + layer_specs + layer_specs
    out_specs = (rows_spec, cache_out, cache_out, cache_out, cache_out)

    def device_step(hidden_in, loc_k, loc_v, glo_k, glo_v, loc_wq, loc_wk, loc_wv, loc_wo, loc_pre, loc_post, glo_wq, glo_wk, glo_wv, glo_wo, glo_pre, glo_post):
        d_model = hidden_in.shape[1]
        rows, heads, blk, hd = loc_k.shape
        q_cols, kv_cols = loc_wq.shape[1], loc_wk.shape[1]
        seq = n * blk
        slots = seq + CACHE_ROOM
        table = jnp.asarray(np.stack(rope_tables(hd, seq)))

        vmem = pl.BlockSpec(memory_space=pltpu.VMEM)
        hbm = pl.BlockSpec(memory_space=pltpu.HBM)
        bf16, f32 = jnp.bfloat16, jnp.float32
        dma = pltpu.SemaphoreType.DMA
        landed = pl.pallas_call(
            Kernel(n, d_model, heads, blk, hd, slots),
            name="decode_step",
            out_shape=(
                pltpu.VMEM(hidden_in.shape, bf16),
                pltpu.VMEM((rows, 1, WINDOW, hd), bf16),
                pltpu.VMEM((rows, 1, WINDOW, hd), bf16),
                pltpu.VMEM((rows, 1, slots, hd), bf16),
                pltpu.VMEM((rows, 1, slots, hd), bf16),
            ),
            in_specs=[hbm] * 18,
            out_specs=(vmem,) * 5,
            scratch_shapes=[
                pltpu.VMEM(hidden_in.shape, bf16),
                pltpu.VMEM((2, hd // 2), f32),
                [pltpu.VMEM((d_model,), bf16)] * 4,
                pltpu.VMEM((2, d_model, q_cols), bf16),
                pltpu.VMEM((2, d_model, kv_cols), bf16),
                pltpu.VMEM((2, d_model, kv_cols), bf16),
                pltpu.VMEM((2, q_cols, d_model), bf16),
                pltpu.VMEM((2, 2, heads, blk, hd), bf16),
                pltpu.VMEM((2, 2, hd), bf16),
                pltpu.VMEM((2, n, 2, hd), bf16),
                pltpu.VMEM((2, CORES, n // CORES, 2, hd + 128), f32),
                pltpu.VMEM((2, n // CORES, 2, hd + 128), f32),
                pltpu.VMEM((2, n // CORES, 2, hd + 128), f32),
                pltpu.VMEM((2, n // CORES, 2, hd + 128), f32),
                pltpu.VMEM((2, CORES, 4, ROW), f32),
                pltpu.VMEM((2, 4, ROW), f32),
                pltpu.VMEM((2, 4, 4, ROW), f32),
                pltpu.VMEM((2, CORES, 4, ROW), f32),
                pltpu.VMEM((RELAY, hd), bf16),
                dma((6,)), dma((16,)), dma((8,)), dma((2, 2)), dma((2, 2)), dma((2, n)), dma((2, n)), dma((2, 4)), dma((2, 2)),
                dma((2, n - 1)), dma((2, n)), dma((2, 2)), dma((2, 3)), dma((2, n // CORES)), dma((2, 2)), dma((2, 2)), dma((2, 2)), dma((2, 2)), dma((4,)), pltpu.SemaphoreType.REGULAR,
            ],
            compiler_params=pltpu.CompilerParams(collective_id=0, has_side_effects=True, vmem_limit_bytes=48 * 2**20),
        )(hidden_in, table, loc_k, loc_v, glo_k, glo_v, loc_wq, loc_wk, loc_wv, loc_wo, loc_pre, loc_post, glo_wq, glo_wk, glo_wv, glo_wo, glo_pre, glo_post)
        return pl.pallas_call(
            store_outputs,
            name="store_outputs",
            out_shape=tuple(jax.ShapeDtypeStruct(x.shape, x.dtype) for x in landed),
            in_specs=[vmem] * 5,
            out_specs=(hbm,) * 5,
            scratch_shapes=[dma((5, STORE_PARTS))],
            compiler_params=pltpu.CompilerParams(vmem_limit_bytes=2**20),
        )(*landed)

    return jax.shard_map(device_step, mesh=mesh, in_specs=in_specs, out_specs=out_specs, check_vma=False)
```

```python
import functools

import jax
import jax.numpy as jnp
import numpy as np
from jax import lax
from jax.experimental import pallas as pl
from jax.experimental.pallas import tpu as pltpu
from jax.sharding import PartitionSpec as P

SOFTCAP = 50.0
NORM_EPS = 1e-6
ROPE_BASE = 10000.0
WINDOW = 4096
CACHE_ROOM = 512
MESH = pl.DeviceIdType.MESH
CORES = 2
ROW = 512
STORE_PARTS = 2
RELAY = 120
SCHEDULE = (1, 2, 3, 4, 5, 6, 7)
NEG = -1e30


def rope_tables(head_dim, position):
    half = head_dim // 2
    inv = np.float32(ROPE_BASE) ** (np.float32(-2.0) * np.arange(half, dtype=np.float32) / np.float32(head_dim))
    ang = np.float32(position) * inv.astype(np.float32)
    return np.cos(ang).astype(np.float32), np.sin(ang).astype(np.float32)


def softcap(scores, scale):
    return SOFTCAP * jnp.tanh(scores * scale / SOFTCAP)


def rows_like(width):
    return lax.broadcasted_iota(jnp.int32, (8, width), 0)


def store_outputs(*refs):
    landed, outs, sem = refs[:5], refs[5:10], refs[10]
    copies = [pltpu.make_async_copy(landed[0], outs[0], sem.at[0, 0])]
    for j in range(1, 5):
        part = landed[j].shape[2] // STORE_PARTS
        for p in range(STORE_PARTS):
            rows = pl.ds(p * part, part)
            copies.append(pltpu.make_async_copy(landed[j].at[0, 0, rows], outs[j].at[0, 0, rows], sem.at[j, p]))
    for cp in copies:
        cp.start()
    for cp in copies:
        cp.wait()


class Kernel:
    def __init__(self, n, d_model, heads, blk, hd, slots):
        self.n, self.d_model, self.heads, self.blk, self.hd, self.slots = n, d_model, heads, blk, hd, slots
        self.seq = n * blk
        self.first_pos = self.seq - WINDOW + 1
        self.first_src = self.first_pos // blk
        self.chunks = d_model // ROW
        self.q_groups = 2

    def __call__(self, hid_in, table_in, loc_k, loc_v, glo_k, glo_v, lwq, lwk, lwv, lwo, lpre, lpost, gwq, gwk, gwv, gwo, gpre, gpost,
                 hid_out, lk_out, lv_out, gk_out, gv_out,
                 hid_b, table, gain_b, wq_b, wk_b, wv_b, wo_b, kv_b, q_msg, q_all, p_msg, p_mate, p_out, p_all, y_part, y_mate, y_chip, y_half, relay_b,
                 in_sem, f_sem, g_sem, d_sem, own_sem, glo_rsem, loc_rsem, w_sem, kv_sem,
                 qs_sem, qr_sem, pm_sem, ps_sem, pr_sem, m_sem, ys_sem, yr_sem, h_sem, r_sem, go_sem):
        n, blk, hd = self.n, self.blk, self.hd
        half = hd // 2
        me = lax.axis_index("a")
        chips = n // CORES
        chip, core = me // CORES, lax.rem(me, CORES)
        has_loc = me >= self.first_src
        right, left, opp = [lax.rem(chip + i, chips) for i in (1, chips - 1, chips // 2)]
        even = lax.rem(chip, 2) == 0
        near_f = jnp.where(even, right, left)
        near_g = jnp.where(even, left, right)

        mate = chip * CORES + (CORES - 1 - core)

        relay_from, relay_via = chips // 2, chips // 2 - 1
        relay_to = (relay_from + chips // 2) % chips

        barrier = pltpu.get_barrier_semaphore()

        def greet(devices):
            for dev in devices:
                pl.semaphore_signal(barrier, inc=1, device_id={"a": dev}, device_id_type=MESH)

        def cores_of(c):
            return [c * CORES + j for j in range(CORES)]

        def tell(c):
            pl.semaphore_signal(go_sem, inc=1, device_id={"a": c * CORES + core}, device_id_type=MESH)

        late = chips - 1
        early_devices = list(range(self.first_src))

        @pl.when(jnp.logical_not(has_loc))
        def _():
            greet([mate] + cores_of(near_f) + cores_of(near_g))

        @pl.when(chip == late)
        def _():
            greet([mate] + early_devices)

        @pl.when(chip == relay_from)
        def _():
            greet(cores_of(late) + early_devices)

        weights = [((lwq, gwq), wq_b), ((lwk, gwk), wk_b), ((lwv, gwv), wv_b), ((lwo, gwo), wo_b)]
        w_cp = [[pltpu.make_async_copy(srcs[la], dst.at[la], w_sem.at[la, j]) for j, (srcs, dst) in enumerate(weights)] for la in range(2)]
        kv_cp = [[pltpu.make_async_copy(src.at[0], kv_b.at[la, j], kv_sem.at[la, j]) for j, src in enumerate(pair)]
                 for la, pair in enumerate(((loc_k, loc_v), (glo_k, glo_v)))]
        glo_pairs = ((glo_k, gk_out), (glo_v, gv_out))
        loc_pairs = ((loc_k, lk_out), (loc_v, lv_out))

        def glo_dst(out, src_dev):
            return out.at[0, 0, pl.ds(pl.multiple_of(src_dev * blk, blk), blk)]

        def loc_dst(out, src_dev, lo=0):
            if lo == 0:
                return out.at[0, 0, pl.ds(pl.multiple_of(lax.rem(src_dev * blk, WINDOW), blk), blk)]
            return out.at[0, 0, pl.ds(pl.multiple_of(lax.rem(src_dev * blk, WINDOW) + lo, 8), blk - lo)]

        in_cp = [pltpu.make_async_copy(hid_in, hid_b, in_sem.at[0]), pltpu.make_async_copy(table_in, table, in_sem.at[1])]
        in_cp += [pltpu.make_async_copy(g, b, in_sem.at[2 + j]) for j, (g, b) in enumerate(zip((lpre, lpost, gpre, gpost), gain_b))]
        for cp in in_cp + w_cp[0][:3]:
            cp.start()

        @pl.when(has_loc)
        def _():
            for cp in kv_cp[0]:
                cp.start()

        w_cp[0][3].start()

        @pl.when(jnp.logical_not(has_loc))
        def _():
            pl.semaphore_wait(barrier, n - 1)

        @pl.when(chip == late)
        def _():
            pl.semaphore_wait(barrier, 1 + 2 * CORES)
            tell(relay_from)

        def glo_send(kv, dst, sem):
            src, out = glo_pairs[kv]
            return pltpu.make_async_remote_copy(src_ref=src.at[0, dst], dst_ref=glo_dst(out, me), send_sem=sem,
                                                recv_sem=glo_rsem.at[kv, me], device_id={"a": dst}, device_id_type=MESH)

        def loc_send(kv, dst, sem, lo=0):
            src, out = loc_pairs[kv]
            return pltpu.make_async_remote_copy(src_ref=src.at[0, dst, lo:], dst_ref=loc_dst(out, me, lo), send_sem=sem,
                                                recv_sem=loc_rsem.at[kv, me], device_id={"a": dst}, device_id_type=MESH)

        def relay_send():
            dst = relay_to * CORES + (CORES - 1 - core)
            return pltpu.make_async_remote_copy(src_ref=loc_v.at[0, dst, pl.ds(0, RELAY)], dst_ref=relay_b, send_sem=r_sem.at[0],
                                                recv_sem=r_sem.at[1], device_id={"a": relay_via * CORES + core}, device_id_type=MESH)

        def relay_forward(src_core, dst_core):
            src_dev = relay_from * CORES + src_core
            dst_ref = lv_out.at[0, 0, pl.ds(pl.multiple_of(lax.rem(src_dev * blk, WINDOW), blk), RELAY)]
            return pltpu.make_async_remote_copy(src_ref=relay_b, dst_ref=dst_ref, send_sem=r_sem.at[2],
                                                recv_sem=r_sem.at[3], device_id={"a": relay_to * CORES + dst_core}, device_id_type=MESH)

        steps = 8

        def step_items(step):
            part = step // 2 if step < steps else step % 4
            kv, peer = part % 2, lax.rem(core + part // 2, CORES)
            if step >= steps:
                return kv, [(opp * CORES + peer, f_sem.at[step])]
            return kv, [(near_f * CORES + peer, f_sem.at[step]), (near_g * CORES + peer, g_sem.at[step])]

        def bulk(step, act, sides=slice(None)):
            kv, items = step_items(step)
            items = items[sides]
            if step >= 12 or (step < steps and step % 2 == 1):
                for dst, sem in items:
                    act(glo_send(kv, dst, sem))
            elif step == 11:
                (dst, sem), = items

                @pl.when(chip == relay_from)
                def _():
                    act(loc_send(kv, dst, sem, RELAY))

                @pl.when(jnp.logical_and(has_loc, chip != relay_from))
                def _():
                    act(loc_send(kv, dst, sem))
            else:
                @pl.when(has_loc)
                def _():
                    for dst, sem in items:
                        act(loc_send(kv, dst, sem))

        def bulk_start(step, sides=slice(None)):
            bulk(step, lambda cp: cp.start(), sides)

        def bulk_wait(step):
            bulk(step, lambda cp: cp.wait_send())

        @pl.when(chip == relay_from)
        def _():
            pl.semaphore_wait(barrier, CORES)
            relay_send().start()
            bulk_start(0, slice(1, 2))
            pl.semaphore_wait(go_sem, 1)
            tell(late)
            bulk_start(0, slice(0, 1))

        @pl.when(chip != relay_from)
        def _():
            bulk_start(0)

        own_glo = [pltpu.make_async_copy(src.at[0, me], glo_dst(out, me), own_sem.at[0, kv]) for kv, (src, out) in enumerate(glo_pairs)]
        own_loc = [pltpu.make_async_copy(src.at[0, me], loc_dst(out, me), own_sem.at[1, kv]) for kv, (src, out) in enumerate(loc_pairs)]
        for kv in range(2):
            glo_send(kv, mate, d_sem.at[0, kv]).start()
            own_glo[kv].start()

        @pl.when(has_loc)
        def _():
            for kv in range(2):
                loc_send(kv, mate, d_sem.at[1, kv]).start()
                own_loc[kv].start()

        for cp in in_cp:
            cp.wait()

        def q_send(la, dst, i):
            return pltpu.make_async_remote_copy(src_ref=q_msg.at[la], dst_ref=q_all.at[la, me], send_sem=qs_sem.at[la, i - 1],
                                                recv_sem=qr_sem.at[la, me], device_id={"a": dst}, device_id_type=MESH)

        def p_mate_send(la):
            return pltpu.make_async_remote_copy(src_ref=p_msg.at[la, 1 - core], dst_ref=p_mate.at[la], send_sem=pm_sem.at[la, 0],
                                                recv_sem=pm_sem.at[la, 1], device_id={"a": mate}, device_id_type=MESH)

        def p_send(la, other, i):
            return pltpu.make_async_remote_copy(src_ref=p_out.at[la, other], dst_ref=p_all.at[la, chip], send_sem=ps_sem.at[la, i],
                                                recv_sem=pr_sem.at[la, chip], device_id={"a": other * CORES + core}, device_id_type=MESH)

        def mate_send(la):
            return pltpu.make_async_remote_copy(src_ref=y_part.at[la, 1 - core], dst_ref=y_mate.at[la], send_sem=m_sem.at[la, 0],
                                                recv_sem=m_sem.at[la, 1], device_id={"a": mate}, device_id_type=MESH)

        def pair_copy(la, turn):
            near = near_f if turn else near_g
            return pltpu.make_async_remote_copy(src_ref=y_chip.at[la, 2 * turn], dst_ref=y_chip.at[la, 2 * turn + 1], send_sem=ys_sem.at[la, turn],
                                                recv_sem=yr_sem.at[la, turn], device_id={"a": near * CORES + core}, device_id_type=MESH)

        def half_copy(la, slot):
            return pltpu.make_async_remote_copy(src_ref=y_half.at[la, slot], dst_ref=y_half.at[la, slot], send_sem=h_sem.at[la, 0],
                                                recv_sem=h_sem.at[la, 1], device_id={"a": mate}, device_id_type=MESH)

        others = [(lax.rem(chip + i, chips), i - 1) for i in range(1, chips)]

        def q_arrival(la, src):
            return pltpu.make_async_remote_copy(src_ref=q_msg.at[la], dst_ref=q_all.at[la, src], send_sem=qs_sem.at[la, 0],
                                                recv_sem=qr_sem.at[la, src], device_id={"a": src}, device_id_type=MESH)

        def p_arrival(la, other):
            return pltpu.make_async_remote_copy(src_ref=p_out.at[la, other], dst_ref=p_all.at[la, other], send_sem=ps_sem.at[la, 0],
                                                recv_sem=pr_sem.at[la, other], device_id={"a": other * CORES + core}, device_id_type=MESH)

        def peers():
            return [(lax.rem(me + i, n), i) for i in range(1, n)]

        def norm(x):
            total = jnp.sum(jnp.sum(x * x, axis=1, keepdims=True), axis=0, keepdims=True)
            return x * lax.rsqrt(total / self.d_model + NORM_EPS)

        cosine, sine = table[0:1, :], table[1:2, :]

        def tiled(piece):
            row = rows_like(ROW)
            out = jnp.zeros((8, ROW), jnp.float32)
            for i in range(self.chunks):
                out = jnp.where(row == i, piece(i), out)
            return out

        def gain(j):
            return tiled(lambda i: gain_b[j][i * ROW:(i + 1) * ROW].astype(jnp.float32).reshape(1, ROW))

        def rope(x):
            first, second = x[:, :half], x[:, half:]
            return jnp.concatenate([first * cosine - second * sine, second * cosine + first * sine], axis=1)

        def round_bf16(x):
            return x.astype(jnp.bfloat16).astype(jnp.float32)

        def project(la, hidden, pre):
            a = norm(hidden) * (1.0 + pre)
            for j in range(3):
                w_cp[la][j].wait()
            q = k = v = None
            for i in range(self.chunks):
                lhs = jnp.broadcast_to(a[i:i + 1, :], (16, ROW)).astype(jnp.bfloat16)
                part = [jnp.dot(lhs, w[la, i * ROW:(i + 1) * ROW, :], preferred_element_type=jnp.float32) for w in (wq_b, wk_b, wv_b)]
                q, k, v = part if q is None else (q + part[0], k + part[1], v + part[2])
            q, k, v = q[:2], k[:2], v[:2]
            q0, q1 = rope(q[:, :hd]), rope(q[:, hd:])
            q = round_bf16(jnp.where(lax.broadcasted_iota(jnp.int32, (2, hd), 0) == 0, q0, q1))
            return q, round_bf16(rope(k)), round_bf16(v)

        def attend_block(la, h, masked):
            q = q_all[la, h]
            s = lax.dot_general(q, kv_b[la, 0, h], (((1,), (1,)), ((), ())), preferred_element_type=jnp.float32)
            s = softcap(s, hd ** -0.5)
            if masked:
                pos = me * blk + lax.broadcasted_iota(jnp.int32, s.shape, 1)
                s = jnp.where(pos >= self.first_pos, s, NEG)
            top = jnp.max(s, axis=1, keepdims=True)
            e = jnp.exp(s - top)
            if masked:
                e = jnp.where(pos >= self.first_pos, e, 0.0)
            total = jnp.sum(e, axis=1, keepdims=True)
            o = jnp.dot(e.astype(jnp.bfloat16), kv_b[la, 1, h], preferred_element_type=jnp.float32)
            lane = lax.broadcasted_iota(jnp.int32, (2, 128), 1)
            p_msg[la, lax.rem(h, CORES), h // CORES, :, 0:hd] = o
            p_msg[la, lax.rem(h, CORES), h // CORES, :, hd:hd + 128] = jnp.where(lane < 64, top, total)

        def attend_all(la, masked):
            for cp in kv_cp[la]:
                cp.wait()

            def body(h, carry):
                attend_block(la, h, masked)
                return carry

            lax.fori_loop(0, n, body, 0)
            p_mate_send(la).start()
            p_mate_send(la).wait_recv()
            lane = lax.broadcasted_iota(jnp.int32, (2, 128), 1)
            for c in range(chips):
                top, total, o = merge([p_msg[la, core, c], p_mate[la, c]])
                p_out[la, c, :, 0:hd] = o
                p_out[la, c, :, hd:hd + 128] = jnp.where(lane < 64, top, total)
            for other, i in others:
                p_send(la, other, i).start()
            p_all[la, chip] = p_out[la, chip]

        def merge(parts):
            tops = [p[:, hd:hd + 1] for p in parts]
            top = functools.reduce(jnp.maximum, tops)
            weights = [jnp.exp(t - top) for t in tops]
            total = sum(w * p[:, hd + 64:hd + 65] for w, p in zip(weights, parts))
            return top, total, sum(w * p[:, 0:hd] for w, p in zip(weights, parts))

        def combine(la, q, k_new, v_new, first_chip):
            s_new = softcap(jnp.sum(q * k_new, axis=1, keepdims=True), hd ** -0.5)
            old_top, old_total, old_o = merge([p_all[la, c] for c in range(first_chip, chips)])
            top = jnp.maximum(s_new, old_top)
            e_new, w = jnp.exp(s_new - top), jnp.exp(old_top - top)
            return (round_bf16(e_new) * v_new + w * old_o) / (e_new + w * old_total)

        def out_project(la, o):
            w_cp[la][3].wait()
            lhs = [jnp.broadcast_to(o[g:g + 1, :], (16, hd)).astype(jnp.bfloat16) for g in range(self.q_groups)]
            row = rows_like(ROW)
            msg = jnp.zeros((8, ROW), jnp.float32)
            for i in range(self.chunks):
                y = None
                for g in range(self.q_groups):
                    part = jnp.dot(lhs[g], wo_b[la, g * hd:(g + 1) * hd, i * ROW:(i + 1) * ROW], preferred_element_type=jnp.float32)
                    y = part if y is None else y + part
                msg = jnp.where(row == i, y[:8], msg)
            y_part[la, 0] = msg[:4]
            y_part[la, 1] = msg[4:]
            mate_send(la).start()
            mate_send(la).wait_recv()
            y_chip[la, 0] = y_part[la, core] + y_mate[la]
            pair_copy(la, 0).start()

        def stage(k):
            for step in range(SCHEDULE[k], SCHEDULE[k + 1]):
                bulk_start(step)
            for step in range(SCHEDULE[k - 1] if k else 0, SCHEDULE[k]):
                bulk_wait(step)

        hidden = tiled(lambda i: hid_b[:, i * ROW:(i + 1) * ROW].astype(jnp.float32))
        fresh = []
        for la in range(2):
            pre, post = gain(2 * la), gain(2 * la + 1)
            q, k_new, v_new = project(la, hidden, pre)
            fresh.append((k_new, v_new))
            q_msg[la] = q.astype(jnp.bfloat16)
            q_all[la, me] = q.astype(jnp.bfloat16)
            for dst, i in peers():
                @pl.when(jnp.logical_or(la == 1, dst >= self.first_src))
                def _():
                    q_send(la, dst, i).start()
            stage(4 * la)
            if la == 0:
                for cp in w_cp[1] + kv_cp[1]:
                    cp.start()
            if la == 0:
                @pl.when(has_loc)
                def _():
                    @pl.when(chip == late)
                    def _():
                        pl.semaphore_wait(go_sem, 1)

                    for src, i in peers():
                        q_arrival(0, src).wait_recv()
                    attend_all(0, True)
            else:
                for src, i in peers():
                    q_arrival(1, src).wait_recv()
                attend_all(1, False)
            stage(4 * la + 1)
            first_chip = self.first_src // CORES if la == 0 else 0
            for other, i in others:
                @pl.when(other >= first_chip)
                def _():
                    p_arrival(la, other).wait_recv()
            out_project(la, combine(la, q, k_new, v_new, first_chip))
            if la == 0:
                stage(2)
            else:
                bulk_start(steps - 1, slice(1, 2))
                for later in range(steps, 2 * steps):
                    bulk_start(later)
            pair_copy(la, 0).wait_recv()
            y_chip[la, 2] = y_chip[la, 0] + y_chip[la, 1]
            pair_copy(la, 1).start()
            if la == 0:
                stage(3)
            else:
                bulk_start(steps - 1, slice(0, 1))

                @pl.when(chip == relay_via)
                def _():
                    relay_send().wait_recv()
                    relay_forward(core, CORES - 1 - core).start()

            pair_copy(la, 1).wait_recv()
            total = y_chip[la, 2] + y_chip[la, 3]
            y_half[la, core] = total
            half_copy(la, core).start()
            half_copy(la, 1 - core).wait_recv()
            y = jnp.concatenate([y_half[la, 0], y_half[la, 1]], axis=0)
            hidden = round_bf16(hidden + norm(y) * (1.0 + post))
        for i in range(self.chunks):
            hid_out[:, i * ROW:(i + 1) * ROW] = hidden[i:i + 1, :].astype(jnp.bfloat16)

        row16 = lax.broadcasted_iota(jnp.int32, (16, hd), 0)
        for kv, out in enumerate((gk_out, gv_out)):
            new = jnp.broadcast_to(fresh[1][kv][0:1], (16, hd))
            out[0, 0, self.seq:self.seq + 16, :] = jnp.where(row16 == 0, new, 0.0).astype(jnp.bfloat16)
            out[0, 0, self.seq + 16:self.slots, :] = jnp.zeros((self.slots - self.seq - 16, hd), jnp.bfloat16)

        for la in range(2):
            for dst, i in peers():
                @pl.when(jnp.logical_or(la == 1, dst >= self.first_src))
                def _():
                    q_send(la, dst, i).wait_send()
            mate_send(la).wait_send()
            for turn in range(2):
                pair_copy(la, turn).wait_send()
            half_copy(la, core).wait_send()
        p_mate_send(1).wait_send()
        for other, i in others:
            p_send(1, other, i).wait_send()

        @pl.when(has_loc)
        def _():
            p_mate_send(0).wait_send()
            for other, i in others:
                p_send(0, other, i).wait_send()
            for kv in range(2):
                loc_send(kv, mate, d_sem.at[1, kv]).wait_send()
                own_loc[kv].wait()

        for kv in range(2):
            glo_send(kv, mate, d_sem.at[0, kv]).wait_send()
            own_glo[kv].wait()

        def glo_arrival(kv, src_dev):
            src, out = glo_pairs[kv]
            return pltpu.make_async_remote_copy(src_ref=src.at[0, 0], dst_ref=glo_dst(out, src_dev), send_sem=d_sem.at[0, kv],
                                                recv_sem=glo_rsem.at[kv, src_dev], device_id={"a": src_dev}, device_id_type=MESH)

        def loc_arrival(kv, src_dev, lo=0):
            src, out = loc_pairs[kv]
            return pltpu.make_async_remote_copy(src_ref=src.at[0, 0, lo:], dst_ref=loc_dst(out, src_dev, lo), send_sem=d_sem.at[1, kv],
                                                recv_sem=loc_rsem.at[kv, src_dev], device_id={"a": src_dev}, device_id_type=MESH)

        for src_dev, i in peers():
            short = jnp.logical_and(chip == relay_to, src_dev == relay_from * CORES + (CORES - 1 - core))

            @pl.when(src_dev >= self.first_src)
            def _():
                loc_arrival(0, src_dev).wait_recv()

            @pl.when(jnp.logical_and(src_dev >= self.first_src, jnp.logical_not(short)))
            def _():
                loc_arrival(1, src_dev).wait_recv()

            @pl.when(short)
            def _():
                loc_arrival(1, src_dev, RELAY).wait_recv()

        @pl.when(chip == relay_from)
        def _():
            relay_send().wait_send()

        @pl.when(chip == relay_via)
        def _():
            relay_forward(core, CORES - 1 - core).wait_send()

        @pl.when(chip == relay_to)
        def _():
            relay_forward(CORES - 1 - core, core).wait_recv()

        slot = (self.seq % WINDOW) // 16 * 16
        for kv, out in enumerate((lk_out, lv_out)):
            new = jnp.broadcast_to(fresh[0][kv][0:1], (16, hd))
            old = out[0, 0, slot:slot + 16, :].astype(jnp.float32)
            out[0, 0, slot:slot + 16, :] = jnp.where(row16 == self.seq % WINDOW - slot, new, old).astype(jnp.bfloat16)

        for step in range(SCHEDULE[5], 2 * steps):
            bulk_wait(step)
        for c in (chip, near_f, opp, near_g):
            for src_dev in ([mate] if c is chip else cores_of(c)):
                for kv in range(2):
                    glo_arrival(kv, src_dev).wait_recv()


def solution(mesh):
    n = mesh.shape["a"]
    cache_in = P("dp", None, "a", None)
    cache_out = P("dp", "a", None, None)
    rows_spec = P("dp", None)
    layer_specs = (P(None, "a"), P(None, "a"), P(None, "a"), P("a", None), P(None), P(None))
    in_specs = (rows_spec, cache_in, cache_in, cache_in, cache_in) + layer_specs + layer_specs
    out_specs = (rows_spec, cache_out, cache_out, cache_out, cache_out)

    def device_step(hidden_in, loc_k, loc_v, glo_k, glo_v, loc_wq, loc_wk, loc_wv, loc_wo, loc_pre, loc_post, glo_wq, glo_wk, glo_wv, glo_wo, glo_pre, glo_post):
        d_model = hidden_in.shape[1]
        rows, heads, blk, hd = loc_k.shape
        q_cols, kv_cols = loc_wq.shape[1], loc_wk.shape[1]
        seq = n * blk
        slots = seq + CACHE_ROOM
        table = jnp.asarray(np.stack(rope_tables(hd, seq)))

        vmem = pl.BlockSpec(memory_space=pltpu.VMEM)
        hbm = pl.BlockSpec(memory_space=pltpu.HBM)
        bf16, f32 = jnp.bfloat16, jnp.float32
        dma = pltpu.SemaphoreType.DMA
        landed = pl.pallas_call(
            Kernel(n, d_model, heads, blk, hd, slots),
            name="decode_step",
            out_shape=(
                pltpu.VMEM(hidden_in.shape, bf16),
                pltpu.VMEM((rows, 1, WINDOW, hd), bf16),
                pltpu.VMEM((rows, 1, WINDOW, hd), bf16),
                pltpu.VMEM((rows, 1, slots, hd), bf16),
                pltpu.VMEM((rows, 1, slots, hd), bf16),
            ),
            in_specs=[hbm] * 18,
            out_specs=(vmem,) * 5,
            scratch_shapes=[
                pltpu.VMEM(hidden_in.shape, bf16),
                pltpu.VMEM((2, hd // 2), f32),
                [pltpu.VMEM((d_model,), bf16)] * 4,
                pltpu.VMEM((2, d_model, q_cols), bf16),
                pltpu.VMEM((2, d_model, kv_cols), bf16),
                pltpu.VMEM((2, d_model, kv_cols), bf16),
                pltpu.VMEM((2, q_cols, d_model), bf16),
                pltpu.VMEM((2, 2, heads, blk, hd), bf16),
                pltpu.VMEM((2, 2, hd), bf16),
                pltpu.VMEM((2, n, 2, hd), bf16),
                pltpu.VMEM((2, CORES, n // CORES, 2, hd + 128), f32),
                pltpu.VMEM((2, n // CORES, 2, hd + 128), f32),
                pltpu.VMEM((2, n // CORES, 2, hd + 128), f32),
                pltpu.VMEM((2, n // CORES, 2, hd + 128), f32),
                pltpu.VMEM((2, CORES, 4, ROW), f32),
                pltpu.VMEM((2, 4, ROW), f32),
                pltpu.VMEM((2, 4, 4, ROW), f32),
                pltpu.VMEM((2, CORES, 4, ROW), f32),
                pltpu.VMEM((RELAY, hd), bf16),
                dma((6,)), dma((16,)), dma((8,)), dma((2, 2)), dma((2, 2)), dma((2, n)), dma((2, n)), dma((2, 4)), dma((2, 2)),
                dma((2, n - 1)), dma((2, n)), dma((2, 2)), dma((2, 3)), dma((2, n // CORES)), dma((2, 2)), dma((2, 2)), dma((2, 2)), dma((2, 2)), dma((4,)), pltpu.SemaphoreType.REGULAR,
            ],
            compiler_params=pltpu.CompilerParams(collective_id=0, has_side_effects=True, vmem_limit_bytes=48 * 2**20),
        )(hidden_in, table, loc_k, loc_v, glo_k, glo_v, loc_wq, loc_wk, loc_wv, loc_wo, loc_pre, loc_post, glo_wq, glo_wk, glo_wv, glo_wo, glo_pre, glo_post)
        return pl.pallas_call(
            store_outputs,
            name="store_outputs",
            out_shape=tuple(jax.ShapeDtypeStruct(x.shape, x.dtype) for x in landed),
            in_specs=[vmem] * 5,
            out_specs=(hbm,) * 5,
            scratch_shapes=[dma((5, STORE_PARTS))],
            compiler_params=pltpu.CompilerParams(vmem_limit_bytes=2**20),
        )(*landed)

    return jax.shard_map(device_step, mesh=mesh, in_specs=in_specs, out_specs=out_specs, check_vma=False)
```

```python
import functools

import jax
import jax.numpy as jnp
import numpy as np
from jax import lax
from jax.experimental import pallas as pl
from jax.experimental.pallas import tpu as pltpu
from jax.sharding import PartitionSpec as P

SOFTCAP = 50.0
NORM_EPS = 1e-6
ROPE_BASE = 10000.0
WINDOW = 4096
CACHE_ROOM = 512
MESH = pl.DeviceIdType.MESH
CORES = 2
ROW = 512
STORE_PARTS = 2
RELAY = 120
SCHEDULE = (1, 2, 3, 4, 5, 6, 7)
NEG = -1e30


def rope_tables(head_dim, position):
    half = head_dim // 2
    inv = np.float32(ROPE_BASE) ** (np.float32(-2.0) * np.arange(half, dtype=np.float32) / np.float32(head_dim))
    ang = np.float32(position) * inv.astype(np.float32)
    return np.cos(ang).astype(np.float32), np.sin(ang).astype(np.float32)


def softcap(scores, scale):
    return SOFTCAP * jnp.tanh(scores * scale / SOFTCAP)


def rows_like(width):
    return lax.broadcasted_iota(jnp.int32, (8, width), 0)


def store_outputs(*refs):
    landed, outs, sem = refs[:5], refs[5:10], refs[10]
    copies = [pltpu.make_async_copy(landed[0], outs[0], sem.at[0, 0])]
    for j in range(1, 5):
        part = landed[j].shape[2] // STORE_PARTS
        for p in range(STORE_PARTS):
            rows = pl.ds(p * part, part)
            copies.append(pltpu.make_async_copy(landed[j].at[0, 0, rows], outs[j].at[0, 0, rows], sem.at[j, p]))
    for cp in reversed(copies):
        cp.start()
    for cp in copies:
        cp.wait()


class Kernel:
    def __init__(self, n, d_model, heads, blk, hd, slots):
        self.n, self.d_model, self.heads, self.blk, self.hd, self.slots = n, d_model, heads, blk, hd, slots
        self.seq = n * blk
        self.first_pos = self.seq - WINDOW + 1
        self.first_src = self.first_pos // blk
        self.chunks = d_model // ROW
        self.q_groups = 2

    def __call__(self, hid_in, table_in, loc_k, loc_v, glo_k, glo_v, lwq, lwk, lwv, lwo, lpre, lpost, gwq, gwk, gwv, gwo, gpre, gpost,
                 hid_out, lk_out, lv_out, gk_out, gv_out,
                 hid_b, table, gain_b, wq_b, wk_b, wv_b, wo_b, kv_b, q_msg, q_all, p_msg, p_mate, p_out, p_all, y_part, y_mate, y_chip, y_half, relay_b,
                 in_sem, f_sem, g_sem, d_sem, own_sem, glo_rsem, loc_rsem, w_sem, kv_sem,
                 qs_sem, qr_sem, pm_sem, ps_sem, pr_sem, m_sem, ys_sem, yr_sem, h_sem, r_sem, go_sem):
        n, blk, hd = self.n, self.blk, self.hd
        half = hd // 2
        me = lax.axis_index("a")
        chips = n // CORES
        chip, core = me // CORES, lax.rem(me, CORES)
        has_loc = me >= self.first_src
        right, left, opp = [lax.rem(chip + i, chips) for i in (1, chips - 1, chips // 2)]
        even = lax.rem(chip, 2) == 0
        near_f = jnp.where(even, right, left)
        near_g = jnp.where(even, left, right)

        mate = chip * CORES + (CORES - 1 - core)

        relay_from, relay_via = chips // 2, chips // 2 - 1
        relay_to = (relay_from + chips // 2) % chips

        barrier = pltpu.get_barrier_semaphore()

        def greet(devices):
            for dev in devices:
                pl.semaphore_signal(barrier, inc=1, device_id={"a": dev}, device_id_type=MESH)

        def cores_of(c):
            return [c * CORES + j for j in range(CORES)]

        def tell(c):
            pl.semaphore_signal(go_sem, inc=1, device_id={"a": c * CORES + core}, device_id_type=MESH)

        late = chips - 1
        early_devices = list(range(self.first_src))

        @pl.when(jnp.logical_not(has_loc))
        def _():
            greet([mate] + cores_of(near_f) + cores_of(near_g))

        @pl.when(chip == late)
        def _():
            greet([mate] + early_devices)

        @pl.when(chip == relay_from)
        def _():
            greet(cores_of(late) + early_devices)

        weights = [((lwq, gwq), wq_b), ((lwk, gwk), wk_b), ((lwv, gwv), wv_b), ((lwo, gwo), wo_b)]
        w_cp = [[pltpu.make_async_copy(srcs[la], dst.at[la], w_sem.at[la, j]) for j, (srcs, dst) in enumerate(weights)] for la in range(2)]
        kv_cp = [[pltpu.make_async_copy(src.at[0], kv_b.at[la, j], kv_sem.at[la, j]) for j, src in enumerate(pair)]
                 for la, pair in enumerate(((loc_k, loc_v), (glo_k, glo_v)))]
        glo_pairs = ((glo_k, gk_out), (glo_v, gv_out))
        loc_pairs = ((loc_k, lk_out), (loc_v, lv_out))

        def glo_dst(out, src_dev):
            return out.at[0, 0, pl.ds(pl.multiple_of(src_dev * blk, blk), blk)]

        def loc_dst(out, src_dev, lo=0):
            if lo == 0:
                return out.at[0, 0, pl.ds(pl.multiple_of(lax.rem(src_dev * blk, WINDOW), blk), blk)]
            return out.at[0, 0, pl.ds(pl.multiple_of(lax.rem(src_dev * blk, WINDOW) + lo, 8), blk - lo)]

        in_cp = [pltpu.make_async_copy(hid_in, hid_b, in_sem.at[0]), pltpu.make_async_copy(table_in, table, in_sem.at[1])]
        in_cp += [pltpu.make_async_copy(g, b, in_sem.at[2 + j]) for j, (g, b) in enumerate(zip((lpre, lpost, gpre, gpost), gain_b))]
        for cp in in_cp + w_cp[0][:3]:
            cp.start()

        @pl.when(has_loc)
        def _():
            for cp in kv_cp[0]:
                cp.start()

        w_cp[0][3].start()

        @pl.when(jnp.logical_not(has_loc))
        def _():
            pl.semaphore_wait(barrier, n - 1)

        @pl.when(chip == late)
        def _():
            pl.semaphore_wait(barrier, 1 + 2 * CORES)
            tell(relay_from)

        def glo_send(kv, dst, sem):
            src, out = glo_pairs[kv]
            return pltpu.make_async_remote_copy(src_ref=src.at[0, dst], dst_ref=glo_dst(out, me), send_sem=sem,
                                                recv_sem=glo_rsem.at[kv, me], device_id={"a": dst}, device_id_type=MESH)

        def loc_send(kv, dst, sem, lo=0):
            src, out = loc_pairs[kv]
            return pltpu.make_async_remote_copy(src_ref=src.at[0, dst, lo:], dst_ref=loc_dst(out, me, lo), send_sem=sem,
                                                recv_sem=loc_rsem.at[kv, me], device_id={"a": dst}, device_id_type=MESH)

        def relay_send():
            dst = relay_to * CORES + (CORES - 1 - core)
            return pltpu.make_async_remote_copy(src_ref=loc_v.at[0, dst, pl.ds(0, RELAY)], dst_ref=relay_b, send_sem=r_sem.at[0],
                                                recv_sem=r_sem.at[1], device_id={"a": relay_via * CORES + core}, device_id_type=MESH)

        def relay_forward(src_core, dst_core):
            src_dev = relay_from * CORES + src_core
            dst_ref = lv_out.at[0, 0, pl.ds(pl.multiple_of(lax.rem(src_dev * blk, WINDOW), blk), RELAY)]
            return pltpu.make_async_remote_copy(src_ref=relay_b, dst_ref=dst_ref, send_sem=r_sem.at[2],
                                                recv_sem=r_sem.at[3], device_id={"a": relay_to * CORES + dst_core}, device_id_type=MESH)

        steps = 8

        def step_items(step):
            part = step // 2 if step < steps else step % 4
            kv, peer = part % 2, lax.rem(core + part // 2, CORES)
            if step >= steps:
                return kv, [(opp * CORES + peer, f_sem.at[step])]
            return kv, [(near_f * CORES + peer, f_sem.at[step]), (near_g * CORES + peer, g_sem.at[step])]

        def bulk(step, act, sides=slice(None)):
            kv, items = step_items(step)
            items = items[sides]
            if step >= 12 or (step < steps and step % 2 == 1):
                for dst, sem in items:
                    act(glo_send(kv, dst, sem))
            elif step == 11:
                (dst, sem), = items

                @pl.when(chip == relay_from)
                def _():
                    act(loc_send(kv, dst, sem, RELAY))

                @pl.when(jnp.logical_and(has_loc, chip != relay_from))
                def _():
                    act(loc_send(kv, dst, sem))
            else:
                @pl.when(has_loc)
                def _():
                    for dst, sem in items:
                        act(loc_send(kv, dst, sem))

        def bulk_start(step, sides=slice(None)):
            bulk(step, lambda cp: cp.start(), sides)

        def bulk_wait(step):
            bulk(step, lambda cp: cp.wait_send())

        @pl.when(chip == relay_from)
        def _():
            pl.semaphore_wait(barrier, CORES)
            relay_send().start()
            bulk_start(0, slice(1, 2))
            pl.semaphore_wait(go_sem, 1)
            tell(late)
            bulk_start(0, slice(0, 1))

        @pl.when(chip != relay_from)
        def _():
            bulk_start(0)

        own_glo = [pltpu.make_async_copy(src.at[0, me], glo_dst(out, me), own_sem.at[0, kv]) for kv, (src, out) in enumerate(glo_pairs)]
        own_loc = [pltpu.make_async_copy(src.at[0, me], loc_dst(out, me), own_sem.at[1, kv]) for kv, (src, out) in enumerate(loc_pairs)]
        for kv in range(2):
            glo_send(kv, mate, d_sem.at[0, kv]).start()
            own_glo[kv].start()

        @pl.when(has_loc)
        def _():
            for kv in range(2):
                loc_send(kv, mate, d_sem.at[1, kv]).start()
                own_loc[kv].start()

        for cp in in_cp:
            cp.wait()

        def q_send(la, dst, i):
            return pltpu.make_async_remote_copy(src_ref=q_msg.at[la], dst_ref=q_all.at[la, me], send_sem=qs_sem.at[la, i - 1],
                                                recv_sem=qr_sem.at[la, me], device_id={"a": dst}, device_id_type=MESH)

        def p_mate_send(la):
            return pltpu.make_async_remote_copy(src_ref=p_msg.at[la, 1 - core], dst_ref=p_mate.at[la], send_sem=pm_sem.at[la, 0],
                                                recv_sem=pm_sem.at[la, 1], device_id={"a": mate}, device_id_type=MESH)

        def p_send(la, other, i):
            return pltpu.make_async_remote_copy(src_ref=p_out.at[la, other], dst_ref=p_all.at[la, chip], send_sem=ps_sem.at[la, i],
                                                recv_sem=pr_sem.at[la, chip], device_id={"a": other * CORES + core}, device_id_type=MESH)

        def mate_send(la):
            return pltpu.make_async_remote_copy(src_ref=y_part.at[la, 1 - core], dst_ref=y_mate.at[la], send_sem=m_sem.at[la, 0],
                                                recv_sem=m_sem.at[la, 1], device_id={"a": mate}, device_id_type=MESH)

        def pair_copy(la, turn):
            near = near_f if turn else near_g
            return pltpu.make_async_remote_copy(src_ref=y_chip.at[la, 2 * turn], dst_ref=y_chip.at[la, 2 * turn + 1], send_sem=ys_sem.at[la, turn],
                                                recv_sem=yr_sem.at[la, turn], device_id={"a": near * CORES + core}, device_id_type=MESH)

        def half_copy(la, slot):
            return pltpu.make_async_remote_copy(src_ref=y_half.at[la, slot], dst_ref=y_half.at[la, slot], send_sem=h_sem.at[la, 0],
                                                recv_sem=h_sem.at[la, 1], device_id={"a": mate}, device_id_type=MESH)

        others = [(lax.rem(chip + i, chips), i - 1) for i in range(1, chips)]

        def q_arrival(la, src):
            return pltpu.make_async_remote_copy(src_ref=q_msg.at[la], dst_ref=q_all.at[la, src], send_sem=qs_sem.at[la, 0],
                                                recv_sem=qr_sem.at[la, src], device_id={"a": src}, device_id_type=MESH)

        def p_arrival(la, other):
            return pltpu.make_async_remote_copy(src_ref=p_out.at[la, other], dst_ref=p_all.at[la, other], send_sem=ps_sem.at[la, 0],
                                                recv_sem=pr_sem.at[la, other], device_id={"a": other * CORES + core}, device_id_type=MESH)

        def peers():
            return [(lax.rem(me + i, n), i) for i in range(1, n)]

        def norm(x):
            total = jnp.sum(jnp.sum(x * x, axis=1, keepdims=True), axis=0, keepdims=True)
            return x * lax.rsqrt(total / self.d_model + NORM_EPS)

        cosine, sine = table[0:1, :], table[1:2, :]

        def tiled(piece):
            row = rows_like(ROW)
            out = jnp.zeros((8, ROW), jnp.float32)
            for i in range(self.chunks):
                out = jnp.where(row == i, piece(i), out)
            return out

        def gain(j):
            return tiled(lambda i: gain_b[j][i * ROW:(i + 1) * ROW].astype(jnp.float32).reshape(1, ROW))

        def rope(x):
            first, second = x[:, :half], x[:, half:]
            return jnp.concatenate([first * cosine - second * sine, second * cosine + first * sine], axis=1)

        def round_bf16(x):
            return x.astype(jnp.bfloat16).astype(jnp.float32)

        def project(la, hidden, pre):
            a = norm(hidden) * (1.0 + pre)
            for j in range(3):
                w_cp[la][j].wait()
            q = k = v = None
            for i in range(self.chunks):
                lhs = jnp.broadcast_to(a[i:i + 1, :], (16, ROW)).astype(jnp.bfloat16)
                part = [jnp.dot(lhs, w[la, i * ROW:(i + 1) * ROW, :], preferred_element_type=jnp.float32) for w in (wq_b, wk_b, wv_b)]
                q, k, v = part if q is None else (q + part[0], k + part[1], v + part[2])
            q, k, v = q[:2], k[:2], v[:2]
            q0, q1 = rope(q[:, :hd]), rope(q[:, hd:])
            q = round_bf16(jnp.where(lax.broadcasted_iota(jnp.int32, (2, hd), 0) == 0, q0, q1))
            return q, round_bf16(rope(k)), round_bf16(v)

        def attend_block(la, h, masked):
            q = q_all[la, h]
            s = lax.dot_general(q, kv_b[la, 0, h], (((1,), (1,)), ((), ())), preferred_element_type=jnp.float32)
            s = softcap(s, hd ** -0.5)
            if masked:
                pos = me * blk + lax.broadcasted_iota(jnp.int32, s.shape, 1)
                s = jnp.where(pos >= self.first_pos, s, NEG)
            top = jnp.max(s, axis=1, keepdims=True)
            e = jnp.exp(s - top)
            if masked:
                e = jnp.where(pos >= self.first_pos, e, 0.0)
            total = jnp.sum(e, axis=1, keepdims=True)
            o = jnp.dot(e.astype(jnp.bfloat16), kv_b[la, 1, h], preferred_element_type=jnp.float32)
            lane = lax.broadcasted_iota(jnp.int32, (2, 128), 1)
            p_msg[la, lax.rem(h, CORES), h // CORES, :, 0:hd] = o
            p_msg[la, lax.rem(h, CORES), h // CORES, :, hd:hd + 128] = jnp.where(lane < 64, top, total)

        def attend_all(la, masked):
            for cp in kv_cp[la]:
                cp.wait()

            def body(h, carry):
                attend_block(la, h, masked)
                return carry

            lax.fori_loop(0, n, body, 0)
            p_mate_send(la).start()
            p_mate_send(la).wait_recv()
            lane = lax.broadcasted_iota(jnp.int32, (2, 128), 1)
            for c in range(chips):
                top, total, o = merge([p_msg[la, core, c], p_mate[la, c]])
                p_out[la, c, :, 0:hd] = o
                p_out[la, c, :, hd:hd + 128] = jnp.where(lane < 64, top, total)
            for other, i in others:
                p_send(la, other, i).start()
            p_all[la, chip] = p_out[la, chip]

        def merge(parts):
            tops = [p[:, hd:hd + 1] for p in parts]
            top = functools.reduce(jnp.maximum, tops)
            weights = [jnp.exp(t - top) for t in tops]
            total = sum(w * p[:, hd + 64:hd + 65] for w, p in zip(weights, parts))
            return top, total, sum(w * p[:, 0:hd] for w, p in zip(weights, parts))

        def combine(la, q, k_new, v_new, first_chip):
            s_new = softcap(jnp.sum(q * k_new, axis=1, keepdims=True), hd ** -0.5)
            old_top, old_total, old_o = merge([p_all[la, c] for c in range(first_chip, chips)])
            top = jnp.maximum(s_new, old_top)
            e_new, w = jnp.exp(s_new - top), jnp.exp(old_top - top)
            return (round_bf16(e_new) * v_new + w * old_o) / (e_new + w * old_total)

        def out_project(la, o):
            w_cp[la][3].wait()
            lhs = [jnp.broadcast_to(o[g:g + 1, :], (16, hd)).astype(jnp.bfloat16) for g in range(self.q_groups)]
            row = rows_like(ROW)
            msg = jnp.zeros((8, ROW), jnp.float32)
            for i in range(self.chunks):
                y = None
                for g in range(self.q_groups):
                    part = jnp.dot(lhs[g], wo_b[la, g * hd:(g + 1) * hd, i * ROW:(i + 1) * ROW], preferred_element_type=jnp.float32)
                    y = part if y is None else y + part
                msg = jnp.where(row == i, y[:8], msg)
            y_part[la, 0] = msg[:4]
            y_part[la, 1] = msg[4:]
            mate_send(la).start()
            mate_send(la).wait_recv()
            y_chip[la, 0] = y_part[la, core] + y_mate[la]
            pair_copy(la, 0).start()

        def stage(k):
            for step in range(SCHEDULE[k], SCHEDULE[k + 1]):
                bulk_start(step)
            for step in range(SCHEDULE[k - 1] if k else 0, SCHEDULE[k]):
                bulk_wait(step)

        hidden = tiled(lambda i: hid_b[:, i * ROW:(i + 1) * ROW].astype(jnp.float32))
        fresh = []
        for la in range(2):
            pre, post = gain(2 * la), gain(2 * la + 1)
            q, k_new, v_new = project(la, hidden, pre)
            fresh.append((k_new, v_new))
            q_msg[la] = q.astype(jnp.bfloat16)
            q_all[la, me] = q.astype(jnp.bfloat16)
            for dst, i in peers():
                @pl.when(jnp.logical_or(la == 1, dst >= self.first_src))
                def _():
                    q_send(la, dst, i).start()
            stage(4 * la)
            if la == 0:
                for cp in w_cp[1] + kv_cp[1]:
                    cp.start()
            if la == 0:
                @pl.when(has_loc)
                def _():
                    @pl.when(chip == late)
                    def _():
                        pl.semaphore_wait(go_sem, 1)

                    for src, i in peers():
                        q_arrival(0, src).wait_recv()
                    attend_all(0, True)
            else:
                for src, i in peers():
                    q_arrival(1, src).wait_recv()
                attend_all(1, False)
            stage(4 * la + 1)
            first_chip = self.first_src // CORES if la == 0 else 0
            for other, i in others:
                @pl.when(other >= first_chip)
                def _():
                    p_arrival(la, other).wait_recv()
            out_project(la, combine(la, q, k_new, v_new, first_chip))
            if la == 0:
                stage(2)
            else:
                bulk_start(steps - 1, slice(1, 2))
                for later in range(steps, 2 * steps):
                    bulk_start(later)
            pair_copy(la, 0).wait_recv()
            y_chip[la, 2] = y_chip[la, 0] + y_chip[la, 1]
            pair_copy(la, 1).start()
            if la == 0:
                stage(3)
            else:
                bulk_start(steps - 1, slice(0, 1))

                @pl.when(chip == relay_via)
                def _():
                    relay_send().wait_recv()
                    relay_forward(core, CORES - 1 - core).start()

            pair_copy(la, 1).wait_recv()
            total = y_chip[la, 2] + y_chip[la, 3]
            y_half[la, core] = total
            half_copy(la, core).start()
            half_copy(la, 1 - core).wait_recv()
            y = jnp.concatenate([y_half[la, 0], y_half[la, 1]], axis=0)
            hidden = round_bf16(hidden + norm(y) * (1.0 + post))
        for i in range(self.chunks):
            hid_out[:, i * ROW:(i + 1) * ROW] = hidden[i:i + 1, :].astype(jnp.bfloat16)

        row16 = lax.broadcasted_iota(jnp.int32, (16, hd), 0)
        for kv, out in enumerate((gk_out, gv_out)):
            new = jnp.broadcast_to(fresh[1][kv][0:1], (16, hd))
            out[0, 0, self.seq:self.seq + 16, :] = jnp.where(row16 == 0, new, 0.0).astype(jnp.bfloat16)
            out[0, 0, self.seq + 16:self.slots, :] = jnp.zeros((self.slots - self.seq - 16, hd), jnp.bfloat16)

        for la in range(2):
            for dst, i in peers():
                @pl.when(jnp.logical_or(la == 1, dst >= self.first_src))
                def _():
                    q_send(la, dst, i).wait_send()
            mate_send(la).wait_send()
            for turn in range(2):
                pair_copy(la, turn).wait_send()
            half_copy(la, core).wait_send()
        p_mate_send(1).wait_send()
        for other, i in others:
            p_send(1, other, i).wait_send()

        @pl.when(has_loc)
        def _():
            p_mate_send(0).wait_send()
            for other, i in others:
                p_send(0, other, i).wait_send()
            for kv in range(2):
                loc_send(kv, mate, d_sem.at[1, kv]).wait_send()
                own_loc[kv].wait()

        for kv in range(2):
            glo_send(kv, mate, d_sem.at[0, kv]).wait_send()
            own_glo[kv].wait()

        def glo_arrival(kv, src_dev):
            src, out = glo_pairs[kv]
            return pltpu.make_async_remote_copy(src_ref=src.at[0, 0], dst_ref=glo_dst(out, src_dev), send_sem=d_sem.at[0, kv],
                                                recv_sem=glo_rsem.at[kv, src_dev], device_id={"a": src_dev}, device_id_type=MESH)

        def loc_arrival(kv, src_dev, lo=0):
            src, out = loc_pairs[kv]
            return pltpu.make_async_remote_copy(src_ref=src.at[0, 0, lo:], dst_ref=loc_dst(out, src_dev, lo), send_sem=d_sem.at[1, kv],
                                                recv_sem=loc_rsem.at[kv, src_dev], device_id={"a": src_dev}, device_id_type=MESH)

        for src_dev, i in peers():
            short = jnp.logical_and(chip == relay_to, src_dev == relay_from * CORES + (CORES - 1 - core))

            @pl.when(src_dev >= self.first_src)
            def _():
                loc_arrival(0, src_dev).wait_recv()

            @pl.when(jnp.logical_and(src_dev >= self.first_src, jnp.logical_not(short)))
            def _():
                loc_arrival(1, src_dev).wait_recv()

            @pl.when(short)
            def _():
                loc_arrival(1, src_dev, RELAY).wait_recv()

        @pl.when(chip == relay_from)
        def _():
            relay_send().wait_send()

        @pl.when(chip == relay_via)
        def _():
            relay_forward(core, CORES - 1 - core).wait_send()

        @pl.when(chip == relay_to)
        def _():
            relay_forward(CORES - 1 - core, core).wait_recv()

        slot = (self.seq % WINDOW) // 16 * 16
        for kv, out in enumerate((lk_out, lv_out)):
            new = jnp.broadcast_to(fresh[0][kv][0:1], (16, hd))
            old = out[0, 0, slot:slot + 16, :].astype(jnp.float32)
            out[0, 0, slot:slot + 16, :] = jnp.where(row16 == self.seq % WINDOW - slot, new, old).astype(jnp.bfloat16)

        for step in range(SCHEDULE[5], 2 * steps):
            bulk_wait(step)
        for c in (chip, near_f, opp, near_g):
            for src_dev in ([mate] if c is chip else cores_of(c)):
                for kv in range(2):
                    glo_arrival(kv, src_dev).wait_recv()


def solution(mesh):
    n = mesh.shape["a"]
    cache_in = P("dp", None, "a", None)
    cache_out = P("dp", "a", None, None)
    rows_spec = P("dp", None)
    layer_specs = (P(None, "a"), P(None, "a"), P(None, "a"), P("a", None), P(None), P(None))
    in_specs = (rows_spec, cache_in, cache_in, cache_in, cache_in) + layer_specs + layer_specs
    out_specs = (rows_spec, cache_out, cache_out, cache_out, cache_out)

    def device_step(hidden_in, loc_k, loc_v, glo_k, glo_v, loc_wq, loc_wk, loc_wv, loc_wo, loc_pre, loc_post, glo_wq, glo_wk, glo_wv, glo_wo, glo_pre, glo_post):
        d_model = hidden_in.shape[1]
        rows, heads, blk, hd = loc_k.shape
        q_cols, kv_cols = loc_wq.shape[1], loc_wk.shape[1]
        seq = n * blk
        slots = seq + CACHE_ROOM
        table = jnp.asarray(np.stack(rope_tables(hd, seq)))

        vmem = pl.BlockSpec(memory_space=pltpu.VMEM)
        hbm = pl.BlockSpec(memory_space=pltpu.HBM)
        bf16, f32 = jnp.bfloat16, jnp.float32
        dma = pltpu.SemaphoreType.DMA
        landed = pl.pallas_call(
            Kernel(n, d_model, heads, blk, hd, slots),
            name="decode_step",
            out_shape=(
                pltpu.VMEM(hidden_in.shape, bf16),
                pltpu.VMEM((rows, 1, WINDOW, hd), bf16),
                pltpu.VMEM((rows, 1, WINDOW, hd), bf16),
                pltpu.VMEM((rows, 1, slots, hd), bf16),
                pltpu.VMEM((rows, 1, slots, hd), bf16),
            ),
            in_specs=[hbm] * 18,
            out_specs=(vmem,) * 5,
            scratch_shapes=[
                pltpu.VMEM(hidden_in.shape, bf16),
                pltpu.VMEM((2, hd // 2), f32),
                [pltpu.VMEM((d_model,), bf16)] * 4,
                pltpu.VMEM((2, d_model, q_cols), bf16),
                pltpu.VMEM((2, d_model, kv_cols), bf16),
                pltpu.VMEM((2, d_model, kv_cols), bf16),
                pltpu.VMEM((2, q_cols, d_model), bf16),
                pltpu.VMEM((2, 2, heads, blk, hd), bf16),
                pltpu.VMEM((2, 2, hd), bf16),
                pltpu.VMEM((2, n, 2, hd), bf16),
                pltpu.VMEM((2, CORES, n // CORES, 2, hd + 128), f32),
                pltpu.VMEM((2, n // CORES, 2, hd + 128), f32),
                pltpu.VMEM((2, n // CORES, 2, hd + 128), f32),
                pltpu.VMEM((2, n // CORES, 2, hd + 128), f32),
                pltpu.VMEM((2, CORES, 4, ROW), f32),
                pltpu.VMEM((2, 4, ROW), f32),
                pltpu.VMEM((2, 4, 4, ROW), f32),
                pltpu.VMEM((2, CORES, 4, ROW), f32),
                pltpu.VMEM((RELAY, hd), bf16),
                dma((6,)), dma((16,)), dma((8,)), dma((2, 2)), dma((2, 2)), dma((2, n)), dma((2, n)), dma((2, 4)), dma((2, 2)),
                dma((2, n - 1)), dma((2, n)), dma((2, 2)), dma((2, 3)), dma((2, n // CORES)), dma((2, 2)), dma((2, 2)), dma((2, 2)), dma((2, 2)), dma((4,)), pltpu.SemaphoreType.REGULAR,
            ],
            compiler_params=pltpu.CompilerParams(collective_id=0, has_side_effects=True, vmem_limit_bytes=48 * 2**20),
        )(hidden_in, table, loc_k, loc_v, glo_k, glo_v, loc_wq, loc_wk, loc_wv, loc_wo, loc_pre, loc_post, glo_wq, glo_wk, glo_wv, glo_wo, glo_pre, glo_post)
        return pl.pallas_call(
            store_outputs,
            name="store_outputs",
            out_shape=tuple(jax.ShapeDtypeStruct(x.shape, x.dtype) for x in landed),
            in_specs=[vmem] * 5,
            out_specs=(hbm,) * 5,
            scratch_shapes=[dma((5, STORE_PARTS))],
            compiler_params=pltpu.CompilerParams(vmem_limit_bytes=2**20),
        )(*landed)

    return jax.shard_map(device_step, mesh=mesh, in_specs=in_specs, out_specs=out_specs, check_vma=False)
```
